256 devices in a mesh: grp: 2 (over z), row: 16 (over x, core), sub: 8 (over y).
Axes of the slice: x: 8, y: 8, z: 2, core: 2. Of those that a mesh axis runs over, the one named last changes fastest.
The devices are a block of a 8x8x16 slice.
Arguments:
- residual_in: float32 [4, 2048, 2048], P('grp', ('row', 'sub')), parts along dimension 0, may hold values from -100 to 100
- direction: float32 [4, 2048, 2048], P('grp', ('row', 'sub')), parts along dimension 0, may hold values from -100 to 100
- spectrum: float32 [8192, 4096], P('grp', ('row', 'sub')), parts along dimension 0, may hold values from 0.0999 to 10.001, as said below
- noise_var: float32 [2], P('grp'), parts along dimension 0, may hold values from 0.5 to 2
Outputs:
- residual_out: float32 [4, 2048, 2048], P('grp', ('row', 'sub')), parts along dimension 0
- direction_out: float32 [4, 2048, 2048], P('grp', ('row', 'sub')), parts along dimension 0
- step_size: float32 [4], P('grp'), parts along dimension 0
The draws below stay inside these ranges and needn't reach their ends.
There are 2 independent parts, one for each index of `grp`. The reference program is written for one: setup_inputs(seed, part) draws one part's arguments, and reference() takes and returns one part's arrays. A program takes and returns all parts, laid end to end along the dimension named above; each array names one. Nothing has to cross between parts.
Inputs may be any that keep to these rules, and one draw needn't show every extreme that they name: spectrum[k, l] = spectrum[(4096 - k) % 4096, (4096 - l) % 4096] for all k, l.
All inputs are finite; a program needn't handle non-finite values.
Results may differ from the reference program's by a relative error of at most 0.00005.
Values sent between devices are 32-bit elements; how exact they have to be, the bound alone decides.
A program may use at most 64 MiB of HBM per device.

```python
import math
import jax
import jax.numpy as jnp
from jax import lax

GRID = 2048
EMBED = 4096
PROBES = 2


def field_values(key):
    subkeys = jax.random.split(key, 4)
    row_pos = jnp.arange(GRID, dtype=jnp.float32) / GRID
    row_log = 0.5 * row_pos + 0.5 * jax.random.uniform(subkeys[0], (GRID,))
    col_log = jax.random.uniform(subkeys[1], (GRID,))
    raw_vals = jax.random.normal(subkeys[3], (PROBES, GRID, GRID))
    values = raw_vals * jnp.power(10.0, row_log[:, None] + col_log[None, :] - 1.0)
    return jnp.clip(values, -100.0, 100.0).astype(jnp.float32)


def draw_residual_in(key, part):
    return field_values(jax.random.fold_in(key, 101))


def draw_direction(key, part):
    return field_values(jax.random.fold_in(key, 202))


def draw_spectrum(key, part):
    subkey = jax.random.fold_in(key, 303)
    raw_log = jax.random.uniform(subkey, (EMBED, EMBED), minval=-1.0, maxval=1.0)
    mirrored = jnp.roll(jnp.flip(raw_log, (0, 1)), 1, (0, 1))
    return jnp.power(10.0, 0.5 * (raw_log + mirrored)).astype(jnp.float32)


def setup_inputs(seed: int = 0, part: int = 0) -> dict:
    key_of = jax.random.split(jax.random.key(seed), 5)
    part_keys = jax.random.split(jax.random.fold_in(key_of[4], part), 5)
    return {
        "residual_in": draw_residual_in(jax.random.fold_in(jax.random.fold_in(key_of[4], part), 71), part),
        "direction": draw_direction(jax.random.fold_in(jax.random.fold_in(key_of[4], part), 71), part),
        "spectrum": draw_spectrum(jax.random.fold_in(jax.random.fold_in(key_of[4], part), 71), part),
        "noise_var": jnp.clip(jnp.exp(jax.random.uniform(part_keys[3], (1,), jnp.float32, math.log(0.5), math.log(2.0))), 0.5, 2.0),
    }


tiny_value = 1e-6


def reference(residual_in, direction, spectrum, noise_var):
    def one_probe(field_in):
        padded = jnp.pad(field_in, ((0, EMBED - GRID), (0, EMBED - GRID)))
        spectral = jnp.fft.fft2(padded)
        restored = jnp.fft.ifft2(spectral * spectrum)
        return jnp.real(restored)[:GRID, :GRID] + noise_var[0] * field_in

    image_out = lax.map(one_probe, direction)
    old_norm = jnp.sum(residual_in * residual_in, axis=(1, 2))
    curvature = jnp.sum(direction * image_out, axis=(1, 2))
    step_size = old_norm / curvature
    residual_out = residual_in - step_size[:, None, None] * image_out
    new_norm = jnp.sum(residual_out * residual_out, axis=(1, 2))
    direction_out = residual_out + (new_norm / (old_norm + tiny_value))[:, None, None] * direction
    return residual_out, direction_out, step_size
```

```python
import functools
import math

import jax
import jax.numpy as jnp
import ml_dtypes
import numpy as np
from jax import lax
from jax.experimental import pallas as pl
from jax.experimental.pallas import tpu as pltpu
from jax.sharding import PartitionSpec as P

ROW_SUB = ("row", "sub")
MESH = pl.DeviceIdType.MESH
TINY = 1e-06
LANES = 128
RADIX = 16
F32 = jnp.float32
BF16 = jnp.bfloat16


def roots(left, right, modulus, sign):
    turns = np.mod(np.outer(left, right), modulus)
    return np.exp(sign * 2j * np.pi * turns / modulus)


def real_form(table):
    return np.block([[table.real, -table.imag], [table.imag, table.real]])


def halves(table):
    high = table.astype(ml_dtypes.bfloat16)
    low = (table - high.astype(np.float64)).astype(ml_dtypes.bfloat16)
    return np.stack([high, low])


def tables(rows_dev, grid_len, devices):
    embed = 2 * grid_len
    lane_ids = np.arange(LANES)
    dev_ids = np.arange(devices)
    block = LANES // RADIX
    long_row = real_form(roots(dev_ids, lane_ids, LANES, -1))
    low_ids = np.arange(embed // RADIX)
    long_col = real_form(roots(low_ids, dev_ids, embed // RADIX, -1))
    short = roots(np.arange(RADIX), np.arange(RADIX), RADIX, -1)
    mixed = np.zeros((block, RADIX, RADIX, block), complex)
    for e in range(block):
        mixed[e, :, :, e] = short
    mixed = mixed.reshape(LANES, LANES)
    short_col = real_form(mixed.T).T
    short_back = real_form(np.conj(mixed)).T
    long_back = real_form(np.conj(roots(dev_ids, low_ids, embed // RADIX, -1)))
    half = long_back.shape[1] // 2
    row_back = real_form(np.conj(roots(lane_ids, dev_ids, LANES, -1))).T
    stacked = np.concatenate(
        [long_row, long_col, short_col, short_back, long_back[:, :half], long_back[:, half:], row_back], axis=0
    )
    consts = halves(stacked)
    turn_col = np.tile(roots(low_ids, np.arange(RADIX), embed, -1), (1, block))
    turn_col = np.stack([turn_col.real, turn_col.imag]).astype(np.float32)
    turn_row = np.zeros((2, 2 * RADIX, 2, LANES))
    for ch in range(2):
        for e in range(RADIX):
            turn = roots([2 * e + ch], lane_ids, embed, -1)[0]
            turn_row[ch, e] = [turn.real, turn.imag]
            odd = np.exp(-2j * np.pi * e * ch / (2 * RADIX))
            turn_row[ch, RADIX + e, 0] = odd.real
            turn_row[ch, RADIX + e, 1] = odd.imag
    turn_row = turn_row.reshape(2, 4 * RADIX, LANES).astype(np.float32)
    width = 2 * RADIX
    pick = np.zeros((RADIX, width, 2, 2, RADIX, block))
    for high in range(RADIX):
        for ch in range(2):
            for tile in range(2):
                for e in range(block):
                    pick[high, 2 * (block * tile + e) + ch, ch, tile, high, e] = 1
    pick = pick.reshape(RADIX * width, 4 * LANES).astype(ml_dtypes.bfloat16)
    return consts, turn_col, turn_row, pick


def add(x, y):
    return (x[0] + y[0], x[1] + y[1])


def sub(x, y):
    return (x[0] - y[0], x[1] - y[1])


def times(x, y):
    return (x[0] * y[0] - x[1] * y[1], x[0] * y[1] + x[1] * y[0])


def times_conj(x, y):
    return (x[0] * y[0] + x[1] * y[1], x[1] * y[0] - x[0] * y[1])


def by_root(x, power, sign):
    power %= RADIX
    if power == 0:
        return x
    if power == 4:
        return (x[1], -x[0]) if sign < 0 else (-x[1], x[0])
    if power == 8:
        return (-x[0], -x[1])
    angle = sign * 2.0 * math.pi * power / RADIX
    return times(x, (math.cos(angle), math.sin(angle)))


def four(x, sign):
    even, odd = add(x[0], x[2]), sub(x[0], x[2])
    both, diff = add(x[1], x[3]), sub(x[1], x[3])
    turned = (diff[1], -diff[0]) if sign < 0 else (-diff[1], diff[0])
    return [add(even, both), add(odd, turned), sub(even, both), sub(odd, turned)]


def sixteen(x, sign):
    inner = [four([x[4 * i + j] for i in range(4)], sign) for j in range(4)]
    out = [None] * RADIX
    for first in range(4):
        column = [by_root(inner[j][first], j * first, sign) for j in range(4)]
        for second, value in enumerate(four(column, sign)):
            out[first + 4 * second] = value
    return out


def split(value):
    high = value.astype(BF16)
    return high, (value - high.astype(F32)).astype(BF16)


def dot(left, right, transposed=False):
    dims = (((1,), (1 if transposed else 0,)), ((), ()))
    return lax.dot_general(left, right, dims, preferred_element_type=F32)


def dot3(left, right, transposed=False):
    return (
        dot(left[1], right[0], transposed) + dot(left[0], right[1], transposed) + dot(left[0], right[0], transposed)
    )


def far_first(n_row, n_sub):
    def chips(row, sub_):
        hop = row // 2
        return min(hop, n_row // 2 - hop) + min(sub_, n_sub - sub_)

    offsets = [(i, j) for i in range(n_row) for j in range(n_sub)][1:]
    return sorted(offsets, key=lambda pair: -chips(*pair))


def kernel(
    n_row, n_sub, scale,
    noise_ref, resid_hbm, dir_hbm, spec_hbm, consts_hbm, turn_col_hbm, turn_row_hbm, pick_hbm,
    resid_out, dir_out, step_out,
    resid, direct, spec, consts, turn_col, turn_row, pick,
    out_f, in_f, out_b, in_b, sums, spec_t, image,
    work, tall, left_hi, left_lo, right_hi, right_lo,
    load_sem, send_f, recv_f, send_b, recv_b, send_s, recv_s,
):
    devices = n_row * n_sub
    row, sub_ = lax.axis_index("row"), lax.axis_index("sub")
    me = row * n_sub + sub_
    offsets = far_first(n_row, n_sub)
    wide = 2 * LANES
    low_len = turn_col.shape[1]

    def load(src, dst, slot):
        copy = pltpu.make_async_copy(src, dst, load_sem.at[slot])
        copy.start()
        return copy

    loads = [
        load(dir_hbm, direct, 0),
        load(turn_row_hbm, turn_row, 1),
        load(consts_hbm, consts, 2),
        load(spec_hbm, spec, 3),
        load(pick_hbm, pick, 4),
        load(turn_col_hbm, turn_col, 5),
        load(resid_hbm, resid, 6),
    ]

    def peer(i, j):
        return lax.rem(row + i, n_row), lax.rem(sub_ + j, n_sub)

    barrier = pltpu.get_barrier_semaphore()

    def greet(t, carry):
        other = peer(t // n_sub, lax.rem(t, n_sub))
        pl.semaphore_signal(
            barrier, inc=1, device_id={"row": other[0], "sub": other[1]}, device_id_type=MESH
        )
        return carry

    lax.fori_loop(1, devices, greet, 0)

    def const(index, count=1):
        rows = pl.ds(wide * index, wide * count)
        return consts[0, rows, :], consts[1, rows, :]

    def send_all(src, dst, ch, send_sem, recv_sem):
        part = pl.ds(4 * ch, 4)
        for i, j in offsets:
            to_row, to_sub = peer(i, j)
            pltpu.make_async_remote_copy(
                src.at[to_row * n_sub + to_sub, part],
                dst.at[me, part],
                send_sem.at[ch],
                recv_sem.at[ch],
                device_id={"row": to_row, "sub": to_sub},
                device_id_type=MESH,
            ).start()
        dst[me, part] = src[me, part]

    def wait_all(ref, ch, sem):
        others = ref.at[pl.ds(0, devices - 1), pl.ds(4 * ch, 4)]
        pltpu.make_async_copy(others, others, sem.at[ch]).wait()

    def flat(ref):
        return ref.reshape(devices * 8, LANES)

    def turn(ch, index):
        both = turn_row[ch, pl.ds(2 * index, 2), :]
        return both[0:1], both[1:2]

    loads[0].wait()
    loads[1].wait()
    loads[2].wait()

    def rows_forward(ch, carry):
        for top in range(2):
            lines = pl.ds(8 * top, 8)
            values = []
            for a in range(RADIX):
                lanes = pl.ds(LANES * a, LANES)
                values.append(times((direct[0, lines, lanes], direct[1, lines, lanes]), turn(ch, RADIX + a)))
            for e, value in enumerate(sixteen(values, -1)):
                value = times(value, turn(ch, e))
                for part in range(2):
                    work[pl.ds(RADIX * e + 8 * top, 8), pl.ds(LANES * part, LANES)] = value[part]
        for at in range(0, wide, 32):
            lines = pl.ds(at, 32)
            right_hi[lines, :], right_lo[lines, :] = split(work[lines, :])
        freq = dot3(const(0), (right_hi[pl.ds(0, wide), :], right_lo[pl.ds(0, wide), :]), transposed=True)
        for part in range(2):
            for tile in range(2):
                flat(out_f)[pl.ds(4 * ch + 2 * part + tile, devices, stride=8), :] = freq[
                    devices * part : devices * (part + 1), LANES * tile : LANES * (tile + 1)
                ]

        @pl.when(ch == 0)
        def _():
            pl.semaphore_wait(barrier, devices - 1)

        send_all(out_f, in_f, ch, send_f, recv_f)
        return carry

    lax.fori_loop(0, 2, rows_forward, 0)

    loads[3].wait()
    loads[4].wait()
    loads[5].wait()
    loads[6].wait()
    for at in range(0, low_len, 64):
        parts = [spec[pl.ds(low_len * high + at, 64), :] for high in range(RADIX)]
        joined = jnp.concatenate(parts, axis=1) * scale
        first = joined.astype(BF16)
        rest = joined - first.astype(F32)
        second, third = split(rest)
        spec_t[pl.ds(at, 64), :] = (dot(third, pick[...]) + dot(second, pick[...])) + dot(first, pick[...])

    def columns(ch, carry):
        wait_all(in_f, ch, recv_f)
        for part in range(2):
            for tile in range(2):
                here = (pl.ds(devices * part, devices), pl.ds(LANES * tile, LANES))
                right_hi[here], right_lo[here] = split(
                    flat(in_f)[pl.ds(4 * ch + 2 * part + tile, devices, stride=8), :]
                )
        tall[...] = dot3(const(1, 2), (right_hi[pl.ds(0, wide), :], right_lo[pl.ds(0, wide), :]))
        step = 32
        for tile in range(2):
            lanes = pl.ds(LANES * tile, LANES)
            for at in range(0, low_len, step):
                lines = pl.ds(at, step)
                value = times(
                    (tall[lines, lanes], tall[pl.ds(low_len + at, step), lanes]),
                    (turn_col[0, lines, :], turn_col[1, lines, :]),
                )
                for part in range(2):
                    here = (pl.ds(low_len * tile + at, step), pl.ds(LANES * part, LANES))
                    left_hi[here], left_lo[here] = split(value[part])
        tall[...] = dot3((left_hi[...], left_lo[...]), const(3))
        for tile in range(2):
            for at in range(0, low_len, step):
                weight = spec_t[pl.ds(at, step), pl.ds(pl.multiple_of(wide * ch + LANES * tile, LANES), LANES)]
                for part in range(2):
                    here = (pl.ds(low_len * tile + at, step), pl.ds(LANES * part, LANES))
                    left_hi[here], left_lo[here] = split(tall[here] * weight)
        tall[...] = dot3((left_hi[...], left_lo[...]), const(4))
        for tile in range(2):
            for at in range(0, low_len, step):
                lines = pl.ds(at, step)
                here = pl.ds(low_len * tile + at, step)
                value = times_conj(
                    (tall[here, pl.ds(0, LANES)], tall[here, pl.ds(LANES, LANES)]),
                    (turn_col[0, lines, :], turn_col[1, lines, :]),
                )
                for part in range(2):
                    there = (pl.ds(low_len * part + at, step), pl.ds(LANES * tile, LANES))
                    right_hi[there], right_lo[there] = split(value[part])
        low, high = pl.ds(0, low_len), pl.ds(low_len, low_len)
        grid = dot3(const(5), (right_hi[low, :], right_lo[low, :])) + dot3(
            const(6), (right_hi[high, :], right_lo[high, :])
        )
        for part in range(2):
            for tile in range(2):
                flat(out_b)[pl.ds(4 * ch + 2 * part + tile, devices, stride=8), :] = grid[
                    devices * part : devices * (part + 1), LANES * tile : LANES * (tile + 1)
                ]
        send_all(out_b, in_b, ch, send_b, recv_b)
        return carry

    lax.fori_loop(0, 2, columns, 0)

    noise = noise_ref[0]
    image[...] = noise * direct[...]

    def rows_back(ch, carry):
        wait_all(in_b, ch, recv_b)
        for part in range(2):
            for tile in range(2):
                here = (pl.ds(LANES * tile, LANES), pl.ds(devices * part, devices))
                block = flat(in_b)[pl.ds(4 * ch + 2 * part + tile, devices, stride=8), :]
                left_hi[here], left_lo[here] = split(block.T)
        work[...] = dot3((left_hi[pl.ds(0, wide), :], left_lo[pl.ds(0, wide), :]), const(7))
        for top in range(2):
            values = []
            for e in range(RADIX):
                lines = pl.ds(RADIX * e + 8 * top, 8)
                values.append(
                    times_conj((work[lines, pl.ds(0, LANES)], work[lines, pl.ds(LANES, LANES)]), turn(ch, e))
                )
            lines = pl.ds(8 * top, 8)
            for a, value in enumerate(sixteen(values, 1)):
                value = times_conj(value, turn(ch, RADIX + a))
                lanes = pl.ds(LANES * a, LANES)
                for part in range(2):
                    image[part, lines, lanes] += value[part]
        return carry

    lax.fori_loop(0, 2, rows_back, 0)

    def sum_rows(value):
        return jnp.sum(value, axis=0, keepdims=True)

    lines = []
    for probe in range(2):
        totals = [jnp.zeros((8, LANES), F32) for _ in range(4)]
        for top in range(2):
            for a in range(direct.shape[2] // LANES):
                here = (probe, pl.ds(8 * top, 8), pl.ds(LANES * a, LANES))
                r, d, q = resid[here], direct[here], image[here]
                for index, term in enumerate((r * r, d * q, r * q, q * q)):
                    totals[index] += term
        lines += [sum_rows(total) for total in totals]
    stacked = jnp.sum(jnp.concatenate(lines, axis=0), axis=1, keepdims=True)
    at_row = lax.broadcasted_iota(jnp.int32, (8, LANES), 0)
    at_lane = lax.broadcasted_iota(jnp.int32, (8, LANES), 1)
    mine = sum_rows(jnp.where(at_row == at_lane, stacked, 0.0))
    sums[me] = mine

    def tell(t, carry):
        to_row, to_sub = peer(t // n_sub, lax.rem(t, n_sub))
        pltpu.make_async_remote_copy(
            sums.at[me], sums.at[me], send_s, recv_s,
            device_id={"row": to_row, "sub": to_sub}, device_id_type=MESH,
        ).start()
        return carry

    lax.fori_loop(1, devices, tell, 0)
    for ch in range(2):
        wait_all(out_f, ch, send_f)
        wait_all(out_b, ch, send_b)
    others = sums.at[pl.ds(0, devices - 1)]
    pltpu.make_async_copy(others, others, send_s).wait()
    pltpu.make_async_copy(others, others, recv_s).wait()
    total = jnp.sum(sums[...], axis=0)

    sizes = []
    for probe in range(2):
        old_norm, curvature, cross, square = (total[:, 4 * probe + i : 4 * probe + i + 1] for i in range(4))
        size = old_norm / curvature
        new_norm = old_norm - 2.0 * (size * cross) + size * (size * square)
        ratio = new_norm / (old_norm + TINY)
        sizes.append(size)
        for a in range(direct.shape[2] // LANES):
            here = (probe, slice(None), pl.ds(LANES * a, LANES))
            value = resid[here] - size * image[here]
            resid_out[here] = value
            dir_out[here] = value + ratio * direct[here]
    lane = lax.broadcasted_iota(jnp.int32, (1, LANES), 1)
    step_out[...] = jnp.where(lane == 0, sizes[0], sizes[1])


def body(n_row, n_sub, residual_in, direction, spectrum, noise_var):
    probes, rows_dev, grid_len = direction.shape
    devices = n_row * n_sub
    embed = 2 * grid_len
    consts, turn_col, turn_row, pick = tables(rows_dev, grid_len, devices)
    low_len = embed // RADIX
    wide = 2 * LANES
    slots = (devices, 8, LANES)
    vmem = pltpu.VMEM
    sems = pltpu.SemaphoreType.DMA
    block = (probes, rows_dev, grid_len)
    any_spec = pl.BlockSpec(memory_space=pl.ANY)
    vmem_spec = pl.BlockSpec(memory_space=pltpu.VMEM)
    resid, direct, step = pl.pallas_call(
        functools.partial(kernel, n_row, n_sub, 1.0 / (embed * embed)),
        out_shape=(
            jax.ShapeDtypeStruct(block, F32),
            jax.ShapeDtypeStruct(block, F32),
            jax.ShapeDtypeStruct((1, LANES), F32),
        ),
        in_specs=[pl.BlockSpec(memory_space=pltpu.SMEM)] + [any_spec] * 7,
        out_specs=(vmem_spec,) * 3,
        scratch_shapes=[
            vmem(block, F32), vmem(block, F32), vmem(spectrum.shape, F32),
            vmem(consts.shape, BF16), vmem(turn_col.shape, F32), vmem(turn_row.shape, F32), vmem(pick.shape, BF16),
            vmem(slots, F32), vmem(slots, F32), vmem(slots, F32), vmem(slots, F32),
            vmem((devices, 1, LANES), F32), vmem((low_len, 4 * LANES), F32), vmem(block, F32),
            vmem((wide, wide), F32), vmem((2 * low_len, wide), F32),
            vmem((2 * low_len, wide), BF16), vmem((2 * low_len, wide), BF16),
            vmem((2 * low_len, wide), BF16), vmem((2 * low_len, wide), BF16),
            sems((7,)), sems((2,)), sems((2,)), sems((2,)), sems((2,)), sems, sems,
        ],
        compiler_params=pltpu.CompilerParams(collective_id=0, has_side_effects=True),
        name="cg_step",
    )(noise_var, residual_in, direction, spectrum, *(jnp.asarray(t) for t in (consts, turn_col, turn_row, pick)))
    return resid, direct, step[0, :probes]


def solution(mesh):
    in_specs = (P("grp", ROW_SUB, None), P("grp", ROW_SUB, None), P("grp", ROW_SUB), P("grp"))
    out_specs = (P("grp", ROW_SUB, None), P("grp", ROW_SUB, None), P("grp"))
    return jax.shard_map(
        functools.partial(body, mesh.shape["row"], mesh.shape["sub"]),
        mesh=mesh, in_specs=in_specs, out_specs=out_specs, check_vma=False,
    )
```

```python
import functools
import math

import jax
import jax.numpy as jnp
import ml_dtypes
import numpy as np
from jax import lax
from jax.experimental import pallas as pl
from jax.experimental.pallas import tpu as pltpu
from jax.sharding import PartitionSpec as P

ROW_SUB = ("row", "sub")
MESH = pl.DeviceIdType.MESH
TINY = 1e-06
LANES = 128
RADIX = 16
F32 = jnp.float32
BF16 = jnp.bfloat16


def roots(left, right, modulus, sign):
    turns = np.mod(np.outer(left, right), modulus)
    return np.exp(sign * 2j * np.pi * turns / modulus)


def real_form(table):
    return np.block([[table.real, -table.imag], [table.imag, table.real]])


def halves(table):
    high = table.astype(ml_dtypes.bfloat16)
    low = (table - high.astype(np.float64)).astype(ml_dtypes.bfloat16)
    return np.stack([high, low])


def tables(rows_dev, grid_len, devices):
    embed = 2 * grid_len
    lane_ids = np.arange(LANES)
    dev_ids = np.arange(devices)
    block = LANES // RADIX
    long_row = real_form(roots(dev_ids, lane_ids, LANES, -1))
    low_ids = np.arange(embed // RADIX)
    long_col = real_form(roots(low_ids, dev_ids, embed // RADIX, -1))
    short = roots(np.arange(RADIX), np.arange(RADIX), RADIX, -1)
    mixed = np.zeros((block, RADIX, RADIX, block), complex)
    for e in range(block):
        mixed[e, :, :, e] = short
    mixed = mixed.reshape(LANES, LANES)
    short_col = real_form(mixed.T).T
    short_back = real_form(np.conj(mixed)).T
    long_back = real_form(np.conj(roots(dev_ids, low_ids, embed // RADIX, -1)))
    half = long_back.shape[1] // 2
    row_back = real_form(np.conj(roots(lane_ids, dev_ids, LANES, -1))).T
    stacked = np.concatenate(
        [long_row, long_col, short_col, short_back, long_back[:, :half], long_back[:, half:], row_back], axis=0
    )
    consts = halves(stacked)
    turn_col = np.tile(roots(low_ids, np.arange(RADIX), embed, -1), (1, block))
    turn_col = np.stack([turn_col.real, turn_col.imag]).astype(np.float32)
    turn_row = np.zeros((2, 2 * RADIX, 2, LANES))
    for ch in range(2):
        for e in range(RADIX):
            turn = roots([2 * e + ch], lane_ids, embed, -1)[0]
            turn_row[ch, e] = [turn.real, turn.imag]
            odd = np.exp(-2j * np.pi * e * ch / (2 * RADIX))
            turn_row[ch, RADIX + e, 0] = odd.real
            turn_row[ch, RADIX + e, 1] = odd.imag
    turn_row = turn_row.reshape(2, 4 * RADIX, LANES).astype(np.float32)
    return consts, turn_col, turn_row


def add(x, y):
    return (x[0] + y[0], x[1] + y[1])


def sub(x, y):
    return (x[0] - y[0], x[1] - y[1])


def times(x, y):
    return (x[0] * y[0] - x[1] * y[1], x[0] * y[1] + x[1] * y[0])


def times_conj(x, y):
    return (x[0] * y[0] + x[1] * y[1], x[1] * y[0] - x[0] * y[1])


def by_root(x, power, sign):
    power %= RADIX
    if power == 0:
        return x
    if power == 4:
        return (x[1], -x[0]) if sign < 0 else (-x[1], x[0])
    if power == 8:
        return (-x[0], -x[1])
    angle = sign * 2.0 * math.pi * power / RADIX
    return times(x, (math.cos(angle), math.sin(angle)))


def four(x, sign):
    even, odd = add(x[0], x[2]), sub(x[0], x[2])
    both, diff = add(x[1], x[3]), sub(x[1], x[3])
    turned = (diff[1], -diff[0]) if sign < 0 else (-diff[1], diff[0])
    return [add(even, both), add(odd, turned), sub(even, both), sub(odd, turned)]


def sixteen(x, sign):
    inner = [four([x[4 * i + j] for i in range(4)], sign) for j in range(4)]
    out = [None] * RADIX
    for first in range(4):
        column = [by_root(inner[j][first], j * first, sign) for j in range(4)]
        for second, value in enumerate(four(column, sign)):
            out[first + 4 * second] = value
    return out


def split(value):
    high = value.astype(BF16)
    return high, (value - high.astype(F32)).astype(BF16)


def dot(left, right, transposed=False):
    dims = (((1,), (1 if transposed else 0,)), ((), ()))
    return lax.dot_general(left, right, dims, preferred_element_type=F32)


def dot3(left, right, transposed=False):
    return (
        dot(left[1], right[0], transposed) + dot(left[0], right[1], transposed) + dot(left[0], right[0], transposed)
    )


def far_first(n_row, n_sub):
    def chips(row, sub_):
        hop = row // 2
        return min(hop, n_row // 2 - hop) + min(sub_, n_sub - sub_)

    offsets = [(i, j) for i in range(n_row) for j in range(n_sub)][1:]
    return sorted(offsets, key=lambda pair: -chips(*pair))


def outward(count):
    return [count // 2 + (1 - 2 * (t % 2)) * ((t + 1) // 2) for t in range(count)]


def kernel(
    n_row, n_sub, scale,
    noise_ref, resid_hbm, dir_hbm, spec_hbm, consts_hbm, turn_col_hbm, turn_row_hbm,
    image_out, total_out,
    resid, direct, spec, consts, turn_col, turn_row,
    out_f, in_f, out_b, in_b, sums, spec_t, image,
    work, tall, left_hi, left_lo, right_hi, right_lo,
    load_sem, store_sem, send_f, recv_f, send_b, recv_b, send_s, recv_s,
):
    devices = n_row * n_sub
    row, sub_ = lax.axis_index("row"), lax.axis_index("sub")
    me = row * n_sub + sub_
    offsets = far_first(n_row, n_sub)
    wide = 2 * LANES
    low_len = turn_col.shape[1]

    def load(src, dst, slot):
        copy = pltpu.make_async_copy(src, dst, load_sem.at[slot])
        copy.start()
        return copy

    def wrap(value, count):
        return jnp.where(value >= count, value - count, value)

    def peer(i, j):
        return wrap(row + i, n_row), wrap(sub_ + j, n_sub)

    subs = [wrap(sub_ + j, n_sub) for j in outward(n_sub)]

    def each_peer(act):
        def one_row(t, carry):
            half = n_row // 2
            to_row = wrap(row + half + (1 - 2 * (t % 2)) * ((t + 1) // 2), n_row)
            for to_sub in subs:
                act(to_row, to_sub)
            return carry

        lax.fori_loop(0, n_row - 1, one_row, 0)
        for to_sub in subs[:-1]:
            act(row, to_sub)

    barrier = pltpu.get_barrier_semaphore()

    def greet(to_row, to_sub):
        pl.semaphore_signal(barrier, inc=1, device_id={"row": to_row, "sub": to_sub}, device_id_type=MESH)

    each_peer(greet)
    loads = [
        load(dir_hbm, direct, 0),
        load(turn_row_hbm, turn_row, 1),
        load(consts_hbm, consts, 2),
        load(turn_col_hbm, turn_col, 3),
        load(resid_hbm, resid, 4),
    ]
    loads += [load(spec_hbm.at[:, pl.ds(LANES * t, LANES)], spec.at[t], 5) for t in range(spec.shape[0])]

    def const(index, count=1):
        rows = pl.ds(wide * index, wide * count)
        return consts[0, rows, :], consts[1, rows, :]

    def send_all(src, dst, ch, send_sem, recv_sem):
        part = pl.ds(4 * ch, 4)
        for i, j in offsets:
            to_row, to_sub = peer(i, j)
            pltpu.make_async_remote_copy(
                src.at[to_row * n_sub + to_sub, part],
                dst.at[me, part],
                send_sem.at[ch],
                recv_sem.at[ch],
                device_id={"row": to_row, "sub": to_sub},
                device_id_type=MESH,
            ).start()
        dst[me, part] = src[me, part]

    def wait_all(ref, ch, sem):
        others = ref.at[pl.ds(0, devices - 1), pl.ds(4 * ch, 4)]
        pltpu.make_async_copy(others, others, sem.at[ch]).wait()

    def flat(ref):
        return ref.reshape(devices * 8, LANES)

    def turn(ch, index):
        both = turn_row[ch, pl.ds(2 * index, 2), :]
        return both[0:1], both[1:2]

    loads[0].wait()
    loads[1].wait()
    loads[2].wait()

    def rows_forward(ch, carry):
        for top in range(2):
            lines = pl.ds(8 * top, 8)
            values = []
            for a in range(RADIX):
                lanes = pl.ds(LANES * a, LANES)
                values.append(times((direct[0, lines, lanes], direct[1, lines, lanes]), turn(ch, RADIX + a)))
            for e, value in enumerate(sixteen(values, -1)):
                value = times(value, turn(ch, e))
                for part in range(2):
                    work[pl.ds(RADIX * e + 8 * top, 8), pl.ds(LANES * part, LANES)] = value[part]
        for at in range(0, wide, 32):
            lines = pl.ds(at, 32)
            right_hi[lines, :], right_lo[lines, :] = split(work[lines, :])
        freq = dot3(const(0), (right_hi[pl.ds(0, wide), :], right_lo[pl.ds(0, wide), :]), transposed=True)
        for part in range(2):
            for tile in range(2):
                flat(out_f)[pl.ds(4 * ch + 2 * part + tile, devices, stride=8), :] = freq[
                    devices * part : devices * (part + 1), LANES * tile : LANES * (tile + 1)
                ]

        @pl.when(ch == 0)
        def _():
            pl.semaphore_wait(barrier, devices - 1)

        send_all(out_f, in_f, ch, send_f, recv_f)
        return carry

    lax.fori_loop(0, 2, rows_forward, 0)

    for copy in loads[3:5]:
        copy.wait()
    pltpu.make_async_copy(spec, spec, load_sem.at[5]).wait()
    spec_rows = spec.reshape(spec.shape[0] * spec.shape[1], LANES)
    for ch in range(2):
        for tile in range(2):
            for top in range(low_len // LANES):
                parts = []
                for high in range(RADIX):
                    at = spec.shape[1] * ((low_len // LANES) * high + top) + RADIX * tile + ch
                    parts.append(spec_rows[pl.ds(at, 8, stride=2), :])
                spec_t[pl.ds(LANES * top, LANES), pl.ds(wide * ch + LANES * tile, LANES)] = (
                    jnp.concatenate(parts, axis=0).T * scale
                )

    def columns(ch, carry):
        wait_all(in_f, ch, recv_f)
        for part in range(2):
            for tile in range(2):
                here = (pl.ds(devices * part, devices), pl.ds(LANES * tile, LANES))
                right_hi[here], right_lo[here] = split(
                    flat(in_f)[pl.ds(4 * ch + 2 * part + tile, devices, stride=8), :]
                )
        tall[...] = dot3(const(1, 2), (right_hi[pl.ds(0, wide), :], right_lo[pl.ds(0, wide), :]))
        step = 32
        for tile in range(2):
            lanes = pl.ds(LANES * tile, LANES)
            for at in range(0, low_len, step):
                lines = pl.ds(at, step)
                value = times(
                    (tall[lines, lanes], tall[pl.ds(low_len + at, step), lanes]),
                    (turn_col[0, lines, :], turn_col[1, lines, :]),
                )
                for part in range(2):
                    here = (pl.ds(low_len * tile + at, step), pl.ds(LANES * part, LANES))
                    left_hi[here], left_lo[here] = split(value[part])
        tall[...] = dot3((left_hi[...], left_lo[...]), const(3))
        for tile in range(2):
            for at in range(0, low_len, step):
                weight = spec_t[pl.ds(at, step), pl.ds(pl.multiple_of(wide * ch + LANES * tile, LANES), LANES)]
                for part in range(2):
                    here = (pl.ds(low_len * tile + at, step), pl.ds(LANES * part, LANES))
                    left_hi[here], left_lo[here] = split(tall[here] * weight)
        tall[...] = dot3((left_hi[...], left_lo[...]), const(4))
        for tile in range(2):
            for at in range(0, low_len, step):
                lines = pl.ds(at, step)
                here = pl.ds(low_len * tile + at, step)
                value = times_conj(
                    (tall[here, pl.ds(0, LANES)], tall[here, pl.ds(LANES, LANES)]),
                    (turn_col[0, lines, :], turn_col[1, lines, :]),
                )
                for part in range(2):
                    there = (pl.ds(low_len * part + at, step), pl.ds(LANES * tile, LANES))
                    right_hi[there], right_lo[there] = split(value[part])
        low, high = pl.ds(0, low_len), pl.ds(low_len, low_len)
        grid = dot3(const(5), (right_hi[low, :], right_lo[low, :])) + dot3(
            const(6), (right_hi[high, :], right_lo[high, :])
        )
        for part in range(2):
            for tile in range(2):
                flat(out_b)[pl.ds(4 * ch + 2 * part + tile, devices, stride=8), :] = grid[
                    devices * part : devices * (part + 1), LANES * tile : LANES * (tile + 1)
                ]
        send_all(out_b, in_b, ch, send_b, recv_b)
        return carry

    lax.fori_loop(0, 2, columns, 0)

    noise = noise_ref[0]
    image[...] = noise * direct[...]

    def rows_back(ch, carry):
        wait_all(in_b, ch, recv_b)
        for part in range(2):
            for tile in range(2):
                here = (pl.ds(LANES * tile, LANES), pl.ds(devices * part, devices))
                block = flat(in_b)[pl.ds(4 * ch + 2 * part + tile, devices, stride=8), :]
                left_hi[here], left_lo[here] = split(block.T)
        work[...] = dot3((left_hi[pl.ds(0, wide), :], left_lo[pl.ds(0, wide), :]), const(7))
        for top in range(2):
            values = []
            for e in range(RADIX):
                lines = pl.ds(RADIX * e + 8 * top, 8)
                values.append(
                    times_conj((work[lines, pl.ds(0, LANES)], work[lines, pl.ds(LANES, LANES)]), turn(ch, e))
                )
            lines = pl.ds(8 * top, 8)
            for a, value in enumerate(sixteen(values, 1)):
                value = times_conj(value, turn(ch, RADIX + a))
                lanes = pl.ds(LANES * a, LANES)
                for part in range(2):
                    image[part, lines, lanes] += value[part]
        return carry

    lax.fori_loop(0, 2, rows_back, 0)
    leave = pltpu.make_async_copy(image, image_out, store_sem)
    leave.start()

    def sum_rows(value):
        return jnp.sum(value, axis=0, keepdims=True)

    lines = []
    for probe in range(2):
        totals = [jnp.zeros((8, LANES), F32) for _ in range(4)]
        for top in range(2):
            for a in range(direct.shape[2] // LANES):
                here = (probe, pl.ds(8 * top, 8), pl.ds(LANES * a, LANES))
                r, d, q = resid[here], direct[here], image[here]
                for index, term in enumerate((r * r, d * q, r * q, q * q)):
                    totals[index] += term
        lines += [sum_rows(total) for total in totals]
    stacked = jnp.sum(jnp.concatenate(lines, axis=0), axis=1, keepdims=True)
    at_row = lax.broadcasted_iota(jnp.int32, (8, LANES), 0)
    at_lane = lax.broadcasted_iota(jnp.int32, (8, LANES), 1)
    mine = sum_rows(jnp.where(at_row == at_lane, stacked, 0.0))
    sums[me] = mine

    def tell(to_row, to_sub):
        pltpu.make_async_remote_copy(
            sums.at[me], sums.at[me], send_s, recv_s,
            device_id={"row": to_row, "sub": to_sub}, device_id_type=MESH,
        ).start()

    each_peer(tell)
    for ch in range(2):
        wait_all(out_f, ch, send_f)
        wait_all(out_b, ch, send_b)
    others = sums.at[pl.ds(0, devices - 1)]
    pltpu.make_async_copy(others, others, send_s).wait()
    pltpu.make_async_copy(others, others, recv_s).wait()
    total_out[...] = jnp.sum(sums[...], axis=0)
    leave.wait()


def finish(total_ref, resid, direct, image, resid_out, dir_out, step_out):
    total = total_ref[...]
    for probe in range(2):
        old_norm, curvature, cross, square = (total[:, 4 * probe + i : 4 * probe + i + 1] for i in range(4))
        size = old_norm / curvature
        new_norm = old_norm - 2.0 * (size * cross) + size * (size * square)
        ratio = new_norm / (old_norm + TINY)
        step_out[probe] = size[0, 0]
        for a in range(direct.shape[2] // LANES):
            here = (probe, slice(None), pl.ds(LANES * a, LANES))
            value = resid[here] - size * image[here]
            resid_out[here] = value
            dir_out[here] = value + ratio * direct[here]


def body(n_row, n_sub, residual_in, direction, spectrum, noise_var):
    probes, rows_dev, grid_len = direction.shape
    devices = n_row * n_sub
    embed = 2 * grid_len
    consts, turn_col, turn_row = tables(rows_dev, grid_len, devices)
    low_len = embed // RADIX
    wide = 2 * LANES
    slots = (devices, 8, LANES)
    vmem = pltpu.VMEM
    sems = pltpu.SemaphoreType.DMA
    block = (probes, rows_dev, grid_len)
    hbm_spec = pl.BlockSpec(memory_space=pltpu.HBM)
    vmem_spec = pl.BlockSpec(memory_space=pltpu.VMEM)
    smem_spec = pl.BlockSpec(memory_space=pltpu.SMEM)
    image, total = pl.pallas_call(
        functools.partial(kernel, n_row, n_sub, 1.0 / (embed * embed)),
        out_shape=(jax.ShapeDtypeStruct(block, F32), jax.ShapeDtypeStruct((1, LANES), F32)),
        in_specs=[smem_spec] + [hbm_spec] * 6,
        out_specs=(hbm_spec, vmem_spec),
        scratch_shapes=[
            vmem(block, F32), vmem(block, F32), vmem((embed // LANES, spectrum.shape[1], LANES), F32),
            vmem(consts.shape, BF16), vmem(turn_col.shape, F32), vmem(turn_row.shape, F32),
            vmem(slots, F32), vmem(slots, F32), vmem(slots, F32), vmem(slots, F32),
            vmem((devices, 1, LANES), F32), vmem((low_len, 4 * LANES), F32), vmem(block, F32),
            vmem((wide, wide), F32), vmem((2 * low_len, wide), F32),
            vmem((2 * low_len, wide), BF16), vmem((2 * low_len, wide), BF16),
            vmem((2 * low_len, wide), BF16), vmem((2 * low_len, wide), BF16),
            sems((6,)), sems, sems((2,)), sems((2,)), sems((2,)), sems((2,)), sems, sems,
        ],
        compiler_params=pltpu.CompilerParams(collective_id=0, has_side_effects=True),
        name="cg_step",
    )(noise_var, residual_in, direction, spectrum.T, *(jnp.asarray(t) for t in (consts, turn_col, turn_row)))
    return pl.pallas_call(
        finish,
        out_shape=(
            jax.ShapeDtypeStruct(block, F32),
            jax.ShapeDtypeStruct(block, F32),
            jax.ShapeDtypeStruct((probes,), F32),
        ),
        in_specs=[vmem_spec] * 4,
        out_specs=(vmem_spec, vmem_spec, smem_spec),
        name="finish",
    )(total, residual_in, direction, image)


def solution(mesh):
    in_specs = (P("grp", ROW_SUB, None), P("grp", ROW_SUB, None), P("grp", ROW_SUB), P("grp"))
    out_specs = (P("grp", ROW_SUB, None), P("grp", ROW_SUB, None), P("grp"))
    return jax.shard_map(
        functools.partial(body, mesh.shape["row"], mesh.shape["sub"]),
        mesh=mesh, in_specs=in_specs, out_specs=out_specs, check_vma=False,
    )
```

```python
import functools
import math

import jax
import jax.numpy as jnp
import ml_dtypes
import numpy as np
from jax import lax
from jax.experimental import pallas as pl
from jax.experimental.pallas import tpu as pltpu
from jax.sharding import PartitionSpec as P

ROW_SUB = ("row", "sub")
MESH = pl.DeviceIdType.MESH
TINY = 1e-06
LANES = 128
RADIX = 16
F32 = jnp.float32
BF16 = jnp.bfloat16


def roots(left, right, modulus, sign):
    turns = np.mod(np.outer(left, right), modulus)
    return np.exp(sign * 2j * np.pi * turns / modulus)


def real_form(table):
    return np.block([[table.real, -table.imag], [table.imag, table.real]])


def halves(table):
    high = table.astype(ml_dtypes.bfloat16)
    low = (table - high.astype(np.float64)).astype(ml_dtypes.bfloat16)
    return np.stack([high, low])


def tables(rows_dev, grid_len, devices):
    embed = 2 * grid_len
    lane_ids = np.arange(LANES)
    dev_ids = np.arange(devices)
    block = LANES // RADIX
    long_row = real_form(roots(dev_ids, lane_ids, LANES, -1))
    low_ids = np.arange(embed // RADIX)
    long_col = real_form(roots(low_ids, dev_ids, embed // RADIX, -1))
    short = roots(np.arange(RADIX), np.arange(RADIX), RADIX, -1)
    mixed = np.zeros((block, RADIX, RADIX, block), complex)
    for e in range(block):
        mixed[e, :, :, e] = short
    mixed = mixed.reshape(LANES, LANES)
    short_col = real_form(mixed.T).T
    short_back = real_form(np.conj(mixed)).T
    long_back = real_form(np.conj(roots(dev_ids, low_ids, embed // RADIX, -1)))
    half = long_back.shape[1] // 2
    row_back = real_form(np.conj(roots(lane_ids, dev_ids, LANES, -1))).T
    stacked = np.concatenate(
        [long_row, long_col, short_col, short_back, long_back[:, :half], long_back[:, half:], row_back], axis=0
    )
    consts = halves(stacked)
    turn_col = np.tile(roots(low_ids, np.arange(RADIX), embed, -1), (1, block))
    turn_col = np.stack([turn_col.real, turn_col.imag]).astype(np.float32)
    turn_row = np.zeros((2, 2 * RADIX, 2, LANES))
    for ch in range(2):
        for e in range(RADIX):
            turn = roots([2 * e + ch], lane_ids, embed, -1)[0]
            turn_row[ch, e] = [turn.real, turn.imag]
            odd = np.exp(-2j * np.pi * e * ch / (2 * RADIX))
            turn_row[ch, RADIX + e, 0] = odd.real
            turn_row[ch, RADIX + e, 1] = odd.imag
    turn_row = turn_row.reshape(2, 4 * RADIX, LANES).astype(np.float32)
    return consts, turn_col, turn_row


def add(x, y):
    return (x[0] + y[0], x[1] + y[1])


def sub(x, y):
    return (x[0] - y[0], x[1] - y[1])


def times(x, y):
    return (x[0] * y[0] - x[1] * y[1], x[0] * y[1] + x[1] * y[0])


def times_conj(x, y):
    return (x[0] * y[0] + x[1] * y[1], x[1] * y[0] - x[0] * y[1])


def by_root(x, power, sign):
    power %= RADIX
    if power == 0:
        return x
    if power == 4:
        return (x[1], -x[0]) if sign < 0 else (-x[1], x[0])
    if power == 8:
        return (-x[0], -x[1])
    angle = sign * 2.0 * math.pi * power / RADIX
    return times(x, (math.cos(angle), math.sin(angle)))


def four(x, sign):
    even, odd = add(x[0], x[2]), sub(x[0], x[2])
    both, diff = add(x[1], x[3]), sub(x[1], x[3])
    turned = (diff[1], -diff[0]) if sign < 0 else (-diff[1], diff[0])
    return [add(even, both), add(odd, turned), sub(even, both), sub(odd, turned)]


def sixteen(x, sign):
    inner = [four([x[4 * i + j] for i in range(4)], sign) for j in range(4)]
    out = [None] * RADIX
    for first in range(4):
        column = [by_root(inner[j][first], j * first, sign) for j in range(4)]
        for second, value in enumerate(four(column, sign)):
            out[first + 4 * second] = value
    return out


def split(value):
    high = value.astype(BF16)
    return high, (value - high.astype(F32)).astype(BF16)


def dot(left, right, transposed=False):
    dims = (((1,), (1 if transposed else 0,)), ((), ()))
    return lax.dot_general(left, right, dims, preferred_element_type=F32)


def dot3(left, right, transposed=False):
    return (
        dot(left[1], right[0], transposed) + dot(left[0], right[1], transposed) + dot(left[0], right[0], transposed)
    )


def far_first(n_row, n_sub):
    def chips(row, sub_):
        hop = row // 2
        return min(hop, n_row // 2 - hop) + min(sub_, n_sub - sub_)

    offsets = [(i, j) for i in range(n_row) for j in range(n_sub)][1:]
    return sorted(offsets, key=lambda pair: -chips(*pair))


def outward(count):
    return [count // 2 + (1 - 2 * (t % 2)) * ((t + 1) // 2) for t in range(count)]


def kernel(
    n_row, n_sub, scale,
    noise_ref, resid_hbm, dir_hbm, spec_hbm, consts_hbm, turn_col_hbm, turn_row_hbm,
    image_out, total_out,
    resid, direct, spec, consts, turn_col, turn_row,
    out_f, in_f, out_b, in_b, sums, spec_t, image,
    work, tall, left_hi, left_lo, right_hi, right_lo,
    load_sem, store_sem, send_f, recv_f, send_b, recv_b, send_s, recv_s, here_sem,
):
    devices = n_row * n_sub
    row, sub_ = lax.axis_index("row"), lax.axis_index("sub")
    me = row * n_sub + sub_
    offsets = far_first(n_row, n_sub)
    wide = 2 * LANES
    low_len = turn_col.shape[1]

    def load(src, dst, slot):
        copy = pltpu.make_async_copy(src, dst, load_sem.at[slot])
        copy.start()
        return copy

    def wrap(value, count):
        return jnp.where(value >= count, value - count, value)

    def peer(i, j):
        return wrap(row + i, n_row), wrap(sub_ + j, n_sub)

    subs = [wrap(sub_ + j, n_sub) for j in outward(n_sub)]

    def each_peer(act):
        def one_row(t, carry):
            half = n_row // 2
            to_row = wrap(row + half + (1 - 2 * (t % 2)) * ((t + 1) // 2), n_row)
            for to_sub in subs:
                act(to_row, to_sub)
            return carry

        lax.fori_loop(0, n_row - 1, one_row, 0)
        for to_sub in subs[:-1]:
            act(row, to_sub)

    barrier = pltpu.get_barrier_semaphore()

    def greet(to_row, to_sub):
        pl.semaphore_signal(barrier, inc=1, device_id={"row": to_row, "sub": to_sub}, device_id_type=MESH)

    def announce(to_row, to_sub):
        pl.semaphore_signal(here_sem, inc=1, device_id={"row": to_row, "sub": to_sub}, device_id_type=MESH)

    @pl.when(me != 0)
    def _():
        each_peer(greet)

    loads = [
        load(dir_hbm, direct, 0),
        load(turn_row_hbm, turn_row, 1),
        load(consts_hbm, consts, 2),
        load(turn_col_hbm, turn_col, 3),
        load(resid_hbm, resid, 4),
    ]
    loads += [load(spec_hbm.at[:, pl.ds(LANES * t, LANES)], spec.at[t], 5) for t in range(spec.shape[0])]

    def const(index, count=1):
        rows = pl.ds(wide * index, wide * count)
        return consts[0, rows, :], consts[1, rows, :]

    def send(src, dst, ch, send_sem, recv_sem, to_row, to_sub):
        part = pl.ds(4 * ch, 4)
        pltpu.make_async_remote_copy(
            src.at[to_row * n_sub + to_sub, part],
            dst.at[me, part],
            send_sem.at[ch],
            recv_sem.at[ch],
            device_id={"row": to_row, "sub": to_sub},
            device_id_type=MESH,
        ).start()

    def send_all(src, dst, ch, send_sem, recv_sem, all_here):
        for i, j in offsets:
            to_row, to_sub = peer(i, j)
            go = functools.partial(send, src, dst, ch, send_sem, recv_sem, to_row, to_sub)
            if all_here:
                go()
            else:
                pl.when(to_row + to_sub != 0)(go)
        part = pl.ds(4 * ch, 4)
        dst[me, part] = src[me, part]

    def wait_all(ref, ch, sem):
        others = ref.at[pl.ds(0, devices - 1), pl.ds(4 * ch, 4)]
        pltpu.make_async_copy(others, others, sem.at[ch]).wait()

    def flat(ref):
        return ref.reshape(devices * 8, LANES)

    def turn(ch, index):
        both = turn_row[ch, pl.ds(2 * index, 2), :]
        return both[0:1], both[1:2]

    loads[0].wait()
    loads[1].wait()
    loads[2].wait()

    def rows_forward(ch, carry):
        for top in range(2):
            lines = pl.ds(8 * top, 8)
            values = []
            for a in range(RADIX):
                lanes = pl.ds(LANES * a, LANES)
                values.append(times((direct[0, lines, lanes], direct[1, lines, lanes]), turn(ch, RADIX + a)))
            for e, value in enumerate(sixteen(values, -1)):
                value = times(value, turn(ch, e))
                for part in range(2):
                    work[pl.ds(RADIX * e + 8 * top, 8), pl.ds(LANES * part, LANES)] = value[part]
        for at in range(0, wide, 32):
            lines = pl.ds(at, 32)
            right_hi[lines, :], right_lo[lines, :] = split(work[lines, :])
        freq = dot3(const(0), (right_hi[pl.ds(0, wide), :], right_lo[pl.ds(0, wide), :]), transposed=True)
        for part in range(2):
            for tile in range(2):
                flat(out_f)[pl.ds(4 * ch + 2 * part + tile, devices, stride=8), :] = freq[
                    devices * part : devices * (part + 1), LANES * tile : LANES * (tile + 1)
                ]

        @pl.when(ch == 0)
        def _():
            pl.semaphore_wait(barrier, jnp.where(me == 0, devices - 1, devices - 2))

            @pl.when(me == 0)
            def _():
                each_peer(announce)

        send_all(out_f, in_f, ch, send_f, recv_f, False)
        return carry

    lax.fori_loop(0, 2, rows_forward, 0)

    for copy in loads[3:5]:
        copy.wait()
    pltpu.make_async_copy(spec, spec, load_sem.at[5]).wait()
    spec_rows = spec.reshape(spec.shape[0] * spec.shape[1], LANES)
    for ch in range(2):
        for tile in range(2):
            for top in range(low_len // LANES):
                parts = []
                for high in range(RADIX):
                    at = spec.shape[1] * ((low_len // LANES) * high + top) + RADIX * tile + ch
                    parts.append(spec_rows[pl.ds(at, 8, stride=2), :])
                spec_t[pl.ds(LANES * top, LANES), pl.ds(wide * ch + LANES * tile, LANES)] = (
                    jnp.concatenate(parts, axis=0).T * scale
                )

    @pl.when(me != 0)
    def _():
        pl.semaphore_wait(here_sem, 1)
        for ch in range(2):
            send(out_f, in_f, ch, send_f, recv_f, 0, 0)

    def columns(ch, carry):
        wait_all(in_f, ch, recv_f)
        for part in range(2):
            for tile in range(2):
                here = (pl.ds(devices * part, devices), pl.ds(LANES * tile, LANES))
                right_hi[here], right_lo[here] = split(
                    flat(in_f)[pl.ds(4 * ch + 2 * part + tile, devices, stride=8), :]
                )
        tall[...] = dot3(const(1, 2), (right_hi[pl.ds(0, wide), :], right_lo[pl.ds(0, wide), :]))
        step = 32
        for tile in range(2):
            lanes = pl.ds(LANES * tile, LANES)
            for at in range(0, low_len, step):
                lines = pl.ds(at, step)
                value = times(
                    (tall[lines, lanes], tall[pl.ds(low_len + at, step), lanes]),
                    (turn_col[0, lines, :], turn_col[1, lines, :]),
                )
                for part in range(2):
                    here = (pl.ds(low_len * tile + at, step), pl.ds(LANES * part, LANES))
                    left_hi[here], left_lo[here] = split(value[part])
        tall[...] = dot3((left_hi[...], left_lo[...]), const(3))
        for tile in range(2):
            for at in range(0, low_len, step):
                weight = spec_t[pl.ds(at, step), pl.ds(pl.multiple_of(wide * ch + LANES * tile, LANES), LANES)]
                for part in range(2):
                    here = (pl.ds(low_len * tile + at, step), pl.ds(LANES * part, LANES))
                    left_hi[here], left_lo[here] = split(tall[here] * weight)
        tall[...] = dot3((left_hi[...], left_lo[...]), const(4))
        for tile in range(2):
            for at in range(0, low_len, step):
                lines = pl.ds(at, step)
                here = pl.ds(low_len * tile + at, step)
                value = times_conj(
                    (tall[here, pl.ds(0, LANES)], tall[here, pl.ds(LANES, LANES)]),
                    (turn_col[0, lines, :], turn_col[1, lines, :]),
                )
                for part in range(2):
                    there = (pl.ds(low_len * part + at, step), pl.ds(LANES * tile, LANES))
                    right_hi[there], right_lo[there] = split(value[part])
        low, high = pl.ds(0, low_len), pl.ds(low_len, low_len)
        grid = dot3(const(5), (right_hi[low, :], right_lo[low, :])) + dot3(
            const(6), (right_hi[high, :], right_lo[high, :])
        )
        for part in range(2):
            for tile in range(2):
                flat(out_b)[pl.ds(4 * ch + 2 * part + tile, devices, stride=8), :] = grid[
                    devices * part : devices * (part + 1), LANES * tile : LANES * (tile + 1)
                ]
        send_all(out_b, in_b, ch, send_b, recv_b, True)
        return carry

    lax.fori_loop(0, 2, columns, 0)

    noise = noise_ref[0]
    image[...] = noise * direct[...]

    def rows_back(ch, carry):
        wait_all(in_b, ch, recv_b)
        for part in range(2):
            for tile in range(2):
                here = (pl.ds(LANES * tile, LANES), pl.ds(devices * part, devices))
                block = flat(in_b)[pl.ds(4 * ch + 2 * part + tile, devices, stride=8), :]
                left_hi[here], left_lo[here] = split(block.T)
        work[...] = dot3((left_hi[pl.ds(0, wide), :], left_lo[pl.ds(0, wide), :]), const(7))
        for top in range(2):
            values = []
            for e in range(RADIX):
                lines = pl.ds(RADIX * e + 8 * top, 8)
                values.append(
                    times_conj((work[lines, pl.ds(0, LANES)], work[lines, pl.ds(LANES, LANES)]), turn(ch, e))
                )
            lines = pl.ds(8 * top, 8)
            for a, value in enumerate(sixteen(values, 1)):
                value = times_conj(value, turn(ch, RADIX + a))
                lanes = pl.ds(LANES * a, LANES)
                for part in range(2):
                    image[part, lines, lanes] += value[part]
        return carry

    lax.fori_loop(0, 2, rows_back, 0)
    leave = pltpu.make_async_copy(image, image_out, store_sem)
    leave.start()

    def sum_rows(value):
        return jnp.sum(value, axis=0, keepdims=True)

    lines = []
    for probe in range(2):
        totals = [jnp.zeros((8, LANES), F32) for _ in range(4)]
        for top in range(2):
            for a in range(direct.shape[2] // LANES):
                here = (probe, pl.ds(8 * top, 8), pl.ds(LANES * a, LANES))
                r, d, q = resid[here], direct[here], image[here]
                for index, term in enumerate((r * r, d * q, r * q, q * q)):
                    totals[index] += term
        lines += [sum_rows(total) for total in totals]
    stacked = jnp.sum(jnp.concatenate(lines, axis=0), axis=1, keepdims=True)
    at_row = lax.broadcasted_iota(jnp.int32, (8, LANES), 0)
    at_lane = lax.broadcasted_iota(jnp.int32, (8, LANES), 1)
    mine = sum_rows(jnp.where(at_row == at_lane, stacked, 0.0))
    sums[me] = mine

    def tell(to_row, to_sub):
        pltpu.make_async_remote_copy(
            sums.at[me], sums.at[me], send_s, recv_s,
            device_id={"row": to_row, "sub": to_sub}, device_id_type=MESH,
        ).start()

    each_peer(tell)
    for ch in range(2):
        wait_all(out_f, ch, send_f)
        wait_all(out_b, ch, send_b)
    others = sums.at[pl.ds(0, devices - 1)]
    pltpu.make_async_copy(others, others, send_s).wait()
    pltpu.make_async_copy(others, others, recv_s).wait()
    total_out[...] = jnp.sum(sums[...], axis=0)
    leave.wait()


def finish(total_ref, resid, direct, image, resid_out, dir_out, step_out):
    total = total_ref[...]
    for probe in range(2):
        old_norm, curvature, cross, square = (total[:, 4 * probe + i : 4 * probe + i + 1] for i in range(4))
        size = old_norm / curvature
        new_norm = old_norm - 2.0 * (size * cross) + size * (size * square)
        ratio = new_norm / (old_norm + TINY)
        step_out[probe] = size[0, 0]
        for a in range(direct.shape[2] // LANES):
            here = (probe, slice(None), pl.ds(LANES * a, LANES))
            value = resid[here] - size * image[here]
            resid_out[here] = value
            dir_out[here] = value + ratio * direct[here]


def body(n_row, n_sub, residual_in, direction, spectrum, noise_var):
    probes, rows_dev, grid_len = direction.shape
    devices = n_row * n_sub
    embed = 2 * grid_len
    consts, turn_col, turn_row = tables(rows_dev, grid_len, devices)
    low_len = embed // RADIX
    wide = 2 * LANES
    slots = (devices, 8, LANES)
    vmem = pltpu.VMEM
    sems = pltpu.SemaphoreType.DMA
    block = (probes, rows_dev, grid_len)
    hbm_spec = pl.BlockSpec(memory_space=pltpu.HBM)
    vmem_spec = pl.BlockSpec(memory_space=pltpu.VMEM)
    smem_spec = pl.BlockSpec(memory_space=pltpu.SMEM)
    image, total = pl.pallas_call(
        functools.partial(kernel, n_row, n_sub, 1.0 / (embed * embed)),
        out_shape=(jax.ShapeDtypeStruct(block, F32), jax.ShapeDtypeStruct((1, LANES), F32)),
        in_specs=[smem_spec] + [hbm_spec] * 6,
        out_specs=(hbm_spec, vmem_spec),
        scratch_shapes=[
            vmem(block, F32), vmem(block, F32), vmem((embed // LANES, spectrum.shape[1], LANES), F32),
            vmem(consts.shape, BF16), vmem(turn_col.shape, F32), vmem(turn_row.shape, F32),
            vmem(slots, F32), vmem(slots, F32), vmem(slots, F32), vmem(slots, F32),
            vmem((devices, 1, LANES), F32), vmem((low_len, 4 * LANES), F32), vmem(block, F32),
            vmem((wide, wide), F32), vmem((2 * low_len, wide), F32),
            vmem((2 * low_len, wide), BF16), vmem((2 * low_len, wide), BF16),
            vmem((2 * low_len, wide), BF16), vmem((2 * low_len, wide), BF16),
            sems((6,)), sems, sems((2,)), sems((2,)), sems((2,)), sems((2,)), sems, sems, pltpu.SemaphoreType.REGULAR,
        ],
        compiler_params=pltpu.CompilerParams(collective_id=0, has_side_effects=True),
        name="cg_step",
    )(noise_var, residual_in, direction, spectrum.T, *(jnp.asarray(t) for t in (consts, turn_col, turn_row)))
    return pl.pallas_call(
        finish,
        out_shape=(
            jax.ShapeDtypeStruct(block, F32),
            jax.ShapeDtypeStruct(block, F32),
            jax.ShapeDtypeStruct((probes,), F32),
        ),
        in_specs=[vmem_spec] * 4,
        out_specs=(vmem_spec, vmem_spec, smem_spec),
        name="finish",
    )(total, residual_in, direction, image)


def solution(mesh):
    in_specs = (P("grp", ROW_SUB, None), P("grp", ROW_SUB, None), P("grp", ROW_SUB), P("grp"))
    out_specs = (P("grp", ROW_SUB, None), P("grp", ROW_SUB, None), P("grp"))
    return jax.shard_map(
        functools.partial(body, mesh.shape["row"], mesh.shape["sub"]),
        mesh=mesh, in_specs=in_specs, out_specs=out_specs, check_vma=False,
    )
```

```python
import functools
import math

import jax
import jax.numpy as jnp
import ml_dtypes
import numpy as np
from jax import lax
from jax.experimental import pallas as pl
from jax.experimental.pallas import tpu as pltpu
from jax.sharding import PartitionSpec as P

ROW_SUB = ("row", "sub")
MESH = pl.DeviceIdType.MESH
TINY = 1e-06
VMEM_LIMIT = 56 << 20
LANES = 128
RADIX = 16
F32 = jnp.float32
BF16 = jnp.bfloat16


def roots(left, right, modulus, sign):
    turns = np.mod(np.outer(left, right), modulus)
    return np.exp(sign * 2j * np.pi * turns / modulus)


def real_form(table):
    return np.block([[table.real, -table.imag], [table.imag, table.real]])


def halves(table):
    high = table.astype(ml_dtypes.bfloat16)
    low = (table - high.astype(np.float64)).astype(ml_dtypes.bfloat16)
    return np.stack([high, low])


def tables(rows_dev, grid_len, devices):
    embed = 2 * grid_len
    lane_ids = np.arange(LANES)
    dev_ids = np.arange(devices)
    block = LANES // RADIX
    long_row = real_form(roots(dev_ids, lane_ids, LANES, -1))
    low_ids = np.arange(embed // RADIX)
    long_col = real_form(roots(low_ids, dev_ids, embed // RADIX, -1))
    short = roots(np.arange(RADIX), np.arange(RADIX), RADIX, -1)
    mixed = np.zeros((block, RADIX, RADIX, block), complex)
    for e in range(block):
        mixed[e, :, :, e] = short
    mixed = mixed.reshape(LANES, LANES)
    short_col = real_form(mixed.T).T
    short_back = real_form(np.conj(mixed)).T
    long_back = real_form(np.conj(roots(dev_ids, low_ids, embed // RADIX, -1)))
    half = long_back.shape[1] // 2
    row_back = real_form(np.conj(roots(lane_ids, dev_ids, LANES, -1))).T
    stacked = np.concatenate(
        [long_row, long_col, short_col, short_back, long_back[:, :half], long_back[:, half:], row_back], axis=0
    )
    consts = halves(stacked)
    turn_col = np.tile(roots(low_ids, np.arange(RADIX), embed, -1), (1, block))
    turn_col = np.stack([turn_col.real, turn_col.imag]).astype(np.float32)
    turn_row = np.zeros((2, 2 * RADIX, 2, LANES))
    for ch in range(2):
        for e in range(RADIX):
            turn = roots([2 * e + ch], lane_ids, embed, -1)[0]
            turn_row[ch, e] = [turn.real, turn.imag]
            odd = np.exp(-2j * np.pi * e * ch / (2 * RADIX))
            turn_row[ch, RADIX + e, 0] = odd.real
            turn_row[ch, RADIX + e, 1] = odd.imag
    turn_row = turn_row.reshape(2, 4 * RADIX, LANES).astype(np.float32)
    return consts, turn_col, turn_row


def add(x, y):
    return (x[0] + y[0], x[1] + y[1])


def sub(x, y):
    return (x[0] - y[0], x[1] - y[1])


def times(x, y):
    return (x[0] * y[0] - x[1] * y[1], x[0] * y[1] + x[1] * y[0])


def times_conj(x, y):
    return (x[0] * y[0] + x[1] * y[1], x[1] * y[0] - x[0] * y[1])


def by_root(x, power, sign):
    power %= RADIX
    if power == 0:
        return x
    if power == 4:
        return (x[1], -x[0]) if sign < 0 else (-x[1], x[0])
    if power == 8:
        return (-x[0], -x[1])
    angle = sign * 2.0 * math.pi * power / RADIX
    return times(x, (math.cos(angle), math.sin(angle)))


def four(x, sign):
    even, odd = add(x[0], x[2]), sub(x[0], x[2])
    both, diff = add(x[1], x[3]), sub(x[1], x[3])
    turned = (diff[1], -diff[0]) if sign < 0 else (-diff[1], diff[0])
    return [add(even, both), add(odd, turned), sub(even, both), sub(odd, turned)]


def sixteen(x, sign):
    inner = [four([x[4 * i + j] for i in range(4)], sign) for j in range(4)]
    out = [None] * RADIX
    for first in range(4):
        column = [by_root(inner[j][first], j * first, sign) for j in range(4)]
        for second, value in enumerate(four(column, sign)):
            out[first + 4 * second] = value
    return out


def split(value):
    high = value.astype(BF16)
    return high, (value - high.astype(F32)).astype(BF16)


def dot(left, right, transposed=False):
    dims = (((1,), (1 if transposed else 0,)), ((), ()))
    return lax.dot_general(left, right, dims, preferred_element_type=F32)


def dot3(left, right, transposed=False):
    return (
        dot(left[1], right[0], transposed) + dot(left[0], right[1], transposed) + dot(left[0], right[0], transposed)
    )


def outward(count):
    return [count // 2 + (1 - 2 * (t % 2)) * ((t + 1) // 2) for t in range(count)]


def kernel(
    n_row, n_sub, scale,
    noise_ref, resid_hbm, dir_hbm, spec_hbm, consts_hbm, turn_col_hbm, turn_row_hbm,
    image_out, total_out,
    resid, direct, spec, consts, turn_col, turn_row,
    out_f, in_f, out_b, in_b, sums, spec_t, image,
    work, tall, left_hi, left_lo, right_hi, right_lo,
    load_sem, store_sem, send_f, recv_f, send_b, recv_b, send_s, recv_s, here_sem,
):
    devices = n_row * n_sub
    row, sub_ = lax.axis_index("row"), lax.axis_index("sub")
    me = row * n_sub + sub_
    wide = 2 * LANES
    low_len = turn_col.shape[1]

    def load(src, dst, slot):
        copy = pltpu.make_async_copy(src, dst, load_sem.at[slot])
        copy.start()
        return copy

    def wrap(value, count):
        return jnp.where(value >= count, value - count, value)

    rows = [wrap(row + i, n_row) for i in outward(n_row)]

    def mates(act):
        for to_row in rows[:-1]:
            act(to_row, sub_)

    def other_subs(act, wanted):
        def one_sub(t, carry):
            to_sub = wrap(sub_ + n_sub // 2 + (1 - 2 * (t % 2)) * ((t + 1) // 2), n_sub)

            @pl.when(wanted(to_sub))
            def _():
                for to_row in rows:
                    act(to_row, to_sub)

            return carry

        lax.fori_loop(0, n_sub - 1, one_sub, 0)

    def each_peer(act):
        other_subs(act, lambda to_sub: to_sub >= 0)
        mates(act)

    late = me == 0
    level = jnp.where(late, n_sub, sub_)

    loads = [load(dir_hbm, direct, 0), load(turn_row_hbm, turn_row, 1), load(consts_hbm, consts, 2)]
    barrier = pltpu.get_barrier_semaphore()

    def greet(to_row, to_sub):
        pl.semaphore_signal(barrier, inc=1, device_id={"row": to_row, "sub": to_sub}, device_id_type=MESH)

    def announce(to_row, to_sub):
        pl.semaphore_signal(here_sem.at[level], inc=1, device_id={"row": to_row, "sub": to_sub}, device_id_type=MESH)

    @pl.when(jnp.logical_not(late))
    def _():
        mates(greet)
        other_subs(greet, lambda to_sub: to_sub > sub_)
        pl.when(sub_ != 0)(lambda: greet(0, 0))

    loads += [
        load(turn_col_hbm, turn_col, 3),
        load(resid_hbm, resid, 4),
    ]
    loads += [load(spec_hbm.at[:, pl.ds(LANES * t, LANES)], spec.at[t], 5) for t in range(spec.shape[0])]

    def const(index, count=1):
        rows = pl.ds(wide * index, wide * count)
        return consts[0, rows, :], consts[1, rows, :]

    def send(src, dst, ch, send_sem, recv_sem, to_row, to_sub):
        part = pl.ds(4 * ch, 4)
        pltpu.make_async_remote_copy(
            src.at[to_row * n_sub + to_sub, part],
            dst.at[me, part],
            send_sem.at[ch],
            recv_sem.at[ch],
            device_id={"row": to_row, "sub": to_sub},
            device_id_type=MESH,
        ).start()

    def keep_own(src, dst, ch):
        part = pl.ds(4 * ch, 4)
        dst[me, part] = src[me, part]

    def wait_all(ref, ch, sem):
        others = ref.at[pl.ds(0, devices - 1), pl.ds(4 * ch, 4)]
        pltpu.make_async_copy(others, others, sem.at[ch]).wait()

    def flat(ref):
        return ref.reshape(devices * 8, LANES)

    def turn(ch, index):
        both = turn_row[ch, pl.ds(2 * index, 2), :]
        return both[0:1], both[1:2]

    loads[0].wait()
    loads[1].wait()
    loads[2].wait()

    def rows_forward(ch, carry):
        for top in range(2):
            lines = pl.ds(8 * top, 8)
            values = []
            for a in range(RADIX):
                lanes = pl.ds(LANES * a, LANES)
                values.append(times((direct[0, lines, lanes], direct[1, lines, lanes]), turn(ch, RADIX + a)))
            for e, value in enumerate(sixteen(values, -1)):
                value = times(value, turn(ch, e))
                for part in range(2):
                    work[pl.ds(RADIX * e + 8 * top, 8), pl.ds(LANES * part, LANES)] = value[part]
        for at in range(0, wide, 32):
            lines = pl.ds(at, 32)
            right_hi[lines, :], right_lo[lines, :] = split(work[lines, :])
        freq = dot3(const(0), (right_hi[pl.ds(0, wide), :], right_lo[pl.ds(0, wide), :]), transposed=True)
        for part in range(2):
            for tile in range(2):
                flat(out_f)[pl.ds(4 * ch + 2 * part + tile, devices, stride=8), :] = freq[
                    devices * part : devices * (part + 1), LANES * tile : LANES * (tile + 1)
                ]

        @pl.when(ch == 0)
        def _():
            pl.semaphore_wait(barrier, jnp.where(late, devices - 1, n_row * (sub_ + 1) - 2))
            pl.when(late)(lambda: each_peer(announce))

            @pl.when(jnp.logical_not(late))
            def _():
                for to_sub in range(n_sub):
                    pl.when((to_sub < sub_) & (row + to_sub != 0))(functools.partial(announce, row, to_sub))

        def go(to_row, to_sub):
            pl.when(to_row + to_sub != 0)(
                functools.partial(send, out_f, in_f, ch, send_f, recv_f, to_row, to_sub)
            )

        other_subs(go, lambda to_sub: to_sub <= level)
        mates(go)
        keep_own(out_f, in_f, ch)
        return carry

    lax.fori_loop(0, 2, rows_forward, 0)

    for copy in loads[3:5]:
        copy.wait()
    pltpu.make_async_copy(spec, spec, load_sem.at[5]).wait()
    spec_rows = spec.reshape(spec.shape[0] * spec.shape[1], LANES)
    for ch in range(2):
        for tile in range(2):
            for top in range(low_len // LANES):
                parts = []
                for high in range(RADIX):
                    at = spec.shape[1] * ((low_len // LANES) * high + top) + RADIX * tile + ch
                    parts.append(spec_rows[pl.ds(at, 8, stride=2), :])
                spec_t[pl.ds(LANES * top, LANES), pl.ds(wide * ch + LANES * tile, LANES)] = (
                    jnp.concatenate(parts, axis=0).T * scale
                )

    def later_class(to_sub, carry):
        @pl.when(to_sub > level)
        def _():
            pl.semaphore_wait(here_sem.at[to_sub], 1)
            for ch in range(2):
                for to_row in rows:
                    send(out_f, in_f, ch, send_f, recv_f, to_row, to_sub)

        return carry

    lax.fori_loop(1, n_sub, later_class, 0)

    @pl.when(jnp.logical_not(late))
    def _():
        pl.semaphore_wait(here_sem.at[n_sub], 1)
        for ch in range(2):
            send(out_f, in_f, ch, send_f, recv_f, 0, 0)

    def columns(ch, carry):
        wait_all(in_f, ch, recv_f)
        for part in range(2):
            for tile in range(2):
                here = (pl.ds(devices * part, devices), pl.ds(LANES * tile, LANES))
                right_hi[here], right_lo[here] = split(
                    flat(in_f)[pl.ds(4 * ch + 2 * part + tile, devices, stride=8), :]
                )
        tall[...] = dot3(const(1, 2), (right_hi[pl.ds(0, wide), :], right_lo[pl.ds(0, wide), :]))
        step = 32
        for tile in range(2):
            lanes = pl.ds(LANES * tile, LANES)
            for at in range(0, low_len, step):
                lines = pl.ds(at, step)
                value = times(
                    (tall[lines, lanes], tall[pl.ds(low_len + at, step), lanes]),
                    (turn_col[0, lines, :], turn_col[1, lines, :]),
                )
                for part in range(2):
                    here = (pl.ds(low_len * tile + at, step), pl.ds(LANES * part, LANES))
                    left_hi[here], left_lo[here] = split(value[part])
        tall[...] = dot3((left_hi[...], left_lo[...]), const(3))
        for tile in range(2):
            for at in range(0, low_len, step):
                weight = spec_t[pl.ds(at, step), pl.ds(pl.multiple_of(wide * ch + LANES * tile, LANES), LANES)]
                for part in range(2):
                    here = (pl.ds(low_len * tile + at, step), pl.ds(LANES * part, LANES))
                    left_hi[here], left_lo[here] = split(tall[here] * weight)
        tall[...] = dot3((left_hi[...], left_lo[...]), const(4))
        for tile in range(2):
            for at in range(0, low_len, step):
                lines = pl.ds(at, step)
                here = pl.ds(low_len * tile + at, step)
                value = times_conj(
                    (tall[here, pl.ds(0, LANES)], tall[here, pl.ds(LANES, LANES)]),
                    (turn_col[0, lines, :], turn_col[1, lines, :]),
                )
                for part in range(2):
                    there = (pl.ds(low_len * part + at, step), pl.ds(LANES * tile, LANES))
                    right_hi[there], right_lo[there] = split(value[part])
        low, high = pl.ds(0, low_len), pl.ds(low_len, low_len)
        grid = dot3(const(5), (right_hi[low, :], right_lo[low, :])) + dot3(
            const(6), (right_hi[high, :], right_lo[high, :])
        )
        for part in range(2):
            for tile in range(2):
                flat(out_b)[pl.ds(4 * ch + 2 * part + tile, devices, stride=8), :] = grid[
                    devices * part : devices * (part + 1), LANES * tile : LANES * (tile + 1)
                ]
        each_peer(functools.partial(send, out_b, in_b, ch, send_b, recv_b))
        keep_own(out_b, in_b, ch)
        return carry

    lax.fori_loop(0, 2, columns, 0)

    noise = noise_ref[0]
    image[...] = noise * direct[...]

    def rows_back(ch, carry):
        wait_all(in_b, ch, recv_b)
        for part in range(2):
            for tile in range(2):
                here = (pl.ds(LANES * tile, LANES), pl.ds(devices * part, devices))
                block = flat(in_b)[pl.ds(4 * ch + 2 * part + tile, devices, stride=8), :]
                left_hi[here], left_lo[here] = split(block.T)
        work[...] = dot3((left_hi[pl.ds(0, wide), :], left_lo[pl.ds(0, wide), :]), const(7))
        for top in range(2):
            values = []
            for e in range(RADIX):
                lines = pl.ds(RADIX * e + 8 * top, 8)
                values.append(
                    times_conj((work[lines, pl.ds(0, LANES)], work[lines, pl.ds(LANES, LANES)]), turn(ch, e))
                )
            lines = pl.ds(8 * top, 8)
            for a, value in enumerate(sixteen(values, 1)):
                value = times_conj(value, turn(ch, RADIX + a))
                lanes = pl.ds(LANES * a, LANES)
                for part in range(2):
                    image[part, lines, lanes] += value[part]
        return carry

    lax.fori_loop(0, 2, rows_back, 0)
    leave = pltpu.make_async_copy(image, image_out, store_sem)
    leave.start()

    def sum_rows(value):
        return jnp.sum(value, axis=0, keepdims=True)

    lines = []
    for probe in range(2):
        totals = [jnp.zeros((8, LANES), F32) for _ in range(4)]
        for top in range(2):
            for a in range(direct.shape[2] // LANES):
                here = (probe, pl.ds(8 * top, 8), pl.ds(LANES * a, LANES))
                r, d, q = resid[here], direct[here], image[here]
                for index, term in enumerate((r * r, d * q, r * q, q * q)):
                    totals[index] += term
        lines += [sum_rows(total) for total in totals]
    stacked = jnp.sum(jnp.concatenate(lines, axis=0), axis=1, keepdims=True)
    at_row = lax.broadcasted_iota(jnp.int32, (8, LANES), 0)
    at_lane = lax.broadcasted_iota(jnp.int32, (8, LANES), 1)
    mine = sum_rows(jnp.where(at_row == at_lane, stacked, 0.0))
    sums[me] = mine

    def tell(to_row, to_sub):
        pltpu.make_async_remote_copy(
            sums.at[me], sums.at[me], send_s, recv_s,
            device_id={"row": to_row, "sub": to_sub}, device_id_type=MESH,
        ).start()

    each_peer(tell)
    for ch in range(2):
        wait_all(out_f, ch, send_f)
        wait_all(out_b, ch, send_b)
    others = sums.at[pl.ds(0, devices - 1)]
    pltpu.make_async_copy(others, others, send_s).wait()
    pltpu.make_async_copy(others, others, recv_s).wait()
    total_out[...] = jnp.sum(sums[...], axis=0)
    leave.wait()


def finish(total_ref, resid, direct, image, resid_out, dir_out, step_out):
    total = total_ref[...]
    for probe in range(2):
        old_norm, curvature, cross, square = (total[:, 4 * probe + i : 4 * probe + i + 1] for i in range(4))
        size = old_norm / curvature
        new_norm = old_norm - 2.0 * (size * cross) + size * (size * square)
        ratio = new_norm / (old_norm + TINY)
        step_out[probe] = size[0, 0]
        for a in range(direct.shape[2] // LANES):
            here = (probe, slice(None), pl.ds(LANES * a, LANES))
            value = resid[here] - size * image[here]
            resid_out[here] = value
            dir_out[here] = value + ratio * direct[here]


def body(n_row, n_sub, residual_in, direction, spectrum, noise_var):
    probes, rows_dev, grid_len = direction.shape
    devices = n_row * n_sub
    embed = 2 * grid_len
    consts, turn_col, turn_row = tables(rows_dev, grid_len, devices)
    low_len = embed // RADIX
    wide = 2 * LANES
    slots = (devices, 8, LANES)
    vmem = pltpu.VMEM
    sems = pltpu.SemaphoreType.DMA
    block = (probes, rows_dev, grid_len)
    hbm_spec = pl.BlockSpec(memory_space=pltpu.HBM)
    vmem_spec = pl.BlockSpec(memory_space=pltpu.VMEM)
    smem_spec = pl.BlockSpec(memory_space=pltpu.SMEM)
    image, total = pl.pallas_call(
        functools.partial(kernel, n_row, n_sub, 1.0 / (embed * embed)),
        out_shape=(jax.ShapeDtypeStruct(block, F32), jax.ShapeDtypeStruct((1, LANES), F32)),
        in_specs=[smem_spec] + [hbm_spec] * 6,
        out_specs=(hbm_spec, vmem_spec),
        scratch_shapes=[
            vmem(block, F32), vmem(block, F32), vmem((embed // LANES, spectrum.shape[1], LANES), F32),
            vmem(consts.shape, BF16), vmem(turn_col.shape, F32), vmem(turn_row.shape, F32),
            vmem(slots, F32), vmem(slots, F32), vmem(slots, F32), vmem(slots, F32),
            vmem((devices, 1, LANES), F32), vmem((low_len, 4 * LANES), F32), vmem(block, F32),
            vmem((wide, wide), F32), vmem((2 * low_len, wide), F32),
            vmem((2 * low_len, wide), BF16), vmem((2 * low_len, wide), BF16),
            vmem((2 * low_len, wide), BF16), vmem((2 * low_len, wide), BF16),
            sems((6,)), sems, sems((2,)), sems((2,)), sems((2,)), sems((2,)), sems, sems, pltpu.SemaphoreType.REGULAR((n_sub + 1,)),
        ],
        compiler_params=pltpu.CompilerParams(
            collective_id=0, has_side_effects=True, vmem_limit_bytes=VMEM_LIMIT
        ),
        name="cg_step",
    )(noise_var, residual_in, direction, spectrum.T, *(jnp.asarray(t) for t in (consts, turn_col, turn_row)))
    return pl.pallas_call(
        finish,
        out_shape=(
            jax.ShapeDtypeStruct(block, F32),
            jax.ShapeDtypeStruct(block, F32),
            jax.ShapeDtypeStruct((probes,), F32),
        ),
        in_specs=[vmem_spec] * 4,
        out_specs=(vmem_spec, vmem_spec, smem_spec),
        compiler_params=pltpu.CompilerParams(vmem_limit_bytes=VMEM_LIMIT),
        name="finish",
    )(total, residual_in, direction, image)


def solution(mesh):
    in_specs = (P("grp", ROW_SUB, None), P("grp", ROW_SUB, None), P("grp", ROW_SUB), P("grp"))
    out_specs = (P("grp", ROW_SUB, None), P("grp", ROW_SUB, None), P("grp"))
    return jax.shard_map(
        functools.partial(body, mesh.shape["row"], mesh.shape["sub"]),
        mesh=mesh, in_specs=in_specs, out_specs=out_specs, check_vma=False,
    )
```

```python
import functools
import math

import jax
import jax.numpy as jnp
import ml_dtypes
import numpy as np
from jax import lax
from jax.experimental import pallas as pl
from jax.experimental.pallas import tpu as pltpu
from jax.sharding import PartitionSpec as P

ROW_SUB = ("row", "sub")
MESH = pl.DeviceIdType.MESH
TINY = 1e-06
VMEM_LIMIT = 107 << 19
LANES = 128
RADIX = 16
F32 = jnp.float32
BF16 = jnp.bfloat16


def roots(left, right, modulus, sign):
    turns = np.mod(np.outer(left, right), modulus)
    return np.exp(sign * 2j * np.pi * turns / modulus)


def real_form(table):
    return np.block([[table.real, -table.imag], [table.imag, table.real]])


def halves(table):
    high = table.astype(ml_dtypes.bfloat16)
    low = (table - high.astype(np.float64)).astype(ml_dtypes.bfloat16)
    return np.stack([high, low])


def tables(rows_dev, grid_len, devices):
    embed = 2 * grid_len
    lane_ids = np.arange(LANES)
    dev_ids = np.arange(devices)
    block = LANES // RADIX
    long_row = real_form(roots(dev_ids, lane_ids, LANES, -1))
    low_ids = np.arange(embed // RADIX)
    long_col = real_form(roots(low_ids, dev_ids, embed // RADIX, -1))
    short = roots(np.arange(RADIX), np.arange(RADIX), RADIX, -1)
    mixed = np.zeros((block, RADIX, RADIX, block), complex)
    for e in range(block):
        mixed[e, :, :, e] = short
    mixed = mixed.reshape(LANES, LANES)
    short_col = real_form(mixed.T).T
    short_back = real_form(np.conj(mixed)).T
    long_back = real_form(np.conj(roots(dev_ids, low_ids, embed // RADIX, -1)))
    half = long_back.shape[1] // 2
    row_back = real_form(np.conj(roots(lane_ids, dev_ids, LANES, -1))).T
    stacked = np.concatenate(
        [long_row, long_col, short_col, short_back, long_back[:, :half], long_back[:, half:], row_back], axis=0
    )
    consts = halves(stacked)
    turn_col = np.tile(roots(low_ids, np.arange(RADIX), embed, -1), (1, block))
    turn_col = np.stack([turn_col.real, turn_col.imag]).astype(np.float32)
    turn_row = np.zeros((2, 2 * RADIX, 2, LANES))
    for ch in range(2):
        for e in range(RADIX):
            turn = roots([2 * e + ch], lane_ids, embed, -1)[0]
            turn_row[ch, e] = [turn.real, turn.imag]
            odd = np.exp(-2j * np.pi * e * ch / (2 * RADIX))
            turn_row[ch, RADIX + e, 0] = odd.real
            turn_row[ch, RADIX + e, 1] = odd.imag
    turns = np.concatenate([turn_row.reshape(-1, LANES), turn_col.reshape(-1, LANES)]).astype(np.float32)
    return consts, turns


def add(x, y):
    return (x[0] + y[0], x[1] + y[1])


def sub(x, y):
    return (x[0] - y[0], x[1] - y[1])


def times(x, y):
    return (x[0] * y[0] - x[1] * y[1], x[0] * y[1] + x[1] * y[0])


def times_conj(x, y):
    return (x[0] * y[0] + x[1] * y[1], x[1] * y[0] - x[0] * y[1])


def by_root(x, power, sign):
    power %= RADIX
    if power == 0:
        return x
    if power == 4:
        return (x[1], -x[0]) if sign < 0 else (-x[1], x[0])
    if power == 8:
        return (-x[0], -x[1])
    angle = sign * 2.0 * math.pi * power / RADIX
    return times(x, (math.cos(angle), math.sin(angle)))


def four(x, sign):
    even, odd = add(x[0], x[2]), sub(x[0], x[2])
    both, diff = add(x[1], x[3]), sub(x[1], x[3])
    turned = (diff[1], -diff[0]) if sign < 0 else (-diff[1], diff[0])
    return [add(even, both), add(odd, turned), sub(even, both), sub(odd, turned)]


def sixteen(x, sign):
    inner = [four([x[4 * i + j] for i in range(4)], sign) for j in range(4)]
    out = [None] * RADIX
    for first in range(4):
        column = [by_root(inner[j][first], j * first, sign) for j in range(4)]
        for second, value in enumerate(four(column, sign)):
            out[first + 4 * second] = value
    return out


def split(value):
    high = value.astype(BF16)
    return high, (value - high.astype(F32)).astype(BF16)


def dot(left, right, transposed=False):
    dims = (((1,), (1 if transposed else 0,)), ((), ()))
    return lax.dot_general(left, right, dims, preferred_element_type=F32)


def dot3(left, right, transposed=False):
    return (
        dot(left[1], right[0], transposed) + dot(left[0], right[1], transposed) + dot(left[0], right[0], transposed)
    )


def far_first(n_row, n_sub):
    def chips(row, sub_):
        hop = row // 2
        return min(hop, n_row // 2 - hop) + min(sub_, n_sub - sub_)

    offsets = [(i, j) for i in range(n_row) for j in range(n_sub)][1:]
    return sorted(offsets, key=lambda pair: -chips(*pair))


def outward(count):
    return [count // 2 + (1 - 2 * (t % 2)) * ((t + 1) // 2) for t in range(count)]


def kernel(
    n_row, n_sub, scale,
    noise_ref, resid_hbm, dir_hbm, spec_hbm, consts_hbm, turns_hbm,
    image, total_out,
    resid, direct, spec, consts, turns,
    out_f, in_f, out_b, in_b, sums, spec_t,
    work, tall, left_hi, left_lo, right_hi, right_lo,
    load_sem, send_f, recv_f, send_b, recv_b, send_s, recv_s, here_sem,
):
    devices = n_row * n_sub
    row, sub_ = lax.axis_index("row"), lax.axis_index("sub")
    me = row * n_sub + sub_
    offsets = far_first(n_row, n_sub)
    wide = 2 * LANES
    low_len = tall.shape[0] // 2

    def load(src, dst, slot):
        copy = pltpu.make_async_copy(src, dst, load_sem.at[slot])
        copy.start()
        return copy

    def wrap(value, count):
        return jnp.where(value >= count, value - count, value)

    def peer(i, j):
        return wrap(row + i, n_row), wrap(sub_ + j, n_sub)

    subs = [wrap(sub_ + j, n_sub) for j in outward(n_sub)]

    def each_peer(act):
        def one_row(t, carry):
            half = n_row // 2
            to_row = wrap(row + half + (1 - 2 * (t % 2)) * ((t + 1) // 2), n_row)
            for to_sub in subs:
                act(to_row, to_sub)
            return carry

        lax.fori_loop(0, n_row - 1, one_row, 0)
        for to_sub in subs[:-1]:
            act(row, to_sub)

    loads = [load(dir_hbm, direct, 0), load(turns_hbm, turns, 1), load(consts_hbm, consts, 2)]
    barrier = pltpu.get_barrier_semaphore()

    def greet(to_row, to_sub):
        pl.semaphore_signal(barrier, inc=1, device_id={"row": to_row, "sub": to_sub}, device_id_type=MESH)

    def announce(to_row, to_sub):
        pl.semaphore_signal(here_sem, inc=1, device_id={"row": to_row, "sub": to_sub}, device_id_type=MESH)

    @pl.when(me != 0)
    def _():
        each_peer(greet)

    load(resid_hbm, resid, 3)
    for t in range(spec.shape[0]):
        load(spec_hbm.at[:, pl.ds(LANES * t, LANES)], spec.at[t], 4)

    def const(index, count=1):
        rows = pl.ds(wide * index, wide * count)
        return consts[0, rows, :], consts[1, rows, :]

    def send(src, dst, ch, send_sem, recv_sem, to_row, to_sub):
        part = pl.ds(4 * ch, 4)
        pltpu.make_async_remote_copy(
            src.at[to_row * n_sub + to_sub, part],
            dst.at[me, part],
            send_sem.at[ch],
            recv_sem.at[ch],
            device_id={"row": to_row, "sub": to_sub},
            device_id_type=MESH,
        ).start()

    def send_all(src, dst, ch, send_sem, recv_sem, all_here):
        for i, j in offsets:
            to_row, to_sub = peer(i, j)
            go = functools.partial(send, src, dst, ch, send_sem, recv_sem, to_row, to_sub)
            if all_here:
                go()
            else:
                pl.when(to_row + to_sub != 0)(go)
        part = pl.ds(4 * ch, 4)
        dst[me, part] = src[me, part]

    def wait_all(ref, ch, sem):
        others = ref.at[pl.ds(0, devices - 1), pl.ds(4 * ch, 4)]
        pltpu.make_async_copy(others, others, sem.at[ch]).wait()

    def flat(ref):
        return ref.reshape(devices * 8, LANES)

    def turn(ch, index):
        both = turns[pl.ds(4 * RADIX * ch + 2 * index, 2), :]
        return both[0:1], both[1:2]

    def turn_col(at, step):
        first = 8 * RADIX + at
        return turns[pl.ds(first, step), :], turns[pl.ds(first + low_len, step), :]

    for copy in loads:
        copy.wait()

    def rows_forward(ch, carry):
        for top in range(2):
            lines = pl.ds(8 * top, 8)
            values = []
            for a in range(RADIX):
                lanes = pl.ds(LANES * a, LANES)
                values.append(times((direct[0, lines, lanes], direct[1, lines, lanes]), turn(ch, RADIX + a)))
            for e, value in enumerate(sixteen(values, -1)):
                value = times(value, turn(ch, e))
                for part in range(2):
                    work[pl.ds(RADIX * e + 8 * top, 8), pl.ds(LANES * part, LANES)] = value[part]
        for at in range(0, wide, 32):
            lines = pl.ds(at, 32)
            right_hi[lines, :], right_lo[lines, :] = split(work[lines, :])
        freq = dot3(const(0), (right_hi[pl.ds(0, wide), :], right_lo[pl.ds(0, wide), :]), transposed=True)
        for part in range(2):
            for tile in range(2):
                flat(out_f)[pl.ds(4 * ch + 2 * part + tile, devices, stride=8), :] = freq[
                    devices * part : devices * (part + 1), LANES * tile : LANES * (tile + 1)
                ]

        @pl.when(ch == 0)
        def _():
            pl.semaphore_wait(barrier, jnp.where(me == 0, devices - 1, devices - 2))

            @pl.when(me == 0)
            def _():
                each_peer(announce)

        send_all(out_f, in_f, ch, send_f, recv_f, False)
        return carry

    lax.fori_loop(0, 2, rows_forward, 0)

    pltpu.make_async_copy(resid, resid, load_sem.at[3]).wait()
    pltpu.make_async_copy(spec, spec, load_sem.at[4]).wait()
    spec_rows = spec.reshape(spec.shape[0] * spec.shape[1], LANES)
    for ch in range(2):
        for tile in range(2):
            for top in range(low_len // LANES):
                parts = []
                for high in range(RADIX):
                    at = spec.shape[1] * ((low_len // LANES) * high + top) + RADIX * tile + ch
                    parts.append(spec_rows[pl.ds(at, 8, stride=2), :])
                spec_t[pl.ds(LANES * top, LANES), pl.ds(wide * ch + LANES * tile, LANES)] = (
                    jnp.concatenate(parts, axis=0).T * scale
                )

    @pl.when(me != 0)
    def _():
        pl.semaphore_wait(here_sem, 1)
        for ch in range(2):
            send(out_f, in_f, ch, send_f, recv_f, 0, 0)

    def columns(ch, carry):
        wait_all(in_f, ch, recv_f)
        for part in range(2):
            for tile in range(2):
                here = (pl.ds(devices * part, devices), pl.ds(LANES * tile, LANES))
                right_hi[here], right_lo[here] = split(
                    flat(in_f)[pl.ds(4 * ch + 2 * part + tile, devices, stride=8), :]
                )
        tall[...] = dot3(const(1, 2), (right_hi[pl.ds(0, wide), :], right_lo[pl.ds(0, wide), :]))
        step = 32
        for tile in range(2):
            lanes = pl.ds(LANES * tile, LANES)
            for at in range(0, low_len, step):
                lines = pl.ds(at, step)
                value = times(
                    (tall[lines, lanes], tall[pl.ds(low_len + at, step), lanes]),
                    turn_col(at, step),
                )
                for part in range(2):
                    here = (pl.ds(low_len * tile + at, step), pl.ds(LANES * part, LANES))
                    left_hi[here], left_lo[here] = split(value[part])
        tall[...] = dot3((left_hi[...], left_lo[...]), const(3))
        for tile in range(2):
            for at in range(0, low_len, step):
                weight = spec_t[pl.ds(at, step), pl.ds(pl.multiple_of(wide * ch + LANES * tile, LANES), LANES)]
                for part in range(2):
                    here = (pl.ds(low_len * tile + at, step), pl.ds(LANES * part, LANES))
                    left_hi[here], left_lo[here] = split(tall[here] * weight)
        tall[...] = dot3((left_hi[...], left_lo[...]), const(4))
        for tile in range(2):
            for at in range(0, low_len, step):
                lines = pl.ds(at, step)
                here = pl.ds(low_len * tile + at, step)
                value = times_conj(
                    (tall[here, pl.ds(0, LANES)], tall[here, pl.ds(LANES, LANES)]),
                    turn_col(at, step),
                )
                for part in range(2):
                    there = (pl.ds(low_len * part + at, step), pl.ds(LANES * tile, LANES))
                    right_hi[there], right_lo[there] = split(value[part])
        low, high = pl.ds(0, low_len), pl.ds(low_len, low_len)
        grid = dot3(const(5), (right_hi[low, :], right_lo[low, :])) + dot3(
            const(6), (right_hi[high, :], right_lo[high, :])
        )
        for part in range(2):
            for tile in range(2):
                flat(out_b)[pl.ds(4 * ch + 2 * part + tile, devices, stride=8), :] = grid[
                    devices * part : devices * (part + 1), LANES * tile : LANES * (tile + 1)
                ]
        send_all(out_b, in_b, ch, send_b, recv_b, True)
        return carry

    lax.fori_loop(0, 2, columns, 0)

    noise = noise_ref[0]
    image[...] = noise * direct[...]

    def rows_back(ch, carry):
        wait_all(in_b, ch, recv_b)
        for part in range(2):
            for tile in range(2):
                here = (pl.ds(LANES * tile, LANES), pl.ds(devices * part, devices))
                block = flat(in_b)[pl.ds(4 * ch + 2 * part + tile, devices, stride=8), :]
                left_hi[here], left_lo[here] = split(block.T)
        work[...] = dot3((left_hi[pl.ds(0, wide), :], left_lo[pl.ds(0, wide), :]), const(7))
        for top in range(2):
            values = []
            for e in range(RADIX):
                lines = pl.ds(RADIX * e + 8 * top, 8)
                values.append(
                    times_conj((work[lines, pl.ds(0, LANES)], work[lines, pl.ds(LANES, LANES)]), turn(ch, e))
                )
            lines = pl.ds(8 * top, 8)
            for a, value in enumerate(sixteen(values, 1)):
                value = times_conj(value, turn(ch, RADIX + a))
                lanes = pl.ds(LANES * a, LANES)
                for part in range(2):
                    image[part, lines, lanes] += value[part]
        return carry

    lax.fori_loop(0, 2, rows_back, 0)

    def sum_rows(value):
        return jnp.sum(value, axis=0, keepdims=True)

    lines = []
    for probe in range(2):
        totals = [jnp.zeros((8, LANES), F32) for _ in range(4)]
        for top in range(2):
            for a in range(direct.shape[2] // LANES):
                here = (probe, pl.ds(8 * top, 8), pl.ds(LANES * a, LANES))
                r, d, q = resid[here], direct[here], image[here]
                for index, term in enumerate((r * r, d * q, r * q, q * q)):
                    totals[index] += term
        lines += [sum_rows(total) for total in totals]
    stacked = jnp.sum(jnp.concatenate(lines, axis=0), axis=1, keepdims=True)
    at_row = lax.broadcasted_iota(jnp.int32, (8, LANES), 0)
    at_lane = lax.broadcasted_iota(jnp.int32, (8, LANES), 1)
    mine = sum_rows(jnp.where(at_row == at_lane, stacked, 0.0))
    sums[me] = mine

    def tell(to_row, to_sub):
        pltpu.make_async_remote_copy(
            sums.at[me], sums.at[me], send_s, recv_s,
            device_id={"row": to_row, "sub": to_sub}, device_id_type=MESH,
        ).start()

    each_peer(tell)
    for ch in range(2):
        wait_all(out_f, ch, send_f)
        wait_all(out_b, ch, send_b)
    others = sums.at[pl.ds(0, devices - 1)]
    pltpu.make_async_copy(others, others, send_s).wait()
    pltpu.make_async_copy(others, others, recv_s).wait()
    total_out[...] = jnp.sum(sums[...], axis=0)


def finish(total_ref, resid, direct, image, resid_out, dir_out, step_out):
    total = total_ref[...]
    for probe in range(2):
        old_norm, curvature, cross, square = (total[:, 4 * probe + i : 4 * probe + i + 1] for i in range(4))
        size = old_norm / curvature
        new_norm = old_norm - 2.0 * (size * cross) + size * (size * square)
        ratio = new_norm / (old_norm + TINY)
        step_out[probe] = size[0, 0]
        for a in range(direct.shape[2] // LANES):
            here = (probe, slice(None), pl.ds(LANES * a, LANES))
            value = resid[here] - size * image[here]
            resid_out[here] = value
            dir_out[here] = value + ratio * direct[here]


def body(n_row, n_sub, residual_in, direction, spectrum, noise_var):
    probes, rows_dev, grid_len = direction.shape
    devices = n_row * n_sub
    embed = 2 * grid_len
    consts, turns = tables(rows_dev, grid_len, devices)
    low_len = embed // RADIX
    wide = 2 * LANES
    slots = (devices, 8, LANES)
    vmem = pltpu.VMEM
    sems = pltpu.SemaphoreType.DMA
    block = (probes, rows_dev, grid_len)
    hbm_spec = pl.BlockSpec(memory_space=pltpu.HBM)
    vmem_spec = pl.BlockSpec(memory_space=pltpu.VMEM)
    smem_spec = pl.BlockSpec(memory_space=pltpu.SMEM)
    image, total = pl.pallas_call(
        functools.partial(kernel, n_row, n_sub, 1.0 / (embed * embed)),
        out_shape=(jax.ShapeDtypeStruct(block, F32), jax.ShapeDtypeStruct((1, LANES), F32)),
        in_specs=[smem_spec] + [hbm_spec] * 5,
        out_specs=(vmem_spec, vmem_spec),
        scratch_shapes=[
            vmem(block, F32), vmem(block, F32), vmem((embed // LANES, spectrum.shape[1], LANES), F32),
            vmem(consts.shape, BF16), vmem(turns.shape, F32),
            vmem(slots, F32), vmem(slots, F32), vmem(slots, F32), vmem(slots, F32),
            vmem((devices, 1, LANES), F32), vmem((low_len, 4 * LANES), F32),
            vmem((wide, wide), F32), vmem((2 * low_len, wide), F32),
            vmem((2 * low_len, wide), BF16), vmem((2 * low_len, wide), BF16),
            vmem((2 * low_len, wide), BF16), vmem((2 * low_len, wide), BF16),
            sems((5,)), sems((2,)), sems((2,)), sems((2,)), sems((2,)), sems, sems, pltpu.SemaphoreType.REGULAR,
        ],
        compiler_params=pltpu.CompilerParams(
            collective_id=0, has_side_effects=True, vmem_limit_bytes=VMEM_LIMIT
        ),
        name="cg_step",
    )(noise_var, residual_in, direction, spectrum.T, *(jnp.asarray(t) for t in (consts, turns)))
    return pl.pallas_call(
        finish,
        out_shape=(
            jax.ShapeDtypeStruct(block, F32),
            jax.ShapeDtypeStruct(block, F32),
            jax.ShapeDtypeStruct((probes,), F32),
        ),
        in_specs=[vmem_spec] * 4,
        out_specs=(vmem_spec, vmem_spec, smem_spec),
        compiler_params=pltpu.CompilerParams(vmem_limit_bytes=8 << 20),
        name="finish",
    )(total, residual_in, direction, image)


def solution(mesh):
    in_specs = (P("grp", ROW_SUB, None), P("grp", ROW_SUB, None), P("grp", ROW_SUB), P("grp"))
    out_specs = (P("grp", ROW_SUB, None), P("grp", ROW_SUB, None), P("grp"))
    return jax.shard_map(
        functools.partial(body, mesh.shape["row"], mesh.shape["sub"]),
        mesh=mesh, in_specs=in_specs, out_specs=out_specs, check_vma=False,
    )
```

```python
import functools
import math

import jax
import jax.numpy as jnp
import ml_dtypes
import numpy as np
from jax import lax
from jax.experimental import pallas as pl
from jax.experimental.pallas import tpu as pltpu
from jax.sharding import PartitionSpec as P

ROW_SUB = ("row", "sub")
MESH = pl.DeviceIdType.MESH
TINY = 1e-06
VMEM_LIMIT = 107 << 19
LANES = 128
RADIX = 16
F32 = jnp.float32
BF16 = jnp.bfloat16


def roots(left, right, modulus, sign):
    turns = np.mod(np.outer(left, right), modulus)
    return np.exp(sign * 2j * np.pi * turns / modulus)


def real_form(table):
    return np.block([[table.real, -table.imag], [table.imag, table.real]])


def halves(table):
    high = table.astype(ml_dtypes.bfloat16)
    low = (table - high.astype(np.float64)).astype(ml_dtypes.bfloat16)
    return np.stack([high, low])


def tables(rows_dev, grid_len, devices):
    embed = 2 * grid_len
    lane_ids = np.arange(LANES)
    dev_ids = np.arange(devices)
    block = LANES // RADIX
    long_row = real_form(roots(dev_ids, lane_ids, LANES, -1))
    low_ids = np.arange(embed // RADIX)
    long_col = real_form(roots(low_ids, dev_ids, embed // RADIX, -1))
    short = roots(np.arange(RADIX), np.arange(RADIX), RADIX, -1)
    mixed = np.zeros((block, RADIX, RADIX, block), complex)
    for e in range(block):
        mixed[e, :, :, e] = short
    mixed = mixed.reshape(LANES, LANES)
    short_col = real_form(mixed.T).T
    short_back = real_form(np.conj(mixed)).T
    long_back = real_form(np.conj(roots(dev_ids, low_ids, embed // RADIX, -1)))
    half = long_back.shape[1] // 2
    row_back = real_form(np.conj(roots(lane_ids, dev_ids, LANES, -1))).T
    stacked = np.concatenate(
        [long_row, long_col, short_col, short_back, long_back[:, :half], long_back[:, half:], row_back], axis=0
    )
    consts = halves(stacked)
    turn_col = np.tile(roots(low_ids, np.arange(RADIX), embed, -1), (1, block))
    turn_col = np.stack([turn_col.real, turn_col.imag]).astype(np.float32)
    turn_row = np.zeros((2, 2 * RADIX, 2, LANES))
    for ch in range(2):
        for e in range(RADIX):
            turn = roots([2 * e + ch], lane_ids, embed, -1)[0]
            turn_row[ch, e] = [turn.real, turn.imag]
            odd = np.exp(-2j * np.pi * e * ch / (2 * RADIX))
            turn_row[ch, RADIX + e, 0] = odd.real
            turn_row[ch, RADIX + e, 1] = odd.imag
    turns = np.concatenate([turn_row.reshape(-1, LANES), turn_col.reshape(-1, LANES)]).astype(np.float32)
    return consts, turns


def add(x, y):
    return (x[0] + y[0], x[1] + y[1])


def sub(x, y):
    return (x[0] - y[0], x[1] - y[1])


def times(x, y):
    return (x[0] * y[0] - x[1] * y[1], x[0] * y[1] + x[1] * y[0])


def times_conj(x, y):
    return (x[0] * y[0] + x[1] * y[1], x[1] * y[0] - x[0] * y[1])


def by_root(x, power, sign):
    power %= RADIX
    if power == 0:
        return x
    if power == 4:
        return (x[1], -x[0]) if sign < 0 else (-x[1], x[0])
    if power == 8:
        return (-x[0], -x[1])
    angle = sign * 2.0 * math.pi * power / RADIX
    return times(x, (math.cos(angle), math.sin(angle)))


def four(x, sign):
    even, odd = add(x[0], x[2]), sub(x[0], x[2])
    both, diff = add(x[1], x[3]), sub(x[1], x[3])
    turned = (diff[1], -diff[0]) if sign < 0 else (-diff[1], diff[0])
    return [add(even, both), add(odd, turned), sub(even, both), sub(odd, turned)]


def sixteen(x, sign):
    inner = [four([x[4 * i + j] for i in range(4)], sign) for j in range(4)]
    out = [None] * RADIX
    for first in range(4):
        column = [by_root(inner[j][first], j * first, sign) for j in range(4)]
        for second, value in enumerate(four(column, sign)):
            out[first + 4 * second] = value
    return out


def split(value):
    high = value.astype(BF16)
    return high, (value - high.astype(F32)).astype(BF16)


def dot(left, right, transposed=False):
    dims = (((1,), (1 if transposed else 0,)), ((), ()))
    return lax.dot_general(left, right, dims, preferred_element_type=F32)


def dot3(left, right, transposed=False):
    return (
        dot(left[1], right[0], transposed) + dot(left[0], right[1], transposed) + dot(left[0], right[0], transposed)
    )


def outward(count):
    return [count // 2 + (1 - 2 * (t % 2)) * ((t + 1) // 2) for t in range(count)]


def kernel(
    n_row, n_sub, scale,
    noise_ref, resid_hbm, dir_hbm, spec_hbm, consts_hbm, turns_hbm,
    image, total_out,
    resid, direct, spec, consts, turns,
    out_f, in_f, out_b, in_b, sums, spec_t,
    work, tall, left_hi, left_lo, right_hi, right_lo,
    load_sem, send_f, recv_f, send_b, recv_b, send_s, recv_s, here_sem,
):
    devices = n_row * n_sub
    row, sub_ = lax.axis_index("row"), lax.axis_index("sub")
    me = row * n_sub + sub_
    wide = 2 * LANES
    low_len = tall.shape[0] // 2

    def load(src, dst, slot):
        copy = pltpu.make_async_copy(src, dst, load_sem.at[slot])
        copy.start()
        return copy

    def wrap(value, count):
        return jnp.where(value >= count, value - count, value)

    rows = [wrap(row + i, n_row) for i in outward(n_row)]

    def each_peer(act):
        def one_sub(t, carry):
            to_sub = wrap(sub_ + n_sub // 2 + (1 - 2 * (t % 2)) * ((t + 1) // 2), n_sub)
            for to_row in rows:
                act(to_row, to_sub)
            return carry

        lax.fori_loop(0, n_sub - 1, one_sub, 0)
        for to_row in rows[:-1]:
            act(to_row, sub_)

    loads = [load(dir_hbm, direct, 0), load(turns_hbm, turns, 1), load(consts_hbm, consts, 2)]
    barrier = pltpu.get_barrier_semaphore()

    def greet(to_row, to_sub):
        pl.semaphore_signal(barrier, inc=1, device_id={"row": to_row, "sub": to_sub}, device_id_type=MESH)

    def announce(to_row, to_sub):
        pl.semaphore_signal(here_sem, inc=1, device_id={"row": to_row, "sub": to_sub}, device_id_type=MESH)

    @pl.when(me != 0)
    def _():
        each_peer(greet)

    load(resid_hbm, resid, 3)
    for t in range(spec.shape[0]):
        load(spec_hbm.at[:, pl.ds(LANES * t, LANES)], spec.at[t], 4)

    def const(index, count=1):
        rows = pl.ds(wide * index, wide * count)
        return consts[0, rows, :], consts[1, rows, :]

    def lines_of(piece):
        return pl.ds(2 * piece, 4 if isinstance(piece, int) and piece == 2 else 2)

    def send(src, dst, piece, send_sem, recv_sem, to_row, to_sub):
        pltpu.make_async_remote_copy(
            src.at[to_row * n_sub + to_sub, lines_of(piece)],
            dst.at[me, lines_of(piece)],
            send_sem.at[piece],
            recv_sem.at[piece],
            device_id={"row": to_row, "sub": to_sub},
            device_id_type=MESH,
        ).start()

    def send_all(src, dst, piece, send_sem, recv_sem, all_here):
        def act(to_row, to_sub):
            go = functools.partial(send, src, dst, piece, send_sem, recv_sem, to_row, to_sub)
            if all_here:
                go()
            else:
                pl.when(to_row + to_sub != 0)(go)

        each_peer(act)
        dst[me, lines_of(piece)] = src[me, lines_of(piece)]

    def wait_all(ref, piece, sem):
        others = ref.at[pl.ds(0, devices - 1), lines_of(piece)]
        pltpu.make_async_copy(others, others, sem.at[piece]).wait()

    def flat(ref):
        return ref.reshape(devices * 8, LANES)

    def turn(ch, index):
        both = turns[pl.ds(4 * RADIX * ch + 2 * index, 2), :]
        return both[0:1], both[1:2]

    def turn_col(at, step):
        first = 8 * RADIX + at
        return turns[pl.ds(first, step), :], turns[pl.ds(first + low_len, step), :]

    for copy in loads:
        copy.wait()

    def rows_forward(ch):
        for top in range(2):
            lines = pl.ds(8 * top, 8)
            values = []
            for a in range(RADIX):
                lanes = pl.ds(LANES * a, LANES)
                values.append(times((direct[0, lines, lanes], direct[1, lines, lanes]), turn(ch, RADIX + a)))
            for e, value in enumerate(sixteen(values, -1)):
                value = times(value, turn(ch, e))
                for part in range(2):
                    work[pl.ds(RADIX * e + 8 * top, 8), pl.ds(LANES * part, LANES)] = value[part]
        for at in range(0, wide, 32):
            lines = pl.ds(at, 32)
            right_hi[lines, :], right_lo[lines, :] = split(work[lines, :])
        freq = dot3(const(0), (right_hi[pl.ds(0, wide), :], right_lo[pl.ds(0, wide), :]), transposed=True)
        for part in range(2):
            for tile in range(2):
                flat(out_f)[pl.ds(4 * ch + 2 * tile + part, devices, stride=8), :] = freq[
                    devices * part : devices * (part + 1), LANES * tile : LANES * (tile + 1)
                ]

    rows_forward(0)
    pl.semaphore_wait(barrier, jnp.where(me == 0, devices - 1, devices - 2))

    @pl.when(me == 0)
    def _():
        each_peer(announce)

    lax.fori_loop(0, 2, lambda piece, carry: (send_all(out_f, in_f, piece, send_f, recv_f, False), carry)[1], 0)
    rows_forward(1)
    send_all(out_f, in_f, 2, send_f, recv_f, False)

    pltpu.make_async_copy(resid, resid, load_sem.at[3]).wait()
    pltpu.make_async_copy(spec, spec, load_sem.at[4]).wait()
    spec_rows = spec.reshape(spec.shape[0] * spec.shape[1], LANES)
    for ch in range(2):
        for tile in range(2):
            for top in range(low_len // LANES):
                parts = []
                for high in range(RADIX):
                    at = spec.shape[1] * ((low_len // LANES) * high + top) + RADIX * tile + ch
                    parts.append(spec_rows[pl.ds(at, 8, stride=2), :])
                spec_t[pl.ds(LANES * top, LANES), pl.ds(wide * ch + LANES * tile, LANES)] = (
                    jnp.concatenate(parts, axis=0).T * scale
                )

    @pl.when(me != 0)
    def _():
        pl.semaphore_wait(here_sem, 1)
        for piece in range(3):
            send(out_f, in_f, piece, send_f, recv_f, 0, 0)

    def columns(ch, piece, first_tile, tiles):
        wait_all(in_f, piece, recv_f)
        width = LANES * tiles
        count = low_len * tiles
        step = 32
        for part in range(2):
            for tile in range(tiles):
                here = (pl.ds(devices * part, devices), pl.ds(LANES * tile, LANES))
                right_hi[here], right_lo[here] = split(
                    flat(in_f)[pl.ds(4 * ch + 2 * (first_tile + tile) + part, devices, stride=8), :]
                )
        operand = (pl.ds(0, wide), pl.ds(0, width))
        tall[:, pl.ds(0, width)] = dot3(const(1, 2), (right_hi[operand], right_lo[operand]))
        for tile in range(tiles):
            lanes = pl.ds(LANES * tile, LANES)
            for at in range(0, low_len, step):
                lines = pl.ds(at, step)
                value = times((tall[lines, lanes], tall[pl.ds(low_len + at, step), lanes]), turn_col(at, step))
                for part in range(2):
                    here = (pl.ds(low_len * tile + at, step), pl.ds(LANES * part, LANES))
                    left_hi[here], left_lo[here] = split(value[part])
        used = pl.ds(0, count)
        tall[used, :] = dot3((left_hi[used, :], left_lo[used, :]), const(3))
        for tile in range(tiles):
            lanes = pl.ds(pl.multiple_of(wide * ch + LANES * (first_tile + tile), LANES), LANES)
            for at in range(0, low_len, step):
                weight = spec_t[pl.ds(at, step), lanes]
                for part in range(2):
                    here = (pl.ds(low_len * tile + at, step), pl.ds(LANES * part, LANES))
                    left_hi[here], left_lo[here] = split(tall[here] * weight)
        tall[used, :] = dot3((left_hi[used, :], left_lo[used, :]), const(4))
        for tile in range(tiles):
            for at in range(0, low_len, step):
                here = pl.ds(low_len * tile + at, step)
                value = times_conj((tall[here, pl.ds(0, LANES)], tall[here, pl.ds(LANES, LANES)]), turn_col(at, step))
                for part in range(2):
                    there = (pl.ds(low_len * part + at, step), pl.ds(LANES * tile, LANES))
                    right_hi[there], right_lo[there] = split(value[part])
        low, high = (pl.ds(0, low_len), pl.ds(0, width)), (pl.ds(low_len, low_len), pl.ds(0, width))
        grid = dot3(const(5), (right_hi[low], right_lo[low])) + dot3(const(6), (right_hi[high], right_lo[high]))
        for part in range(2):
            for tile in range(tiles):
                flat(out_b)[pl.ds(4 * ch + 2 * (first_tile + tile) + part, devices, stride=8), :] = grid[
                    devices * part : devices * (part + 1), LANES * tile : LANES * (tile + 1)
                ]
        send_all(out_b, in_b, piece, send_b, recv_b, True)

    lax.fori_loop(0, 2, lambda piece, carry: (columns(0, piece, piece, 1), carry)[1], 0)
    columns(1, 2, 0, 2)

    noise = noise_ref[0]
    image[...] = noise * direct[...]

    def rows_back(ch):
        for piece in ((0, 1), (2,))[ch]:
            wait_all(in_b, piece, recv_b)
        for part in range(2):
            for tile in range(2):
                here = (pl.ds(LANES * tile, LANES), pl.ds(devices * part, devices))
                block = flat(in_b)[pl.ds(4 * ch + 2 * tile + part, devices, stride=8), :]
                left_hi[here], left_lo[here] = split(block.T)
        work[...] = dot3((left_hi[pl.ds(0, wide), :], left_lo[pl.ds(0, wide), :]), const(7))
        for top in range(2):
            values = []
            for e in range(RADIX):
                lines = pl.ds(RADIX * e + 8 * top, 8)
                values.append(
                    times_conj((work[lines, pl.ds(0, LANES)], work[lines, pl.ds(LANES, LANES)]), turn(ch, e))
                )
            lines = pl.ds(8 * top, 8)
            for a, value in enumerate(sixteen(values, 1)):
                value = times_conj(value, turn(ch, RADIX + a))
                lanes = pl.ds(LANES * a, LANES)
                for part in range(2):
                    image[part, lines, lanes] += value[part]

    rows_back(0)
    rows_back(1)

    def sum_rows(value):
        return jnp.sum(value, axis=0, keepdims=True)

    lines = []
    for probe in range(2):
        totals = [jnp.zeros((8, LANES), F32) for _ in range(4)]
        for top in range(2):
            for a in range(direct.shape[2] // LANES):
                here = (probe, pl.ds(8 * top, 8), pl.ds(LANES * a, LANES))
                r, d, q = resid[here], direct[here], image[here]
                for index, term in enumerate((r * r, d * q, r * q, q * q)):
                    totals[index] += term
        lines += [sum_rows(total) for total in totals]
    stacked = jnp.sum(jnp.concatenate(lines, axis=0), axis=1, keepdims=True)
    at_row = lax.broadcasted_iota(jnp.int32, (8, LANES), 0)
    at_lane = lax.broadcasted_iota(jnp.int32, (8, LANES), 1)
    mine = sum_rows(jnp.where(at_row == at_lane, stacked, 0.0))
    sums[me] = mine

    def tell(to_row, to_sub):
        pltpu.make_async_remote_copy(
            sums.at[me], sums.at[me], send_s, recv_s,
            device_id={"row": to_row, "sub": to_sub}, device_id_type=MESH,
        ).start()

    each_peer(tell)
    for piece in range(3):
        wait_all(out_f, piece, send_f)
        wait_all(out_b, piece, send_b)
    others = sums.at[pl.ds(0, devices - 1)]
    pltpu.make_async_copy(others, others, send_s).wait()
    pltpu.make_async_copy(others, others, recv_s).wait()
    total_out[...] = jnp.sum(sums[...], axis=0)


def finish(total_ref, resid, direct, image, resid_out, dir_out, step_out):
    total = total_ref[...]
    for probe in range(2):
        old_norm, curvature, cross, square = (total[:, 4 * probe + i : 4 * probe + i + 1] for i in range(4))
        size = old_norm / curvature
        new_norm = old_norm - 2.0 * (size * cross) + size * (size * square)
        ratio = new_norm / (old_norm + TINY)
        step_out[probe] = size[0, 0]
        for a in range(direct.shape[2] // LANES):
            here = (probe, slice(None), pl.ds(LANES * a, LANES))
            value = resid[here] - size * image[here]
            resid_out[here] = value
            dir_out[here] = value + ratio * direct[here]


def body(n_row, n_sub, residual_in, direction, spectrum, noise_var):
    probes, rows_dev, grid_len = direction.shape
    devices = n_row * n_sub
    embed = 2 * grid_len
    consts, turns = tables(rows_dev, grid_len, devices)
    low_len = embed // RADIX
    wide = 2 * LANES
    slots = (devices, 8, LANES)
    vmem = pltpu.VMEM
    sems = pltpu.SemaphoreType.DMA
    block = (probes, rows_dev, grid_len)
    hbm_spec = pl.BlockSpec(memory_space=pltpu.HBM)
    vmem_spec = pl.BlockSpec(memory_space=pltpu.VMEM)
    smem_spec = pl.BlockSpec(memory_space=pltpu.SMEM)
    image, total = pl.pallas_call(
        functools.partial(kernel, n_row, n_sub, 1.0 / (embed * embed)),
        out_shape=(jax.ShapeDtypeStruct(block, F32), jax.ShapeDtypeStruct((1, LANES), F32)),
        in_specs=[smem_spec] + [hbm_spec] * 5,
        out_specs=(vmem_spec, vmem_spec),
        scratch_shapes=[
            vmem(block, F32), vmem(block, F32), vmem((embed // LANES, spectrum.shape[1], LANES), F32),
            vmem(consts.shape, BF16), vmem(turns.shape, F32),
            vmem(slots, F32), vmem(slots, F32), vmem(slots, F32), vmem(slots, F32),
            vmem((devices, 1, LANES), F32), vmem((low_len, 4 * LANES), F32),
            vmem((wide, wide), F32), vmem((2 * low_len, wide), F32),
            vmem((2 * low_len, wide), BF16), vmem((2 * low_len, wide), BF16),
            vmem((2 * low_len, wide), BF16), vmem((2 * low_len, wide), BF16),
            sems((5,)), sems((3,)), sems((3,)), sems((3,)), sems((3,)), sems, sems, pltpu.SemaphoreType.REGULAR,
        ],
        compiler_params=pltpu.CompilerParams(
            collective_id=0, has_side_effects=True, vmem_limit_bytes=VMEM_LIMIT
        ),
        name="cg_step",
    )(noise_var, residual_in, direction, spectrum.T, *(jnp.asarray(t) for t in (consts, turns)))
    return pl.pallas_call(
        finish,
        out_shape=(
            jax.ShapeDtypeStruct(block, F32),
            jax.ShapeDtypeStruct(block, F32),
            jax.ShapeDtypeStruct((probes,), F32),
        ),
        in_specs=[vmem_spec] * 4,
        out_specs=(vmem_spec, vmem_spec, smem_spec),
        compiler_params=pltpu.CompilerParams(vmem_limit_bytes=8 << 20),
        name="finish",
    )(total, residual_in, direction, image)


def solution(mesh):
    in_specs = (P("grp", ROW_SUB, None), P("grp", ROW_SUB, None), P("grp", ROW_SUB), P("grp"))
    out_specs = (P("grp", ROW_SUB, None), P("grp", ROW_SUB, None), P("grp"))
    return jax.shard_map(
        functools.partial(body, mesh.shape["row"], mesh.shape["sub"]),
        mesh=mesh, in_specs=in_specs, out_specs=out_specs, check_vma=False,
    )
```

```python
import functools
import math

import jax
import jax.numpy as jnp
import ml_dtypes
import numpy as np
from jax import lax
from jax.experimental import pallas as pl
from jax.experimental.pallas import tpu as pltpu
from jax.sharding import PartitionSpec as P

ROW_SUB = ("row", "sub")
MESH = pl.DeviceIdType.MESH
TINY = 1e-06
VMEM_LIMIT = 107 << 19
LANES = 128
RADIX = 16
F32 = jnp.float32
BF16 = jnp.bfloat16


def roots(left, right, modulus, sign):
    turns = np.mod(np.outer(left, right), modulus)
    return np.exp(sign * 2j * np.pi * turns / modulus)


def real_form(table):
    return np.block([[table.real, -table.imag], [table.imag, table.real]])


def halves(table):
    high = table.astype(ml_dtypes.bfloat16)
    low = (table - high.astype(np.float64)).astype(ml_dtypes.bfloat16)
    return np.stack([high, low])


def tables(rows_dev, grid_len, devices):
    embed = 2 * grid_len
    lane_ids = np.arange(LANES)
    dev_ids = np.arange(devices)
    block = LANES // RADIX
    long_row = real_form(roots(dev_ids, lane_ids, LANES, -1))
    low_ids = np.arange(embed // RADIX)
    long_col = real_form(roots(low_ids, dev_ids, embed // RADIX, -1))
    short = roots(np.arange(RADIX), np.arange(RADIX), RADIX, -1)
    mixed = np.zeros((block, RADIX, RADIX, block), complex)
    for e in range(block):
        mixed[e, :, :, e] = short
    mixed = mixed.reshape(LANES, LANES)
    short_col = real_form(mixed.T).T
    short_back = real_form(np.conj(mixed)).T
    long_back = real_form(np.conj(roots(dev_ids, low_ids, embed // RADIX, -1)))
    half = long_back.shape[1] // 2
    row_back = real_form(np.conj(roots(lane_ids, dev_ids, LANES, -1))).T
    stacked = np.concatenate(
        [long_row, long_col, short_col, short_back, long_back[:, :half], long_back[:, half:], row_back], axis=0
    )
    consts = halves(stacked)
    turn_col = np.tile(roots(low_ids, np.arange(RADIX), embed, -1), (1, block))
    turn_col = np.stack([turn_col.real, turn_col.imag]).astype(np.float32)
    turn_row = np.zeros((2, 2 * RADIX, 2, LANES))
    for ch in range(2):
        for e in range(RADIX):
            turn = roots([2 * e + ch], lane_ids, embed, -1)[0]
            turn_row[ch, e] = [turn.real, turn.imag]
            odd = np.exp(-2j * np.pi * e * ch / (2 * RADIX))
            turn_row[ch, RADIX + e, 0] = odd.real
            turn_row[ch, RADIX + e, 1] = odd.imag
    turns = np.concatenate([turn_row.reshape(-1, LANES), turn_col.reshape(-1, LANES)]).astype(np.float32)
    return consts, turns


def add(x, y):
    return (x[0] + y[0], x[1] + y[1])


def sub(x, y):
    return (x[0] - y[0], x[1] - y[1])


def times(x, y):
    return (x[0] * y[0] - x[1] * y[1], x[0] * y[1] + x[1] * y[0])


def times_conj(x, y):
    return (x[0] * y[0] + x[1] * y[1], x[1] * y[0] - x[0] * y[1])


def by_root(x, power, sign):
    power %= RADIX
    if power == 0:
        return x
    if power == 4:
        return (x[1], -x[0]) if sign < 0 else (-x[1], x[0])
    if power == 8:
        return (-x[0], -x[1])
    angle = sign * 2.0 * math.pi * power / RADIX
    return times(x, (math.cos(angle), math.sin(angle)))


def four(x, sign):
    even, odd = add(x[0], x[2]), sub(x[0], x[2])
    both, diff = add(x[1], x[3]), sub(x[1], x[3])
    turned = (diff[1], -diff[0]) if sign < 0 else (-diff[1], diff[0])
    return [add(even, both), add(odd, turned), sub(even, both), sub(odd, turned)]


def sixteen(x, sign):
    inner = [four([x[4 * i + j] for i in range(4)], sign) for j in range(4)]
    out = [None] * RADIX
    for first in range(4):
        column = [by_root(inner[j][first], j * first, sign) for j in range(4)]
        for second, value in enumerate(four(column, sign)):
            out[first + 4 * second] = value
    return out


def split(value):
    high = value.astype(BF16)
    return high, (value - high.astype(F32)).astype(BF16)


def dot(left, right, transposed=False):
    dims = (((1,), (1 if transposed else 0,)), ((), ()))
    return lax.dot_general(left, right, dims, preferred_element_type=F32)


def dot3(left, right, transposed=False):
    return (
        dot(left[1], right[0], transposed) + dot(left[0], right[1], transposed) + dot(left[0], right[0], transposed)
    )


def far_first(n_row, n_sub):
    def chips(row, sub_):
        hop = row // 2
        return min(hop, n_row // 2 - hop) + min(sub_, n_sub - sub_)

    offsets = [(i, j) for i in range(n_row) for j in range(n_sub)][1:]
    return sorted(offsets, key=lambda pair: -chips(*pair))


def outward(count):
    return [count // 2 + (1 - 2 * (t % 2)) * ((t + 1) // 2) for t in range(count)]


def kernel(
    n_row, n_sub, scale,
    noise_ref, resid_hbm, dir_hbm, spec_hbm, consts_hbm, turns_hbm,
    image, total_out,
    resid, direct, spec, consts, turns,
    out_f, in_f, out_b, in_b, sums, spec_t,
    work, tall, left_hi, left_lo, right_hi, right_lo,
    load_sem, send_f, recv_f, send_b, recv_b, send_s, recv_s, here_sem,
):
    devices = n_row * n_sub
    row, sub_ = lax.axis_index("row"), lax.axis_index("sub")
    me = row * n_sub + sub_
    offsets = far_first(n_row, n_sub)
    wide = 2 * LANES
    low_len = tall.shape[0] // 2

    def load(src, dst, slot):
        copy = pltpu.make_async_copy(src, dst, load_sem.at[slot])
        copy.start()
        return copy

    def wrap(value, count):
        return jnp.where(value >= count, value - count, value)

    def peer(i, j):
        return wrap(row + i, n_row), wrap(sub_ + j, n_sub)

    subs = [wrap(sub_ + j, n_sub) for j in outward(n_sub)]
    rows = [wrap(row + i, n_row) for i in outward(n_row)]
    late = me == 0
    level = jnp.where(late, n_sub, sub_)

    def each_peer(act):
        def one_row(t, carry):
            half = n_row // 2
            to_row = wrap(row + half + (1 - 2 * (t % 2)) * ((t + 1) // 2), n_row)
            for to_sub in subs:
                act(to_row, to_sub)
            return carry

        lax.fori_loop(0, n_row - 1, one_row, 0)
        for to_sub in subs[:-1]:
            act(row, to_sub)

    loads = [load(dir_hbm, direct, 0), load(turns_hbm, turns, 1), load(consts_hbm, consts, 2)]
    barrier = pltpu.get_barrier_semaphore()

    def greet(to_row, to_sub):
        pl.semaphore_signal(barrier, inc=1, device_id={"row": to_row, "sub": to_sub}, device_id_type=MESH)

    def announce(to_row, to_sub):
        pl.semaphore_signal(here_sem.at[level], inc=1, device_id={"row": to_row, "sub": to_sub}, device_id_type=MESH)

    def greet_sub(to_sub, carry):
        @pl.when(to_sub > sub_)
        def _():
            for to_row in rows:
                greet(to_row, to_sub)

        return carry

    @pl.when(jnp.logical_not(late))
    def _():
        for to_row in rows[:-1]:
            greet(to_row, sub_)
        lax.fori_loop(1, n_sub, greet_sub, 0)
        pl.when(sub_ != 0)(lambda: greet(0, 0))

    load(resid_hbm, resid, 3)
    for t in range(spec.shape[0]):
        load(spec_hbm.at[:, pl.ds(LANES * t, LANES)], spec.at[t], 4)

    def const(index, count=1):
        rows = pl.ds(wide * index, wide * count)
        return consts[0, rows, :], consts[1, rows, :]

    def send(src, dst, ch, send_sem, recv_sem, to_row, to_sub):
        part = pl.ds(4 * ch, 4)
        pltpu.make_async_remote_copy(
            src.at[to_row * n_sub + to_sub, part],
            dst.at[me, part],
            send_sem.at[ch],
            recv_sem.at[ch],
            device_id={"row": to_row, "sub": to_sub},
            device_id_type=MESH,
        ).start()

    def send_all(src, dst, ch, send_sem, recv_sem, all_here):
        for i, j in offsets:
            to_row, to_sub = peer(i, j)
            go = functools.partial(send, src, dst, ch, send_sem, recv_sem, to_row, to_sub)
            if all_here:
                go()
            else:
                pl.when((to_row + to_sub != 0) & (to_sub <= level))(go)
        part = pl.ds(4 * ch, 4)
        dst[me, part] = src[me, part]

    def wait_all(ref, ch, sem):
        others = ref.at[pl.ds(0, devices - 1), pl.ds(4 * ch, 4)]
        pltpu.make_async_copy(others, others, sem.at[ch]).wait()

    def flat(ref):
        return ref.reshape(devices * 8, LANES)

    def turn(ch, index):
        both = turns[pl.ds(4 * RADIX * ch + 2 * index, 2), :]
        return both[0:1], both[1:2]

    def turn_col(at, step):
        first = 8 * RADIX + at
        return turns[pl.ds(first, step), :], turns[pl.ds(first + low_len, step), :]

    for copy in loads:
        copy.wait()

    def rows_forward(ch, carry):
        for top in range(2):
            lines = pl.ds(8 * top, 8)
            values = []
            for a in range(RADIX):
                lanes = pl.ds(LANES * a, LANES)
                values.append(times((direct[0, lines, lanes], direct[1, lines, lanes]), turn(ch, RADIX + a)))
            for e, value in enumerate(sixteen(values, -1)):
                value = times(value, turn(ch, e))
                for part in range(2):
                    work[pl.ds(RADIX * e + 8 * top, 8), pl.ds(LANES * part, LANES)] = value[part]
        for at in range(0, wide, 32):
            lines = pl.ds(at, 32)
            right_hi[lines, :], right_lo[lines, :] = split(work[lines, :])
        freq = dot3(const(0), (right_hi[pl.ds(0, wide), :], right_lo[pl.ds(0, wide), :]), transposed=True)
        for part in range(2):
            for tile in range(2):
                flat(out_f)[pl.ds(4 * ch + 2 * part + tile, devices, stride=8), :] = freq[
                    devices * part : devices * (part + 1), LANES * tile : LANES * (tile + 1)
                ]

        @pl.when(ch == 0)
        def _():
            pl.semaphore_wait(barrier, jnp.where(late, devices - 1, n_row * (sub_ + 1) - 2))
            pl.when(late)(lambda: each_peer(announce))

            @pl.when(jnp.logical_not(late))
            def _():
                for to_sub in range(n_sub):
                    pl.when((to_sub < sub_) & (row + to_sub != 0))(functools.partial(announce, row, to_sub))

        send_all(out_f, in_f, ch, send_f, recv_f, False)
        return carry

    lax.fori_loop(0, 2, rows_forward, 0)

    pltpu.make_async_copy(resid, resid, load_sem.at[3]).wait()
    pltpu.make_async_copy(spec, spec, load_sem.at[4]).wait()
    spec_rows = spec.reshape(spec.shape[0] * spec.shape[1], LANES)
    for ch in range(2):
        for tile in range(2):
            for top in range(low_len // LANES):
                parts = []
                for high in range(RADIX):
                    at = spec.shape[1] * ((low_len // LANES) * high + top) + RADIX * tile + ch
                    parts.append(spec_rows[pl.ds(at, 8, stride=2), :])
                spec_t[pl.ds(LANES * top, LANES), pl.ds(wide * ch + LANES * tile, LANES)] = (
                    jnp.concatenate(parts, axis=0).T * scale
                )

    def later_class(t, carry):
        ch, to_sub = t // n_sub, t % n_sub

        @pl.when(to_sub > level)
        def _():
            pl.when(ch == 0)(lambda: pl.semaphore_wait(here_sem.at[to_sub], 1))
            for to_row in rows:
                send(out_f, in_f, ch, send_f, recv_f, to_row, to_sub)

        return carry

    lax.fori_loop(0, 2 * n_sub, later_class, 0)

    @pl.when(jnp.logical_not(late))
    def _():
        pl.semaphore_wait(here_sem.at[n_sub], 1)
        for ch in range(2):
            send(out_f, in_f, ch, send_f, recv_f, 0, 0)

    def columns(ch, carry):
        wait_all(in_f, ch, recv_f)
        for part in range(2):
            for tile in range(2):
                here = (pl.ds(devices * part, devices), pl.ds(LANES * tile, LANES))
                right_hi[here], right_lo[here] = split(
                    flat(in_f)[pl.ds(4 * ch + 2 * part + tile, devices, stride=8), :]
                )
        tall[...] = dot3(const(1, 2), (right_hi[pl.ds(0, wide), :], right_lo[pl.ds(0, wide), :]))
        step = 32
        for tile in range(2):
            lanes = pl.ds(LANES * tile, LANES)
            for at in range(0, low_len, step):
                lines = pl.ds(at, step)
                value = times(
                    (tall[lines, lanes], tall[pl.ds(low_len + at, step), lanes]),
                    turn_col(at, step),
                )
                for part in range(2):
                    here = (pl.ds(low_len * tile + at, step), pl.ds(LANES * part, LANES))
                    left_hi[here], left_lo[here] = split(value[part])
        tall[...] = dot3((left_hi[...], left_lo[...]), const(3))
        for tile in range(2):
            for at in range(0, low_len, step):
                weight = spec_t[pl.ds(at, step), pl.ds(pl.multiple_of(wide * ch + LANES * tile, LANES), LANES)]
                for part in range(2):
                    here = (pl.ds(low_len * tile + at, step), pl.ds(LANES * part, LANES))
                    left_hi[here], left_lo[here] = split(tall[here] * weight)
        tall[...] = dot3((left_hi[...], left_lo[...]), const(4))
        for tile in range(2):
            for at in range(0, low_len, step):
                lines = pl.ds(at, step)
                here = pl.ds(low_len * tile + at, step)
                value = times_conj(
                    (tall[here, pl.ds(0, LANES)], tall[here, pl.ds(LANES, LANES)]),
                    turn_col(at, step),
                )
                for part in range(2):
                    there = (pl.ds(low_len * part + at, step), pl.ds(LANES * tile, LANES))
                    right_hi[there], right_lo[there] = split(value[part])
        low, high = pl.ds(0, low_len), pl.ds(low_len, low_len)
        grid = dot3(const(5), (right_hi[low, :], right_lo[low, :])) + dot3(
            const(6), (right_hi[high, :], right_lo[high, :])
        )
        for part in range(2):
            for tile in range(2):
                flat(out_b)[pl.ds(4 * ch + 2 * part + tile, devices, stride=8), :] = grid[
                    devices * part : devices * (part + 1), LANES * tile : LANES * (tile + 1)
                ]
        send_all(out_b, in_b, ch, send_b, recv_b, True)
        return carry

    lax.fori_loop(0, 2, columns, 0)

    noise = noise_ref[0]
    image[...] = noise * direct[...]

    def rows_back(ch, carry):
        wait_all(in_b, ch, recv_b)
        for part in range(2):
            for tile in range(2):
                here = (pl.ds(LANES * tile, LANES), pl.ds(devices * part, devices))
                block = flat(in_b)[pl.ds(4 * ch + 2 * part + tile, devices, stride=8), :]
                left_hi[here], left_lo[here] = split(block.T)
        work[...] = dot3((left_hi[pl.ds(0, wide), :], left_lo[pl.ds(0, wide), :]), const(7))
        for top in range(2):
            values = []
            for e in range(RADIX):
                lines = pl.ds(RADIX * e + 8 * top, 8)
                values.append(
                    times_conj((work[lines, pl.ds(0, LANES)], work[lines, pl.ds(LANES, LANES)]), turn(ch, e))
                )
            lines = pl.ds(8 * top, 8)
            for a, value in enumerate(sixteen(values, 1)):
                value = times_conj(value, turn(ch, RADIX + a))
                lanes = pl.ds(LANES * a, LANES)
                for part in range(2):
                    image[part, lines, lanes] += value[part]
        return carry

    lax.fori_loop(0, 2, rows_back, 0)

    def sum_rows(value):
        return jnp.sum(value, axis=0, keepdims=True)

    lines = []
    for probe in range(2):
        totals = [jnp.zeros((8, LANES), F32) for _ in range(4)]
        for top in range(2):
            for a in range(direct.shape[2] // LANES):
                here = (probe, pl.ds(8 * top, 8), pl.ds(LANES * a, LANES))
                r, d, q = resid[here], direct[here], image[here]
                for index, term in enumerate((r * r, d * q, r * q, q * q)):
                    totals[index] += term
        lines += [sum_rows(total) for total in totals]
    stacked = jnp.sum(jnp.concatenate(lines, axis=0), axis=1, keepdims=True)
    at_row = lax.broadcasted_iota(jnp.int32, (8, LANES), 0)
    at_lane = lax.broadcasted_iota(jnp.int32, (8, LANES), 1)
    mine = sum_rows(jnp.where(at_row == at_lane, stacked, 0.0))
    sums[me] = mine

    def tell(to_row, to_sub):
        pltpu.make_async_remote_copy(
            sums.at[me], sums.at[me], send_s, recv_s,
            device_id={"row": to_row, "sub": to_sub}, device_id_type=MESH,
        ).start()

    each_peer(tell)
    for ch in range(2):
        wait_all(out_f, ch, send_f)
        wait_all(out_b, ch, send_b)
    others = sums.at[pl.ds(0, devices - 1)]
    pltpu.make_async_copy(others, others, send_s).wait()
    pltpu.make_async_copy(others, others, recv_s).wait()
    total_out[...] = jnp.sum(sums[...], axis=0)


def finish(total_ref, resid, direct, image, resid_out, dir_out, step_out):
    total = total_ref[...]
    for probe in range(2):
        old_norm, curvature, cross, square = (total[:, 4 * probe + i : 4 * probe + i + 1] for i in range(4))
        size = old_norm / curvature
        new_norm = old_norm - 2.0 * (size * cross) + size * (size * square)
        ratio = new_norm / (old_norm + TINY)
        step_out[probe] = size[0, 0]
        for a in range(direct.shape[2] // LANES):
            here = (probe, slice(None), pl.ds(LANES * a, LANES))
            value = resid[here] - size * image[here]
            resid_out[here] = value
            dir_out[here] = value + ratio * direct[here]


def body(n_row, n_sub, residual_in, direction, spectrum, noise_var):
    probes, rows_dev, grid_len = direction.shape
    devices = n_row * n_sub
    embed = 2 * grid_len
    consts, turns = tables(rows_dev, grid_len, devices)
    low_len = embed // RADIX
    wide = 2 * LANES
    slots = (devices, 8, LANES)
    vmem = pltpu.VMEM
    sems = pltpu.SemaphoreType.DMA
    block = (probes, rows_dev, grid_len)
    hbm_spec = pl.BlockSpec(memory_space=pltpu.HBM)
    vmem_spec = pl.BlockSpec(memory_space=pltpu.VMEM)
    smem_spec = pl.BlockSpec(memory_space=pltpu.SMEM)
    image, total = pl.pallas_call(
        functools.partial(kernel, n_row, n_sub, 1.0 / (embed * embed)),
        out_shape=(jax.ShapeDtypeStruct(block, F32), jax.ShapeDtypeStruct((1, LANES), F32)),
        in_specs=[smem_spec] + [hbm_spec] * 5,
        out_specs=(vmem_spec, vmem_spec),
        scratch_shapes=[
            vmem(block, F32), vmem(block, F32), vmem((embed // LANES, spectrum.shape[1], LANES), F32),
            vmem(consts.shape, BF16), vmem(turns.shape, F32),
            vmem(slots, F32), vmem(slots, F32), vmem(slots, F32), vmem(slots, F32),
            vmem((devices, 1, LANES), F32), vmem((low_len, 4 * LANES), F32),
            vmem((wide, wide), F32), vmem((2 * low_len, wide), F32),
            vmem((2 * low_len, wide), BF16), vmem((2 * low_len, wide), BF16),
            vmem((2 * low_len, wide), BF16), vmem((2 * low_len, wide), BF16),
            sems((5,)), sems((2,)), sems((2,)), sems((2,)), sems((2,)), sems, sems, pltpu.SemaphoreType.REGULAR((n_sub + 1,)),
        ],
        compiler_params=pltpu.CompilerParams(
            collective_id=0, has_side_effects=True, vmem_limit_bytes=VMEM_LIMIT
        ),
        name="cg_step",
    )(noise_var, residual_in, direction, spectrum.T, *(jnp.asarray(t) for t in (consts, turns)))
    return pl.pallas_call(
        finish,
        out_shape=(
            jax.ShapeDtypeStruct(block, F32),
            jax.ShapeDtypeStruct(block, F32),
            jax.ShapeDtypeStruct((probes,), F32),
        ),
        in_specs=[vmem_spec] * 4,
        out_specs=(vmem_spec, vmem_spec, smem_spec),
        compiler_params=pltpu.CompilerParams(vmem_limit_bytes=8 << 20),
        name="finish",
    )(total, residual_in, direction, image)


def solution(mesh):
    in_specs = (P("grp", ROW_SUB, None), P("grp", ROW_SUB, None), P("grp", ROW_SUB), P("grp"))
    out_specs = (P("grp", ROW_SUB, None), P("grp", ROW_SUB, None), P("grp"))
    return jax.shard_map(
        functools.partial(body, mesh.shape["row"], mesh.shape["sub"]),
        mesh=mesh, in_specs=in_specs, out_specs=out_specs, check_vma=False,
    )
```

```python
import functools
import math

import jax
import jax.numpy as jnp
import ml_dtypes
import numpy as np
from jax import lax
from jax.experimental import pallas as pl
from jax.experimental.pallas import tpu as pltpu
from jax.sharding import PartitionSpec as P

ROW_SUB = ("row", "sub")
MESH = pl.DeviceIdType.MESH
TINY = 1e-06
VMEM_LIMIT = 107 << 19
LANES = 128
RADIX = 16
F32 = jnp.float32
BF16 = jnp.bfloat16


def roots(left, right, modulus, sign):
    turns = np.mod(np.outer(left, right), modulus)
    return np.exp(sign * 2j * np.pi * turns / modulus)


def real_form(table):
    return np.block([[table.real, -table.imag], [table.imag, table.real]])


def halves(table):
    high = table.astype(ml_dtypes.bfloat16)
    low = (table - high.astype(np.float64)).astype(ml_dtypes.bfloat16)
    return np.stack([high, low])


def tables(rows_dev, grid_len, devices):
    embed = 2 * grid_len
    lane_ids = np.arange(LANES)
    dev_ids = np.arange(devices)
    block = LANES // RADIX
    long_row = real_form(roots(dev_ids, lane_ids, LANES, -1))
    low_ids = np.arange(embed // RADIX)
    long_col = real_form(roots(low_ids, dev_ids, embed // RADIX, -1))
    short = roots(np.arange(RADIX), np.arange(RADIX), RADIX, -1)
    mixed = np.zeros((block, RADIX, RADIX, block), complex)
    for e in range(block):
        mixed[e, :, :, e] = short
    mixed = mixed.reshape(LANES, LANES)
    short_col = real_form(mixed.T).T
    short_back = real_form(np.conj(mixed)).T
    long_back = real_form(np.conj(roots(dev_ids, low_ids, embed // RADIX, -1)))
    half = long_back.shape[1] // 2
    row_back = real_form(np.conj(roots(lane_ids, dev_ids, LANES, -1))).T
    stacked = np.concatenate(
        [long_row, long_col, short_col, short_back, long_back[:, :half], long_back[:, half:], row_back], axis=0
    )
    consts = halves(stacked)
    turn_col = np.tile(roots(low_ids, np.arange(RADIX), embed, -1), (1, block))
    turn_col = np.stack([turn_col.real, turn_col.imag]).astype(np.float32)
    turn_row = np.zeros((2, 2 * RADIX, 2, LANES))
    for ch in range(2):
        for e in range(RADIX):
            turn = roots([2 * e + ch], lane_ids, embed, -1)[0]
            turn_row[ch, e] = [turn.real, turn.imag]
            odd = np.exp(-2j * np.pi * e * ch / (2 * RADIX))
            turn_row[ch, RADIX + e, 0] = odd.real
            turn_row[ch, RADIX + e, 1] = odd.imag
    turns = np.concatenate([turn_row.reshape(-1, LANES), turn_col.reshape(-1, LANES)]).astype(np.float32)
    return consts, turns


def add(x, y):
    return (x[0] + y[0], x[1] + y[1])


def sub(x, y):
    return (x[0] - y[0], x[1] - y[1])


def times(x, y):
    return (x[0] * y[0] - x[1] * y[1], x[0] * y[1] + x[1] * y[0])


def times_conj(x, y):
    return (x[0] * y[0] + x[1] * y[1], x[1] * y[0] - x[0] * y[1])


def by_root(x, power, sign):
    power %= RADIX
    if power == 0:
        return x
    if power == 4:
        return (x[1], -x[0]) if sign < 0 else (-x[1], x[0])
    if power == 8:
        return (-x[0], -x[1])
    angle = sign * 2.0 * math.pi * power / RADIX
    return times(x, (math.cos(angle), math.sin(angle)))


def four(x, sign):
    even, odd = add(x[0], x[2]), sub(x[0], x[2])
    both, diff = add(x[1], x[3]), sub(x[1], x[3])
    turned = (diff[1], -diff[0]) if sign < 0 else (-diff[1], diff[0])
    return [add(even, both), add(odd, turned), sub(even, both), sub(odd, turned)]


def sixteen(x, sign):
    inner = [four([x[4 * i + j] for i in range(4)], sign) for j in range(4)]
    out = [None] * RADIX
    for first in range(4):
        column = [by_root(inner[j][first], j * first, sign) for j in range(4)]
        for second, value in enumerate(four(column, sign)):
            out[first + 4 * second] = value
    return out


def split(value):
    high = value.astype(BF16)
    return high, (value - high.astype(F32)).astype(BF16)


def dot(left, right, transposed=False):
    dims = (((1,), (1 if transposed else 0,)), ((), ()))
    return lax.dot_general(left, right, dims, preferred_element_type=F32)


def dot3(left, right, transposed=False):
    return (
        dot(left[1], right[0], transposed) + dot(left[0], right[1], transposed) + dot(left[0], right[0], transposed)
    )


def far_first(n_row, n_sub):
    def chips(row, sub_):
        hop = row // 2
        return min(hop, n_row // 2 - hop) + min(sub_, n_sub - sub_)

    offsets = [(i, j) for i in range(n_row) for j in range(n_sub)][1:]
    return sorted(offsets, key=lambda pair: -chips(*pair))


def outward(count):
    return [count // 2 + (1 - 2 * (t % 2)) * ((t + 1) // 2) for t in range(count)]


def kernel(
    n_row, n_sub, scale,
    noise_ref, resid_hbm, dir_hbm, spec_hbm, consts_hbm, turns_hbm,
    image, total_out,
    resid, direct, spec, consts, turns,
    out_f, in_f, out_b, in_b, sums, spec_t,
    work, tall, left_hi, left_lo, right_hi, right_lo,
    load_sem, send_f, recv_f, send_b, recv_b, send_s, recv_s, here_sem,
):
    devices = n_row * n_sub
    row, sub_ = lax.axis_index("row"), lax.axis_index("sub")
    me = row * n_sub + sub_
    offsets = far_first(n_row, n_sub)
    wide = 2 * LANES
    low_len = tall.shape[0] // 2

    def load(src, dst, slot):
        copy = pltpu.make_async_copy(src, dst, load_sem.at[slot])
        copy.start()
        return copy

    def wrap(value, count):
        return jnp.where(value >= count, value - count, value)

    def peer(i, j):
        return wrap(row + i, n_row), wrap(sub_ + j, n_sub)

    subs = [wrap(sub_ + j, n_sub) for j in outward(n_sub)]
    rows = [wrap(row + i, n_row) for i in outward(n_row)]
    apart = lax.axis_index("grp") == 0
    late = apart & (me == 0)

    def ordinary(to_row, to_sub):
        return (to_row + to_sub != 0) | jnp.logical_not(apart)

    level = jnp.where(late, n_sub, sub_)

    def each_peer(act):
        def one_row(t, carry):
            half = n_row // 2
            to_row = wrap(row + half + (1 - 2 * (t % 2)) * ((t + 1) // 2), n_row)
            for to_sub in subs:
                act(to_row, to_sub)
            return carry

        lax.fori_loop(0, n_row - 1, one_row, 0)
        for to_sub in subs[:-1]:
            act(row, to_sub)

    first, rest = pl.ds(0, wide), pl.ds(wide, consts.shape[1] - wide)
    loads = [
        load(dir_hbm, direct, 0),
        load(turns_hbm.at[pl.ds(0, 8 * RADIX)], turns.at[pl.ds(0, 8 * RADIX)], 1),
        load(consts_hbm.at[:, first], consts.at[:, first], 2),
    ]
    barrier = pltpu.get_barrier_semaphore()

    def greet(to_row, to_sub):
        pl.semaphore_signal(barrier, inc=1, device_id={"row": to_row, "sub": to_sub}, device_id_type=MESH)

    def announce(to_row, to_sub):
        pl.semaphore_signal(here_sem.at[level], inc=1, device_id={"row": to_row, "sub": to_sub}, device_id_type=MESH)

    def greet_sub(to_sub, carry):
        @pl.when(to_sub > sub_)
        def _():
            for to_row in rows:
                greet(to_row, to_sub)

        return carry

    @pl.when(jnp.logical_not(late))
    def _():
        for to_row in rows[:-1]:
            greet(to_row, sub_)
        lax.fori_loop(1, n_sub, greet_sub, 0)
        pl.when(apart & (sub_ != 0))(lambda: greet(0, 0))

    later_loads = [
        load(consts_hbm.at[:, rest], consts.at[:, rest], 5),
        load(turns_hbm.at[pl.ds(8 * RADIX, 2 * low_len)], turns.at[pl.ds(8 * RADIX, 2 * low_len)], 6),
        load(resid_hbm, resid, 3),
    ]
    for t in range(spec.shape[0]):
        load(spec_hbm.at[:, pl.ds(LANES * t, LANES)], spec.at[t], 4)

    def const(index, count=1):
        rows = pl.ds(wide * index, wide * count)
        return consts[0, rows, :], consts[1, rows, :]

    def send(src, dst, ch, send_sem, recv_sem, to_row, to_sub):
        part = pl.ds(4 * ch, 4)
        pltpu.make_async_remote_copy(
            src.at[to_row * n_sub + to_sub, part],
            dst.at[me, part],
            send_sem.at[ch],
            recv_sem.at[ch],
            device_id={"row": to_row, "sub": to_sub},
            device_id_type=MESH,
        ).start()

    def send_all(src, dst, ch, send_sem, recv_sem, all_here):
        for i, j in offsets:
            to_row, to_sub = peer(i, j)
            go = functools.partial(send, src, dst, ch, send_sem, recv_sem, to_row, to_sub)
            if all_here:
                go()
            else:
                pl.when(ordinary(to_row, to_sub) & (to_sub <= level))(go)
        part = pl.ds(4 * ch, 4)
        dst[me, part] = src[me, part]

    def wait_all(ref, ch, sem):
        others = ref.at[pl.ds(0, devices - 1), pl.ds(4 * ch, 4)]
        pltpu.make_async_copy(others, others, sem.at[ch]).wait()

    def flat(ref):
        return ref.reshape(devices * 8, LANES)

    def turn(ch, index):
        both = turns[pl.ds(4 * RADIX * ch + 2 * index, 2), :]
        return both[0:1], both[1:2]

    def turn_col(at, step):
        first = 8 * RADIX + at
        return turns[pl.ds(first, step), :], turns[pl.ds(first + low_len, step), :]

    @pl.when(late)
    def _():
        pl.semaphore_wait(barrier, devices - 1)
        each_peer(announce)

    for copy in loads:
        copy.wait()

    def rows_forward(ch, carry):
        for top in range(2):
            lines = pl.ds(8 * top, 8)
            values = []
            for a in range(RADIX):
                lanes = pl.ds(LANES * a, LANES)
                values.append(times((direct[0, lines, lanes], direct[1, lines, lanes]), turn(ch, RADIX + a)))
            for e, value in enumerate(sixteen(values, -1)):
                value = times(value, turn(ch, e))
                for part in range(2):
                    work[pl.ds(RADIX * e + 8 * top, 8), pl.ds(LANES * part, LANES)] = value[part]
        for at in range(0, wide, 32):
            lines = pl.ds(at, 32)
            right_hi[lines, :], right_lo[lines, :] = split(work[lines, :])
        freq = dot3(const(0), (right_hi[pl.ds(0, wide), :], right_lo[pl.ds(0, wide), :]), transposed=True)
        for part in range(2):
            for tile in range(2):
                flat(out_f)[pl.ds(4 * ch + 2 * part + tile, devices, stride=8), :] = freq[
                    devices * part : devices * (part + 1), LANES * tile : LANES * (tile + 1)
                ]

        @pl.when(ch == 0)
        def _():
            @pl.when(jnp.logical_not(late))
            def _():
                pl.semaphore_wait(barrier, n_row * (sub_ + 1) - 1 - apart.astype(jnp.int32))
                for to_sub in range(n_sub):
                    pl.when((to_sub < sub_) & ordinary(row, to_sub))(functools.partial(announce, row, to_sub))

        send_all(out_f, in_f, ch, send_f, recv_f, False)
        return carry

    lax.fori_loop(0, 2, rows_forward, 0)

    for copy in later_loads:
        copy.wait()
    pltpu.make_async_copy(spec, spec, load_sem.at[4]).wait()
    spec_rows = spec.reshape(spec.shape[0] * spec.shape[1], LANES)
    for ch in range(2):
        for tile in range(2):
            for top in range(low_len // LANES):
                parts = []
                for high in range(RADIX):
                    at = spec.shape[1] * ((low_len // LANES) * high + top) + RADIX * tile + ch
                    parts.append(spec_rows[pl.ds(at, 8, stride=2), :])
                spec_t[pl.ds(LANES * top, LANES), pl.ds(wide * ch + LANES * tile, LANES)] = (
                    jnp.concatenate(parts, axis=0).T * scale
                )

    def later_class(t, carry):
        ch, to_sub = t // n_sub, t % n_sub

        @pl.when(to_sub > level)
        def _():
            pl.when(ch == 0)(lambda: pl.semaphore_wait(here_sem.at[to_sub], 1))
            for to_row in rows:
                send(out_f, in_f, ch, send_f, recv_f, to_row, to_sub)

        return carry

    lax.fori_loop(0, 2 * n_sub, later_class, 0)

    @pl.when(apart & jnp.logical_not(late))
    def _():
        pl.semaphore_wait(here_sem.at[n_sub], 1)
        for ch in range(2):
            send(out_f, in_f, ch, send_f, recv_f, 0, 0)

    def columns(ch, carry):
        wait_all(in_f, ch, recv_f)
        for part in range(2):
            for tile in range(2):
                here = (pl.ds(devices * part, devices), pl.ds(LANES * tile, LANES))
                right_hi[here], right_lo[here] = split(
                    flat(in_f)[pl.ds(4 * ch + 2 * part + tile, devices, stride=8), :]
                )
        tall[...] = dot3(const(1, 2), (right_hi[pl.ds(0, wide), :], right_lo[pl.ds(0, wide), :]))
        step = 32
        for tile in range(2):
            lanes = pl.ds(LANES * tile, LANES)
            for at in range(0, low_len, step):
                lines = pl.ds(at, step)
                value = times(
                    (tall[lines, lanes], tall[pl.ds(low_len + at, step), lanes]),
                    turn_col(at, step),
                )
                for part in range(2):
                    here = (pl.ds(low_len * tile + at, step), pl.ds(LANES * part, LANES))
                    left_hi[here], left_lo[here] = split(value[part])
        tall[...] = dot3((left_hi[...], left_lo[...]), const(3))
        for tile in range(2):
            for at in range(0, low_len, step):
                weight = spec_t[pl.ds(at, step), pl.ds(pl.multiple_of(wide * ch + LANES * tile, LANES), LANES)]
                for part in range(2):
                    here = (pl.ds(low_len * tile + at, step), pl.ds(LANES * part, LANES))
                    left_hi[here], left_lo[here] = split(tall[here] * weight)
        tall[...] = dot3((left_hi[...], left_lo[...]), const(4))
        for tile in range(2):
            for at in range(0, low_len, step):
                lines = pl.ds(at, step)
                here = pl.ds(low_len * tile + at, step)
                value = times_conj(
                    (tall[here, pl.ds(0, LANES)], tall[here, pl.ds(LANES, LANES)]),
                    turn_col(at, step),
                )
                for part in range(2):
                    there = (pl.ds(low_len * part + at, step), pl.ds(LANES * tile, LANES))
                    right_hi[there], right_lo[there] = split(value[part])
        low, high = pl.ds(0, low_len), pl.ds(low_len, low_len)
        grid = dot3(const(5), (right_hi[low, :], right_lo[low, :])) + dot3(
            const(6), (right_hi[high, :], right_lo[high, :])
        )
        for part in range(2):
            for tile in range(2):
                flat(out_b)[pl.ds(4 * ch + 2 * part + tile, devices, stride=8), :] = grid[
                    devices * part : devices * (part + 1), LANES * tile : LANES * (tile + 1)
                ]
        send_all(out_b, in_b, ch, send_b, recv_b, True)
        return carry

    lax.fori_loop(0, 2, columns, 0)

    noise = noise_ref[0]
    image[...] = noise * direct[...]

    def rows_back(ch, carry):
        wait_all(in_b, ch, recv_b)
        for part in range(2):
            for tile in range(2):
                here = (pl.ds(LANES * tile, LANES), pl.ds(devices * part, devices))
                block = flat(in_b)[pl.ds(4 * ch + 2 * part + tile, devices, stride=8), :]
                left_hi[here], left_lo[here] = split(block.T)
        work[...] = dot3((left_hi[pl.ds(0, wide), :], left_lo[pl.ds(0, wide), :]), const(7))
        for top in range(2):
            values = []
            for e in range(RADIX):
                lines = pl.ds(RADIX * e + 8 * top, 8)
                values.append(
                    times_conj((work[lines, pl.ds(0, LANES)], work[lines, pl.ds(LANES, LANES)]), turn(ch, e))
                )
            lines = pl.ds(8 * top, 8)
            for a, value in enumerate(sixteen(values, 1)):
                value = times_conj(value, turn(ch, RADIX + a))
                lanes = pl.ds(LANES * a, LANES)
                for part in range(2):
                    image[part, lines, lanes] += value[part]
        return carry

    lax.fori_loop(0, 2, rows_back, 0)

    def sum_rows(value):
        return jnp.sum(value, axis=0, keepdims=True)

    lines = []
    for probe in range(2):
        totals = [jnp.zeros((8, LANES), F32) for _ in range(4)]
        for top in range(2):
            for a in range(direct.shape[2] // LANES):
                here = (probe, pl.ds(8 * top, 8), pl.ds(LANES * a, LANES))
                r, d, q = resid[here], direct[here], image[here]
                for index, term in enumerate((r * r, d * q, r * q, q * q)):
                    totals[index] += term
        lines += [sum_rows(total) for total in totals]
    stacked = jnp.sum(jnp.concatenate(lines, axis=0), axis=1, keepdims=True)
    at_row = lax.broadcasted_iota(jnp.int32, (8, LANES), 0)
    at_lane = lax.broadcasted_iota(jnp.int32, (8, LANES), 1)
    mine = sum_rows(jnp.where(at_row == at_lane, stacked, 0.0))
    sums[me] = mine

    def tell(to_row, to_sub):
        pltpu.make_async_remote_copy(
            sums.at[me], sums.at[me], send_s, recv_s,
            device_id={"row": to_row, "sub": to_sub}, device_id_type=MESH,
        ).start()

    each_peer(tell)
    for ch in range(2):
        wait_all(out_f, ch, send_f)
        wait_all(out_b, ch, send_b)
    others = sums.at[pl.ds(0, devices - 1)]
    pltpu.make_async_copy(others, others, send_s).wait()
    pltpu.make_async_copy(others, others, recv_s).wait()
    total_out[...] = jnp.sum(sums[...], axis=0)


def finish(total_ref, resid, direct, image, resid_out, dir_out, step_out):
    total = total_ref[...]
    for probe in range(2):
        old_norm, curvature, cross, square = (total[:, 4 * probe + i : 4 * probe + i + 1] for i in range(4))
        size = old_norm / curvature
        new_norm = old_norm - 2.0 * (size * cross) + size * (size * square)
        ratio = new_norm / (old_norm + TINY)
        step_out[probe] = size[0, 0]
        for a in range(direct.shape[2] // LANES):
            here = (probe, slice(None), pl.ds(LANES * a, LANES))
            value = resid[here] - size * image[here]
            resid_out[here] = value
            dir_out[here] = value + ratio * direct[here]


def body(n_row, n_sub, residual_in, direction, spectrum, noise_var):
    probes, rows_dev, grid_len = direction.shape
    devices = n_row * n_sub
    embed = 2 * grid_len
    consts, turns = tables(rows_dev, grid_len, devices)
    low_len = embed // RADIX
    wide = 2 * LANES
    slots = (devices, 8, LANES)
    vmem = pltpu.VMEM
    sems = pltpu.SemaphoreType.DMA
    block = (probes, rows_dev, grid_len)
    hbm_spec = pl.BlockSpec(memory_space=pltpu.HBM)
    vmem_spec = pl.BlockSpec(memory_space=pltpu.VMEM)
    smem_spec = pl.BlockSpec(memory_space=pltpu.SMEM)
    image, total = pl.pallas_call(
        functools.partial(kernel, n_row, n_sub, 1.0 / (embed * embed)),
        out_shape=(jax.ShapeDtypeStruct(block, F32), jax.ShapeDtypeStruct((1, LANES), F32)),
        in_specs=[smem_spec] + [hbm_spec] * 5,
        out_specs=(vmem_spec, vmem_spec),
        scratch_shapes=[
            vmem(block, F32), vmem(block, F32), vmem((embed // LANES, spectrum.shape[1], LANES), F32),
            vmem(consts.shape, BF16), vmem(turns.shape, F32),
            vmem(slots, F32), vmem(slots, F32), vmem(slots, F32), vmem(slots, F32),
            vmem((devices, 1, LANES), F32), vmem((low_len, 4 * LANES), F32),
            vmem((wide, wide), F32), vmem((2 * low_len, wide), F32),
            vmem((2 * low_len, wide), BF16), vmem((2 * low_len, wide), BF16),
            vmem((2 * low_len, wide), BF16), vmem((2 * low_len, wide), BF16),
            sems((7,)), sems((2,)), sems((2,)), sems((2,)), sems((2,)), sems, sems, pltpu.SemaphoreType.REGULAR((n_sub + 1,)),
        ],
        compiler_params=pltpu.CompilerParams(
            collective_id=0, has_side_effects=True, vmem_limit_bytes=VMEM_LIMIT
        ),
        name="cg_step",
    )(noise_var, residual_in, direction, spectrum.T, *(jnp.asarray(t) for t in (consts, turns)))
    return pl.pallas_call(
        finish,
        out_shape=(
            jax.ShapeDtypeStruct(block, F32),
            jax.ShapeDtypeStruct(block, F32),
            jax.ShapeDtypeStruct((probes,), F32),
        ),
        in_specs=[vmem_spec] * 4,
        out_specs=(vmem_spec, vmem_spec, smem_spec),
        compiler_params=pltpu.CompilerParams(vmem_limit_bytes=8 << 20),
        name="finish",
    )(total, residual_in, direction, image)


def solution(mesh):
    in_specs = (P("grp", ROW_SUB, None), P("grp", ROW_SUB, None), P("grp", ROW_SUB), P("grp"))
    out_specs = (P("grp", ROW_SUB, None), P("grp", ROW_SUB, None), P("grp"))
    return jax.shard_map(
        functools.partial(body, mesh.shape["row"], mesh.shape["sub"]),
        mesh=mesh, in_specs=in_specs, out_specs=out_specs, check_vma=False,
    )
```

```python
import functools
import math

import jax
import jax.numpy as jnp
import ml_dtypes
import numpy as np
from jax import lax
from jax.experimental import pallas as pl
from jax.experimental.pallas import tpu as pltpu
from jax.sharding import PartitionSpec as P

ROW_SUB = ("row", "sub")
MESH = pl.DeviceIdType.MESH
TINY = 1e-06
VMEM_LIMIT = 107 << 19
LANES = 128
RADIX = 16
F32 = jnp.float32
BF16 = jnp.bfloat16


def roots(left, right, modulus, sign):
    turns = np.mod(np.outer(left, right), modulus)
    return np.exp(sign * 2j * np.pi * turns / modulus)


def real_form(table):
    return np.block([[table.real, -table.imag], [table.imag, table.real]])


def halves(table):
    high = table.astype(ml_dtypes.bfloat16)
    low = (table - high.astype(np.float64)).astype(ml_dtypes.bfloat16)
    return np.stack([high, low])


def tables(rows_dev, grid_len, devices):
    embed = 2 * grid_len
    lane_ids = np.arange(LANES)
    dev_ids = np.arange(devices)
    block = LANES // RADIX
    long_row = real_form(roots(dev_ids, lane_ids, LANES, -1))
    low_ids = np.arange(embed // RADIX)
    long_col = real_form(roots(low_ids, dev_ids, embed // RADIX, -1))
    short = roots(np.arange(RADIX), np.arange(RADIX), RADIX, -1)
    mixed = np.zeros((block, RADIX, RADIX, block), complex)
    for e in range(block):
        mixed[e, :, :, e] = short
    mixed = mixed.reshape(LANES, LANES)
    short_col = real_form(mixed.T).T
    short_back = real_form(np.conj(mixed)).T
    long_back = real_form(np.conj(roots(dev_ids, low_ids, embed // RADIX, -1)))
    half = long_back.shape[1] // 2
    row_back = real_form(np.conj(roots(lane_ids, dev_ids, LANES, -1))).T
    stacked = np.concatenate(
        [long_row, long_col, short_col, short_back, long_back[:, :half], long_back[:, half:], row_back], axis=0
    )
    consts = halves(stacked)
    turn_col = np.tile(roots(low_ids, np.arange(RADIX), embed, -1), (1, block))
    turn_col = np.stack([turn_col.real, turn_col.imag]).astype(np.float32)
    turn_row = np.zeros((2, 2 * RADIX, 2, LANES))
    for ch in range(2):
        for e in range(RADIX):
            turn = roots([2 * e + ch], lane_ids, embed, -1)[0]
            turn_row[ch, e] = [turn.real, turn.imag]
            odd = np.exp(-2j * np.pi * e * ch / (2 * RADIX))
            turn_row[ch, RADIX + e, 0] = odd.real
            turn_row[ch, RADIX + e, 1] = odd.imag
    turns = np.concatenate([turn_row.reshape(-1, LANES), turn_col.reshape(-1, LANES)]).astype(np.float32)
    return consts, turns


def add(x, y):
    return (x[0] + y[0], x[1] + y[1])


def sub(x, y):
    return (x[0] - y[0], x[1] - y[1])


def times(x, y):
    return (x[0] * y[0] - x[1] * y[1], x[0] * y[1] + x[1] * y[0])


def times_conj(x, y):
    return (x[0] * y[0] + x[1] * y[1], x[1] * y[0] - x[0] * y[1])


def by_root(x, power, sign):
    power %= RADIX
    if power == 0:
        return x
    if power == 4:
        return (x[1], -x[0]) if sign < 0 else (-x[1], x[0])
    if power == 8:
        return (-x[0], -x[1])
    angle = sign * 2.0 * math.pi * power / RADIX
    return times(x, (math.cos(angle), math.sin(angle)))


def four(x, sign):
    even, odd = add(x[0], x[2]), sub(x[0], x[2])
    both, diff = add(x[1], x[3]), sub(x[1], x[3])
    turned = (diff[1], -diff[0]) if sign < 0 else (-diff[1], diff[0])
    return [add(even, both), add(odd, turned), sub(even, both), sub(odd, turned)]


def sixteen(x, sign):
    inner = [four([x[4 * i + j] for i in range(4)], sign) for j in range(4)]
    out = [None] * RADIX
    for first in range(4):
        column = [by_root(inner[j][first], j * first, sign) for j in range(4)]
        for second, value in enumerate(four(column, sign)):
            out[first + 4 * second] = value
    return out


def split(value):
    high = value.astype(BF16)
    return high, (value - high.astype(F32)).astype(BF16)


def dot(left, right, transposed=False):
    dims = (((1,), (1 if transposed else 0,)), ((), ()))
    return lax.dot_general(left, right, dims, preferred_element_type=F32)


def dot3(left, right, transposed=False):
    return (
        dot(left[1], right[0], transposed) + dot(left[0], right[1], transposed) + dot(left[0], right[0], transposed)
    )


def far_first(n_row, n_sub):
    def chips(row, sub_):
        hop = row // 2
        return min(hop, n_row // 2 - hop) + min(sub_, n_sub - sub_)

    offsets = [(i, j) for i in range(n_row) for j in range(n_sub)][1:]
    return sorted(offsets, key=lambda pair: -chips(*pair))


def outward(count):
    return [count // 2 + (1 - 2 * (t % 2)) * ((t + 1) // 2) for t in range(count)]


def kernel(
    n_row, n_sub, scale,
    noise_ref, resid_hbm, dir_hbm, spec_hbm, consts_hbm, turns_hbm,
    image, total_out,
    resid, direct, spec, consts, turns,
    out_f, in_f, out_b, in_b, sums, spec_t,
    work, tall, left_hi, left_lo, right_hi, right_lo,
    load_sem, send_f, recv_f, send_b, recv_b, send_s, recv_s, here_sem,
):
    devices = n_row * n_sub
    row, sub_ = lax.axis_index("row"), lax.axis_index("sub")
    me = row * n_sub + sub_
    offsets = far_first(n_row, n_sub)
    wide = 2 * LANES
    low_len = tall.shape[0] // 2

    def load(src, dst, slot):
        copy = pltpu.make_async_copy(src, dst, load_sem.at[slot])
        copy.start()
        return copy

    def wrap(value, count):
        return jnp.where(value >= count, value - count, value)

    def peer(i, j):
        return wrap(row + i, n_row), wrap(sub_ + j, n_sub)

    subs = [wrap(sub_ + j, n_sub) for j in outward(n_sub)]
    rows = [wrap(row + i, n_row) for i in outward(n_row)]
    apart = lax.axis_index("grp") == 0
    late = apart & (me == 0)

    def ordinary(to_row, to_sub):
        return (to_row + to_sub != 0) | jnp.logical_not(apart)

    level = jnp.where(late, n_sub, sub_)

    def each_peer(act):
        def one_row(t, carry):
            half = n_row // 2
            to_row = wrap(row + half + (1 - 2 * (t % 2)) * ((t + 1) // 2), n_row)
            for to_sub in subs:
                act(to_row, to_sub)
            return carry

        lax.fori_loop(0, n_row - 1, one_row, 0)
        for to_sub in subs[:-1]:
            act(row, to_sub)

    first, rest = pl.ds(0, wide), pl.ds(wide, consts.shape[1] - wide)
    loads = [
        load(dir_hbm, direct, 0),
        load(turns_hbm.at[pl.ds(0, 8 * RADIX)], turns.at[pl.ds(0, 8 * RADIX)], 1),
        load(consts_hbm.at[:, first], consts.at[:, first], 2),
    ]
    barrier = pltpu.get_barrier_semaphore()

    def greet(to_row, to_sub):
        pl.semaphore_signal(barrier, inc=1, device_id={"row": to_row, "sub": to_sub}, device_id_type=MESH)

    def announce(to_row, to_sub):
        pl.semaphore_signal(here_sem.at[level], inc=1, device_id={"row": to_row, "sub": to_sub}, device_id_type=MESH)

    def greet_sub(to_sub, carry):
        @pl.when(to_sub > sub_)
        def _():
            for to_row in rows:
                greet(to_row, to_sub)

        return carry

    @pl.when(jnp.logical_not(late))
    def _():
        for to_row in rows[:-1]:
            greet(to_row, sub_)
        lax.fori_loop(1, n_sub, greet_sub, 0)
        pl.when(apart & (sub_ != 0))(lambda: greet(0, 0))

    later_loads = [
        load(consts_hbm.at[:, rest], consts.at[:, rest], 5),
        load(turns_hbm.at[pl.ds(8 * RADIX, 2 * low_len)], turns.at[pl.ds(8 * RADIX, 2 * low_len)], 6),
        load(resid_hbm, resid, 3),
    ]
    for t in range(spec.shape[0]):
        load(spec_hbm.at[:, pl.ds(LANES * t, LANES)], spec.at[t], 4)

    def const(index, count=1):
        rows = pl.ds(wide * index, wide * count)
        return consts[0, rows, :], consts[1, rows, :]

    def send(src, dst, ch, send_sem, recv_sem, to_row, to_sub):
        part = pl.ds(4 * ch, 4)
        pltpu.make_async_remote_copy(
            src.at[to_row * n_sub + to_sub, part],
            dst.at[me, part],
            send_sem.at[ch],
            recv_sem.at[ch],
            device_id={"row": to_row, "sub": to_sub},
            device_id_type=MESH,
        ).start()

    def send_all(src, dst, ch, send_sem, recv_sem, all_here):
        for i, j in offsets:
            to_row, to_sub = peer(i, j)
            go = functools.partial(send, src, dst, ch, send_sem, recv_sem, to_row, to_sub)
            if all_here:
                go()
            else:
                pl.when(ordinary(to_row, to_sub) & (to_sub <= level))(go)
        part = pl.ds(4 * ch, 4)
        dst[me, part] = src[me, part]

    def wait_all(ref, ch, sem):
        others = ref.at[pl.ds(0, devices - 1), pl.ds(4 * ch, 4)]
        pltpu.make_async_copy(others, others, sem.at[ch]).wait()

    def flat(ref):
        return ref.reshape(devices * 8, LANES)

    def turn(ch, index):
        both = turns[pl.ds(4 * RADIX * ch + 2 * index, 2), :]
        return both[0:1], both[1:2]

    def turn_col(at, step):
        first = 8 * RADIX + at
        return turns[pl.ds(first, step), :], turns[pl.ds(first + low_len, step), :]

    @pl.when(late)
    def _():
        pl.semaphore_wait(barrier, devices - 1)
        each_peer(announce)

    for copy in loads:
        copy.wait()

    def rows_forward(ch, carry):
        for top in range(2):
            lines = pl.ds(8 * top, 8)
            values = []
            for a in range(RADIX):
                lanes = pl.ds(LANES * a, LANES)
                values.append(times((direct[0, lines, lanes], direct[1, lines, lanes]), turn(ch, RADIX + a)))
            for e, value in enumerate(sixteen(values, -1)):
                value = times(value, turn(ch, e))
                for part in range(2):
                    work[pl.ds(RADIX * e + 8 * top, 8), pl.ds(LANES * part, LANES)] = value[part]
        for at in range(0, wide, 32):
            lines = pl.ds(at, 32)
            right_hi[lines, :], right_lo[lines, :] = split(work[lines, :])
        freq = dot3(const(0), (right_hi[pl.ds(0, wide), :], right_lo[pl.ds(0, wide), :]), transposed=True)
        for part in range(2):
            for tile in range(2):
                flat(out_f)[pl.ds(4 * ch + 2 * part + tile, devices, stride=8), :] = freq[
                    devices * part : devices * (part + 1), LANES * tile : LANES * (tile + 1)
                ]

        @pl.when(ch == 0)
        def _():
            @pl.when(jnp.logical_not(late))
            def _():
                pl.semaphore_wait(barrier, n_row * (sub_ + 1) - 1 - apart.astype(jnp.int32))
                for to_sub in range(n_sub):
                    pl.when((to_sub < sub_) & ordinary(row, to_sub))(functools.partial(announce, row, to_sub))

        send_all(out_f, in_f, ch, send_f, recv_f, False)
        return carry

    lax.fori_loop(0, 2, rows_forward, 0)

    for copy in later_loads:
        copy.wait()
    pltpu.make_async_copy(spec, spec, load_sem.at[4]).wait()
    spec_rows = spec.reshape(spec.shape[0] * spec.shape[1], LANES)
    for ch in range(2):
        for tile in range(2):
            for top in range(low_len // LANES):
                parts = []
                for high in range(RADIX):
                    at = spec.shape[1] * ((low_len // LANES) * high + top) + RADIX * tile + ch
                    parts.append(spec_rows[pl.ds(at, 8, stride=2), :])
                spec_t[pl.ds(LANES * top, LANES), pl.ds(wide * ch + LANES * tile, LANES)] = (
                    jnp.concatenate(parts, axis=0).T * scale
                )

    def later_class(t, carry):
        ch, to_sub = t // n_sub, t % n_sub

        @pl.when(to_sub > level)
        def _():
            pl.when(ch == 0)(lambda: pl.semaphore_wait(here_sem.at[to_sub], 1))
            for to_row in rows:
                send(out_f, in_f, ch, send_f, recv_f, to_row, to_sub)

        return carry

    lax.fori_loop(0, 2 * n_sub, later_class, 0)

    @pl.when(apart & jnp.logical_not(late))
    def _():
        pl.semaphore_wait(here_sem.at[n_sub], 1)
        for ch in range(2):
            send(out_f, in_f, ch, send_f, recv_f, 0, 0)

    def columns(ch, carry):
        wait_all(in_f, ch, recv_f)
        for part in range(2):
            for tile in range(2):
                here = (pl.ds(devices * part, devices), pl.ds(LANES * tile, LANES))
                right_hi[here], right_lo[here] = split(
                    flat(in_f)[pl.ds(4 * ch + 2 * part + tile, devices, stride=8), :]
                )
        tall[...] = dot3(const(1, 2), (right_hi[pl.ds(0, wide), :], right_lo[pl.ds(0, wide), :]))
        step = 32
        for tile in range(2):
            lanes = pl.ds(LANES * tile, LANES)
            for at in range(0, low_len, step):
                lines = pl.ds(at, step)
                value = times(
                    (tall[lines, lanes], tall[pl.ds(low_len + at, step), lanes]),
                    turn_col(at, step),
                )
                for part in range(2):
                    here = (pl.ds(low_len * tile + at, step), pl.ds(LANES * part, LANES))
                    left_hi[here], left_lo[here] = split(value[part])
        tall[...] = dot3((left_hi[...], left_lo[...]), const(3))
        for tile in range(2):
            for at in range(0, low_len, step):
                weight = spec_t[pl.ds(at, step), pl.ds(pl.multiple_of(wide * ch + LANES * tile, LANES), LANES)]
                for part in range(2):
                    here = (pl.ds(low_len * tile + at, step), pl.ds(LANES * part, LANES))
                    left_hi[here], left_lo[here] = split(tall[here] * weight)
        tall[...] = dot3((left_hi[...], left_lo[...]), const(4))
        for tile in range(2):
            for at in range(0, low_len, step):
                lines = pl.ds(at, step)
                here = pl.ds(low_len * tile + at, step)
                value = times_conj(
                    (tall[here, pl.ds(0, LANES)], tall[here, pl.ds(LANES, LANES)]),
                    turn_col(at, step),
                )
                for part in range(2):
                    there = (pl.ds(low_len * part + at, step), pl.ds(LANES * tile, LANES))
                    right_hi[there], right_lo[there] = split(value[part])
        low, high = pl.ds(0, low_len), pl.ds(low_len, low_len)
        grid = dot3(const(5), (right_hi[low, :], right_lo[low, :])) + dot3(
            const(6), (right_hi[high, :], right_lo[high, :])
        )
        for part in range(2):
            for tile in range(2):
                flat(out_b)[pl.ds(4 * ch + 2 * part + tile, devices, stride=8), :] = grid[
                    devices * part : devices * (part + 1), LANES * tile : LANES * (tile + 1)
                ]
        send_all(out_b, in_b, ch, send_b, recv_b, True)
        return carry

    lax.fori_loop(0, 2, columns, 0)

    noise = noise_ref[0]
    image[...] = noise * direct[...]

    def rows_back(ch, carry):
        wait_all(in_b, ch, recv_b)
        for part in range(2):
            for tile in range(2):
                here = (pl.ds(LANES * tile, LANES), pl.ds(devices * part, devices))
                block = flat(in_b)[pl.ds(4 * ch + 2 * part + tile, devices, stride=8), :]
                left_hi[here], left_lo[here] = split(block.T)
        work[...] = dot3((left_hi[pl.ds(0, wide), :], left_lo[pl.ds(0, wide), :]), const(7))
        for top in range(2):
            values = []
            for e in range(RADIX):
                lines = pl.ds(RADIX * e + 8 * top, 8)
                values.append(
                    times_conj((work[lines, pl.ds(0, LANES)], work[lines, pl.ds(LANES, LANES)]), turn(ch, e))
                )
            lines = pl.ds(8 * top, 8)
            for a, value in enumerate(sixteen(values, 1)):
                value = times_conj(value, turn(ch, RADIX + a))
                lanes = pl.ds(LANES * a, LANES)
                for part in range(2):
                    image[part, lines, lanes] += value[part]
        return carry

    lax.fori_loop(0, 2, rows_back, 0)

    def sum_rows(value):
        return jnp.sum(value, axis=0, keepdims=True)

    lines = []
    for probe in range(2):
        totals = [jnp.zeros((8, LANES), F32) for _ in range(4)]
        for top in range(2):
            for a in range(direct.shape[2] // LANES):
                here = (probe, pl.ds(8 * top, 8), pl.ds(LANES * a, LANES))
                r, d, q = resid[here], direct[here], image[here]
                for index, term in enumerate((r * r, d * q, r * q, q * q)):
                    totals[index] += term
        lines += [sum_rows(total) for total in totals]
    stacked = jnp.sum(jnp.concatenate(lines, axis=0), axis=1, keepdims=True)
    at_row = lax.broadcasted_iota(jnp.int32, (8, LANES), 0)
    at_lane = lax.broadcasted_iota(jnp.int32, (8, LANES), 1)
    mine = sum_rows(jnp.where(at_row == at_lane, stacked, 0.0))
    sums[me] = mine

    def tell(to_row, to_sub):
        pltpu.make_async_remote_copy(
            sums.at[me], sums.at[me], send_s, recv_s,
            device_id={"row": to_row, "sub": to_sub}, device_id_type=MESH,
        ).start()

    for i, j in offsets:
        tell(*peer(i, j))
    for ch in range(2):
        wait_all(out_f, ch, send_f)
        wait_all(out_b, ch, send_b)
    others = sums.at[pl.ds(0, devices - 1)]
    pltpu.make_async_copy(others, others, send_s).wait()
    pltpu.make_async_copy(others, others, recv_s).wait()
    total_out[...] = jnp.sum(sums[...], axis=0)


def finish(total_ref, resid, direct, image, resid_out, dir_out, step_out):
    total = total_ref[...]
    for probe in range(2):
        old_norm, curvature, cross, square = (total[:, 4 * probe + i : 4 * probe + i + 1] for i in range(4))
        size = old_norm / curvature
        new_norm = old_norm - 2.0 * (size * cross) + size * (size * square)
        ratio = new_norm / (old_norm + TINY)
        step_out[probe] = size[0, 0]
        for a in range(direct.shape[2] // LANES):
            here = (probe, slice(None), pl.ds(LANES * a, LANES))
            value = resid[here] - size * image[here]
            resid_out[here] = value
            dir_out[here] = value + ratio * direct[here]


def body(n_row, n_sub, residual_in, direction, spectrum, noise_var):
    probes, rows_dev, grid_len = direction.shape
    devices = n_row * n_sub
    embed = 2 * grid_len
    consts, turns = tables(rows_dev, grid_len, devices)
    low_len = embed // RADIX
    wide = 2 * LANES
    slots = (devices, 8, LANES)
    vmem = pltpu.VMEM
    sems = pltpu.SemaphoreType.DMA
    block = (probes, rows_dev, grid_len)
    hbm_spec = pl.BlockSpec(memory_space=pltpu.HBM)
    vmem_spec = pl.BlockSpec(memory_space=pltpu.VMEM)
    smem_spec = pl.BlockSpec(memory_space=pltpu.SMEM)
    image, total = pl.pallas_call(
        functools.partial(kernel, n_row, n_sub, 1.0 / (embed * embed)),
        out_shape=(jax.ShapeDtypeStruct(block, F32), jax.ShapeDtypeStruct((1, LANES), F32)),
        in_specs=[smem_spec] + [hbm_spec] * 5,
        out_specs=(vmem_spec, vmem_spec),
        scratch_shapes=[
            vmem(block, F32), vmem(block, F32), vmem((embed // LANES, spectrum.shape[1], LANES), F32),
            vmem(consts.shape, BF16), vmem(turns.shape, F32),
            vmem(slots, F32), vmem(slots, F32), vmem(slots, F32), vmem(slots, F32),
            vmem((devices, 1, LANES), F32), vmem((low_len, 4 * LANES), F32),
            vmem((wide, wide), F32), vmem((2 * low_len, wide), F32),
            vmem((2 * low_len, wide), BF16), vmem((2 * low_len, wide), BF16),
            vmem((2 * low_len, wide), BF16), vmem((2 * low_len, wide), BF16),
            sems((7,)), sems((2,)), sems((2,)), sems((2,)), sems((2,)), sems, sems, pltpu.SemaphoreType.REGULAR((n_sub + 1,)),
        ],
        compiler_params=pltpu.CompilerParams(
            collective_id=0, has_side_effects=True, vmem_limit_bytes=VMEM_LIMIT
        ),
        name="cg_step",
    )(noise_var, residual_in, direction, spectrum.T, *(jnp.asarray(t) for t in (consts, turns)))
    return pl.pallas_call(
        finish,
        out_shape=(
            jax.ShapeDtypeStruct(block, F32),
            jax.ShapeDtypeStruct(block, F32),
            jax.ShapeDtypeStruct((probes,), F32),
        ),
        in_specs=[vmem_spec] * 4,
        out_specs=(vmem_spec, vmem_spec, smem_spec),
        compiler_params=pltpu.CompilerParams(vmem_limit_bytes=8 << 20),
        name="finish",
    )(total, residual_in, direction, image)


def solution(mesh):
    in_specs = (P("grp", ROW_SUB, None), P("grp", ROW_SUB, None), P("grp", ROW_SUB), P("grp"))
    out_specs = (P("grp", ROW_SUB, None), P("grp", ROW_SUB, None), P("grp"))
    return jax.shard_map(
        functools.partial(body, mesh.shape["row"], mesh.shape["sub"]),
        mesh=mesh, in_specs=in_specs, out_specs=out_specs, check_vma=False,
    )
```

```python
import functools
import math

import jax
import jax.numpy as jnp
import ml_dtypes
import numpy as np
from jax import lax
from jax.experimental import pallas as pl
from jax.experimental.pallas import tpu as pltpu
from jax.sharding import PartitionSpec as P

ROW_SUB = ("row", "sub")
MESH = pl.DeviceIdType.MESH
TINY = 1e-06
VMEM_LIMIT = 107 << 19
LANES = 128
RADIX = 16
F32 = jnp.float32
BF16 = jnp.bfloat16


def roots(left, right, modulus, sign):
    turns = np.mod(np.outer(left, right), modulus)
    return np.exp(sign * 2j * np.pi * turns / modulus)


def real_form(table):
    return np.block([[table.real, -table.imag], [table.imag, table.real]])


def halves(table):
    high = table.astype(ml_dtypes.bfloat16)
    low = (table - high.astype(np.float64)).astype(ml_dtypes.bfloat16)
    return np.stack([high, low])


def tables(rows_dev, grid_len, devices):
    embed = 2 * grid_len
    lane_ids = np.arange(LANES)
    dev_ids = np.arange(devices)
    block = LANES // RADIX
    long_row = real_form(roots(dev_ids, lane_ids, LANES, -1))
    low_ids = np.arange(embed // RADIX)
    long_col = real_form(roots(low_ids, dev_ids, embed // RADIX, -1))
    short = roots(np.arange(RADIX), np.arange(RADIX), RADIX, -1)
    mixed = np.zeros((block, RADIX, RADIX, block), complex)
    for e in range(block):
        mixed[e, :, :, e] = short
    mixed = mixed.reshape(LANES, LANES)
    short_col = real_form(mixed.T).T
    short_back = real_form(np.conj(mixed)).T
    long_back = real_form(np.conj(roots(dev_ids, low_ids, embed // RADIX, -1)))
    half = long_back.shape[1] // 2
    row_back = real_form(np.conj(roots(lane_ids, dev_ids, LANES, -1))).T
    stacked = np.concatenate(
        [long_row, long_col, short_col, short_back, long_back[:, :half], long_back[:, half:], row_back], axis=0
    )
    consts = halves(stacked)
    turn_col = np.tile(roots(low_ids, np.arange(RADIX), embed, -1), (1, block))
    turn_col = np.stack([turn_col.real, turn_col.imag]).astype(np.float32)
    turn_row = np.zeros((2, 2 * RADIX, 2, LANES))
    for ch in range(2):
        for e in range(RADIX):
            turn = roots([2 * e + ch], lane_ids, embed, -1)[0]
            turn_row[ch, e] = [turn.real, turn.imag]
            odd = np.exp(-2j * np.pi * e * ch / (2 * RADIX))
            turn_row[ch, RADIX + e, 0] = odd.real
            turn_row[ch, RADIX + e, 1] = odd.imag
    turns = np.concatenate([turn_row.reshape(-1, LANES), turn_col.reshape(-1, LANES)]).astype(np.float32)
    return consts, turns


def add(x, y):
    return (x[0] + y[0], x[1] + y[1])


def sub(x, y):
    return (x[0] - y[0], x[1] - y[1])


def times(x, y):
    return (x[0] * y[0] - x[1] * y[1], x[0] * y[1] + x[1] * y[0])


def times_conj(x, y):
    return (x[0] * y[0] + x[1] * y[1], x[1] * y[0] - x[0] * y[1])


def by_root(x, power, sign):
    power %= RADIX
    if power == 0:
        return x
    if power == 4:
        return (x[1], -x[0]) if sign < 0 else (-x[1], x[0])
    if power == 8:
        return (-x[0], -x[1])
    angle = sign * 2.0 * math.pi * power / RADIX
    return times(x, (math.cos(angle), math.sin(angle)))


def four(x, sign):
    even, odd = add(x[0], x[2]), sub(x[0], x[2])
    both, diff = add(x[1], x[3]), sub(x[1], x[3])
    turned = (diff[1], -diff[0]) if sign < 0 else (-diff[1], diff[0])
    return [add(even, both), add(odd, turned), sub(even, both), sub(odd, turned)]


def sixteen(x, sign):
    inner = [four([x[4 * i + j] for i in range(4)], sign) for j in range(4)]
    out = [None] * RADIX
    for first in range(4):
        column = [by_root(inner[j][first], j * first, sign) for j in range(4)]
        for second, value in enumerate(four(column, sign)):
            out[first + 4 * second] = value
    return out


def split(value):
    high = value.astype(BF16)
    return high, (value - high.astype(F32)).astype(BF16)


def dot(left, right, transposed=False):
    dims = (((1,), (1 if transposed else 0,)), ((), ()))
    return lax.dot_general(left, right, dims, preferred_element_type=F32)


def dot3(left, right, transposed=False):
    return (
        dot(left[1], right[0], transposed) + dot(left[0], right[1], transposed) + dot(left[0], right[0], transposed)
    )


def far_first(n_row, n_sub):
    def chips(row, sub_):
        hop = row // 2
        return min(hop, n_row // 2 - hop) + min(sub_, n_sub - sub_)

    offsets = [(i, j) for i in range(n_row) for j in range(n_sub)][1:]
    return sorted(offsets, key=lambda pair: -chips(*pair))


def outward(count):
    return [count // 2 + (1 - 2 * (t % 2)) * ((t + 1) // 2) for t in range(count)]


def kernel(
    n_row, n_sub, scale,
    noise_ref, resid_hbm, dir_hbm, spec_hbm, consts_hbm, turns_hbm,
    image, total_out,
    resid, direct, spec, consts, turns,
    out_f, in_f, out_b, in_b, sums, spec_t,
    work, tall, left_hi, left_lo, right_hi, right_lo,
    load_sem, send_f, recv_f, send_b, recv_b, send_s, recv_s, here_sem,
):
    devices = n_row * n_sub
    row, sub_ = lax.axis_index("row"), lax.axis_index("sub")
    me = row * n_sub + sub_
    offsets = far_first(n_row, n_sub)
    wide = 2 * LANES
    low_len = tall.shape[0] // 2

    def load(src, dst, slot):
        copy = pltpu.make_async_copy(src, dst, load_sem.at[slot])
        copy.start()
        return copy

    def wrap(value, count):
        return jnp.where(value >= count, value - count, value)

    def peer(i, j):
        hop, core = i // 2, row % 2
        to_core = core if i % 2 == 0 else 1 - core
        return 2 * wrap(row // 2 + hop, n_row // 2) + to_core, wrap(sub_ + j, n_sub)

    subs = [wrap(sub_ + j, n_sub) for j in outward(n_sub)]
    rows = [wrap(row + i, n_row) for i in outward(n_row)]
    apart = lax.axis_index("grp") == 0
    late = apart & (me == 0)

    def ordinary(to_row, to_sub):
        return (to_row + to_sub != 0) | jnp.logical_not(apart)

    level = jnp.where(late, n_sub, sub_)

    def each_peer(act):
        def one_row(t, carry):
            half = n_row // 2
            to_row = wrap(row + half + (1 - 2 * (t % 2)) * ((t + 1) // 2), n_row)
            for to_sub in subs:
                act(to_row, to_sub)
            return carry

        lax.fori_loop(0, n_row - 1, one_row, 0)
        for to_sub in subs[:-1]:
            act(row, to_sub)

    first, rest = pl.ds(0, wide), pl.ds(wide, consts.shape[1] - wide)
    loads = [
        load(dir_hbm, direct, 0),
        load(turns_hbm.at[pl.ds(0, 8 * RADIX)], turns.at[pl.ds(0, 8 * RADIX)], 1),
        load(consts_hbm.at[:, first], consts.at[:, first], 2),
    ]
    barrier = pltpu.get_barrier_semaphore()

    def greet(to_row, to_sub):
        pl.semaphore_signal(barrier, inc=1, device_id={"row": to_row, "sub": to_sub}, device_id_type=MESH)

    def announce(to_row, to_sub):
        pl.semaphore_signal(here_sem.at[level], inc=1, device_id={"row": to_row, "sub": to_sub}, device_id_type=MESH)

    def greet_sub(to_sub, carry):
        @pl.when(to_sub > sub_)
        def _():
            for to_row in rows:
                greet(to_row, to_sub)

        return carry

    @pl.when(jnp.logical_not(late))
    def _():
        for to_row in rows[:-1]:
            greet(to_row, sub_)
        lax.fori_loop(1, n_sub, greet_sub, 0)
        pl.when(apart & (sub_ != 0))(lambda: greet(0, 0))

    later_loads = [
        load(consts_hbm.at[:, rest], consts.at[:, rest], 5),
        load(turns_hbm.at[pl.ds(8 * RADIX, 2 * low_len)], turns.at[pl.ds(8 * RADIX, 2 * low_len)], 6),
        load(resid_hbm, resid, 3),
    ]
    for t in range(spec.shape[0]):
        load(spec_hbm.at[:, pl.ds(LANES * t, LANES)], spec.at[t], 4)

    def const(index, count=1):
        rows = pl.ds(wide * index, wide * count)
        return consts[0, rows, :], consts[1, rows, :]

    def send(src, dst, ch, send_sem, recv_sem, to_row, to_sub):
        part = pl.ds(4 * ch, 4)
        pltpu.make_async_remote_copy(
            src.at[to_row * n_sub + to_sub, part],
            dst.at[me, part],
            send_sem.at[ch],
            recv_sem.at[ch],
            device_id={"row": to_row, "sub": to_sub},
            device_id_type=MESH,
        ).start()

    def send_all(src, dst, ch, send_sem, recv_sem, all_here):
        for i, j in offsets:
            to_row, to_sub = peer(i, j)
            go = functools.partial(send, src, dst, ch, send_sem, recv_sem, to_row, to_sub)
            if all_here:
                go()
            else:
                pl.when(ordinary(to_row, to_sub) & (to_sub <= level))(go)
        part = pl.ds(4 * ch, 4)
        dst[me, part] = src[me, part]

    def wait_all(ref, ch, sem):
        others = ref.at[pl.ds(0, devices - 1), pl.ds(4 * ch, 4)]
        pltpu.make_async_copy(others, others, sem.at[ch]).wait()

    def flat(ref):
        return ref.reshape(devices * 8, LANES)

    def turn(ch, index):
        both = turns[pl.ds(4 * RADIX * ch + 2 * index, 2), :]
        return both[0:1], both[1:2]

    def turn_col(at, step):
        first = 8 * RADIX + at
        return turns[pl.ds(first, step), :], turns[pl.ds(first + low_len, step), :]

    @pl.when(late)
    def _():
        pl.semaphore_wait(barrier, devices - 1)
        each_peer(announce)

    for copy in loads:
        copy.wait()

    def rows_forward(ch, carry):
        for top in range(2):
            lines = pl.ds(8 * top, 8)
            values = []
            for a in range(RADIX):
                lanes = pl.ds(LANES * a, LANES)
                values.append(times((direct[0, lines, lanes], direct[1, lines, lanes]), turn(ch, RADIX + a)))
            for e, value in enumerate(sixteen(values, -1)):
                value = times(value, turn(ch, e))
                for part in range(2):
                    work[pl.ds(RADIX * e + 8 * top, 8), pl.ds(LANES * part, LANES)] = value[part]
        for at in range(0, wide, 32):
            lines = pl.ds(at, 32)
            right_hi[lines, :], right_lo[lines, :] = split(work[lines, :])
        freq = dot3(const(0), (right_hi[pl.ds(0, wide), :], right_lo[pl.ds(0, wide), :]), transposed=True)
        for part in range(2):
            for tile in range(2):
                flat(out_f)[pl.ds(4 * ch + 2 * part + tile, devices, stride=8), :] = freq[
                    devices * part : devices * (part + 1), LANES * tile : LANES * (tile + 1)
                ]

        @pl.when(ch == 0)
        def _():
            @pl.when(jnp.logical_not(late))
            def _():
                pl.semaphore_wait(barrier, n_row * (sub_ + 1) - 1 - apart.astype(jnp.int32))
                for to_sub in range(n_sub):
                    pl.when((to_sub < sub_) & ordinary(row, to_sub))(functools.partial(announce, row, to_sub))

        send_all(out_f, in_f, ch, send_f, recv_f, False)
        return carry

    lax.fori_loop(0, 2, rows_forward, 0)

    for copy in later_loads:
        copy.wait()
    pltpu.make_async_copy(spec, spec, load_sem.at[4]).wait()
    spec_rows = spec.reshape(spec.shape[0] * spec.shape[1], LANES)
    for ch in range(2):
        for tile in range(2):
            for top in range(low_len // LANES):
                parts = []
                for high in range(RADIX):
                    at = spec.shape[1] * ((low_len // LANES) * high + top) + RADIX * tile + ch
                    parts.append(spec_rows[pl.ds(at, 8, stride=2), :])
                spec_t[pl.ds(LANES * top, LANES), pl.ds(wide * ch + LANES * tile, LANES)] = (
                    jnp.concatenate(parts, axis=0).T * scale
                )

    def later_class(t, carry):
        ch, to_sub = t // n_sub, t % n_sub

        @pl.when(to_sub > level)
        def _():
            pl.when(ch == 0)(lambda: pl.semaphore_wait(here_sem.at[to_sub], 1))
            for to_row in rows:
                send(out_f, in_f, ch, send_f, recv_f, to_row, to_sub)

        return carry

    lax.fori_loop(0, 2 * n_sub, later_class, 0)

    @pl.when(apart & jnp.logical_not(late))
    def _():
        pl.semaphore_wait(here_sem.at[n_sub], 1)
        for ch in range(2):
            send(out_f, in_f, ch, send_f, recv_f, 0, 0)

    def columns(ch, carry):
        wait_all(in_f, ch, recv_f)
        for part in range(2):
            for tile in range(2):
                here = (pl.ds(devices * part, devices), pl.ds(LANES * tile, LANES))
                right_hi[here], right_lo[here] = split(
                    flat(in_f)[pl.ds(4 * ch + 2 * part + tile, devices, stride=8), :]
                )
        tall[...] = dot3(const(1, 2), (right_hi[pl.ds(0, wide), :], right_lo[pl.ds(0, wide), :]))
        step = 32
        for tile in range(2):
            lanes = pl.ds(LANES * tile, LANES)
            for at in range(0, low_len, step):
                lines = pl.ds(at, step)
                value = times(
                    (tall[lines, lanes], tall[pl.ds(low_len + at, step), lanes]),
                    turn_col(at, step),
                )
                for part in range(2):
                    here = (pl.ds(low_len * tile + at, step), pl.ds(LANES * part, LANES))
                    left_hi[here], left_lo[here] = split(value[part])
        tall[...] = dot3((left_hi[...], left_lo[...]), const(3))
        for tile in range(2):
            for at in range(0, low_len, step):
                weight = spec_t[pl.ds(at, step), pl.ds(pl.multiple_of(wide * ch + LANES * tile, LANES), LANES)]
                for part in range(2):
                    here = (pl.ds(low_len * tile + at, step), pl.ds(LANES * part, LANES))
                    left_hi[here], left_lo[here] = split(tall[here] * weight)
        tall[...] = dot3((left_hi[...], left_lo[...]), const(4))
        for tile in range(2):
            for at in range(0, low_len, step):
                lines = pl.ds(at, step)
                here = pl.ds(low_len * tile + at, step)
                value = times_conj(
                    (tall[here, pl.ds(0, LANES)], tall[here, pl.ds(LANES, LANES)]),
                    turn_col(at, step),
                )
                for part in range(2):
                    there = (pl.ds(low_len * part + at, step), pl.ds(LANES * tile, LANES))
                    right_hi[there], right_lo[there] = split(value[part])
        low, high = pl.ds(0, low_len), pl.ds(low_len, low_len)
        grid = dot3(const(5), (right_hi[low, :], right_lo[low, :])) + dot3(
            const(6), (right_hi[high, :], right_lo[high, :])
        )
        for part in range(2):
            for tile in range(2):
                flat(out_b)[pl.ds(4 * ch + 2 * part + tile, devices, stride=8), :] = grid[
                    devices * part : devices * (part + 1), LANES * tile : LANES * (tile + 1)
                ]
        send_all(out_b, in_b, ch, send_b, recv_b, True)
        return carry

    lax.fori_loop(0, 2, columns, 0)

    noise = noise_ref[0]
    image[...] = noise * direct[...]

    def rows_back(ch, carry):
        wait_all(in_b, ch, recv_b)
        for part in range(2):
            for tile in range(2):
                here = (pl.ds(LANES * tile, LANES), pl.ds(devices * part, devices))
                block = flat(in_b)[pl.ds(4 * ch + 2 * part + tile, devices, stride=8), :]
                left_hi[here], left_lo[here] = split(block.T)
        work[...] = dot3((left_hi[pl.ds(0, wide), :], left_lo[pl.ds(0, wide), :]), const(7))
        for top in range(2):
            values = []
            for e in range(RADIX):
                lines = pl.ds(RADIX * e + 8 * top, 8)
                values.append(
                    times_conj((work[lines, pl.ds(0, LANES)], work[lines, pl.ds(LANES, LANES)]), turn(ch, e))
                )
            lines = pl.ds(8 * top, 8)
            for a, value in enumerate(sixteen(values, 1)):
                value = times_conj(value, turn(ch, RADIX + a))
                lanes = pl.ds(LANES * a, LANES)
                for part in range(2):
                    image[part, lines, lanes] += value[part]
        return carry

    lax.fori_loop(0, 2, rows_back, 0)

    def sum_rows(value):
        return jnp.sum(value, axis=0, keepdims=True)

    lines = []
    for probe in range(2):
        totals = [jnp.zeros((8, LANES), F32) for _ in range(4)]
        for top in range(2):
            for a in range(direct.shape[2] // LANES):
                here = (probe, pl.ds(8 * top, 8), pl.ds(LANES * a, LANES))
                r, d, q = resid[here], direct[here], image[here]
                for index, term in enumerate((r * r, d * q, r * q, q * q)):
                    totals[index] += term
        lines += [sum_rows(total) for total in totals]
    stacked = jnp.sum(jnp.concatenate(lines, axis=0), axis=1, keepdims=True)
    at_row = lax.broadcasted_iota(jnp.int32, (8, LANES), 0)
    at_lane = lax.broadcasted_iota(jnp.int32, (8, LANES), 1)
    mine = sum_rows(jnp.where(at_row == at_lane, stacked, 0.0))
    sums[me] = mine

    def tell(to_row, to_sub):
        pltpu.make_async_remote_copy(
            sums.at[me], sums.at[me], send_s, recv_s,
            device_id={"row": to_row, "sub": to_sub}, device_id_type=MESH,
        ).start()

    for i, j in offsets:
        tell(*peer(i, j))
    for ch in range(2):
        wait_all(out_f, ch, send_f)
        wait_all(out_b, ch, send_b)
    others = sums.at[pl.ds(0, devices - 1)]
    pltpu.make_async_copy(others, others, send_s).wait()
    pltpu.make_async_copy(others, others, recv_s).wait()
    total_out[...] = jnp.sum(sums[...], axis=0)


def finish(total_ref, resid, direct, image, resid_out, dir_out, step_out):
    total = total_ref[...]
    for probe in range(2):
        old_norm, curvature, cross, square = (total[:, 4 * probe + i : 4 * probe + i + 1] for i in range(4))
        size = old_norm / curvature
        new_norm = old_norm - 2.0 * (size * cross) + size * (size * square)
        ratio = new_norm / (old_norm + TINY)
        step_out[probe] = size[0, 0]
        for a in range(direct.shape[2] // LANES):
            here = (probe, slice(None), pl.ds(LANES * a, LANES))
            value = resid[here] - size * image[here]
            resid_out[here] = value
            dir_out[here] = value + ratio * direct[here]


def body(n_row, n_sub, residual_in, direction, spectrum, noise_var):
    probes, rows_dev, grid_len = direction.shape
    devices = n_row * n_sub
    embed = 2 * grid_len
    consts, turns = tables(rows_dev, grid_len, devices)
    low_len = embed // RADIX
    wide = 2 * LANES
    slots = (devices, 8, LANES)
    vmem = pltpu.VMEM
    sems = pltpu.SemaphoreType.DMA
    block = (probes, rows_dev, grid_len)
    hbm_spec = pl.BlockSpec(memory_space=pltpu.HBM)
    vmem_spec = pl.BlockSpec(memory_space=pltpu.VMEM)
    smem_spec = pl.BlockSpec(memory_space=pltpu.SMEM)
    image, total = pl.pallas_call(
        functools.partial(kernel, n_row, n_sub, 1.0 / (embed * embed)),
        out_shape=(jax.ShapeDtypeStruct(block, F32), jax.ShapeDtypeStruct((1, LANES), F32)),
        in_specs=[smem_spec] + [hbm_spec] * 5,
        out_specs=(vmem_spec, vmem_spec),
        scratch_shapes=[
            vmem(block, F32), vmem(block, F32), vmem((embed // LANES, spectrum.shape[1], LANES), F32),
            vmem(consts.shape, BF16), vmem(turns.shape, F32),
            vmem(slots, F32), vmem(slots, F32), vmem(slots, F32), vmem(slots, F32),
            vmem((devices, 1, LANES), F32), vmem((low_len, 4 * LANES), F32),
            vmem((wide, wide), F32), vmem((2 * low_len, wide), F32),
            vmem((2 * low_len, wide), BF16), vmem((2 * low_len, wide), BF16),
            vmem((2 * low_len, wide), BF16), vmem((2 * low_len, wide), BF16),
            sems((7,)), sems((2,)), sems((2,)), sems((2,)), sems((2,)), sems, sems, pltpu.SemaphoreType.REGULAR((n_sub + 1,)),
        ],
        compiler_params=pltpu.CompilerParams(
            collective_id=0, has_side_effects=True, vmem_limit_bytes=VMEM_LIMIT
        ),
        name="cg_step",
    )(noise_var, residual_in, direction, spectrum.T, *(jnp.asarray(t) for t in (consts, turns)))
    return pl.pallas_call(
        finish,
        out_shape=(
            jax.ShapeDtypeStruct(block, F32),
            jax.ShapeDtypeStruct(block, F32),
            jax.ShapeDtypeStruct((probes,), F32),
        ),
        in_specs=[vmem_spec] * 4,
        out_specs=(vmem_spec, vmem_spec, smem_spec),
        compiler_params=pltpu.CompilerParams(vmem_limit_bytes=8 << 20),
        name="finish",
    )(total, residual_in, direction, image)


def solution(mesh):
    in_specs = (P("grp", ROW_SUB, None), P("grp", ROW_SUB, None), P("grp", ROW_SUB), P("grp"))
    out_specs = (P("grp", ROW_SUB, None), P("grp", ROW_SUB, None), P("grp"))
    return jax.shard_map(
        functools.partial(body, mesh.shape["row"], mesh.shape["sub"]),
        mesh=mesh, in_specs=in_specs, out_specs=out_specs, check_vma=False,
    )
```
